32 devices in a mesh: dp: 2 (over core), row: 4 (over y, x), col: 4 (over z).
Axes of the slice: x: 2, y: 2, z: 4, core: 2. Of those that a mesh axis runs over, the one named last changes fastest.
Arguments:
- tokens: bfloat16 [8, 257, 1408], P(('dp', 'col'), None, 'row'), may hold values from -6 to 6
- cotangent: bfloat16 [8, 257, 1408], P(('dp', 'col'), None, 'row'), may hold values from -6 to 6
- qkv_weight: bfloat16 [2, 1408, 3, 1408], P(None, 'row', None, 'col'), may hold values from -0.15625 to 0.15625
- qv_bias: float32 [2, 2, 1408], P(None, None, 'col'), may hold values from -3 to 3
- proj_weight: bfloat16 [2, 1408, 1408], P(None, 'col', 'row'), may hold values from -0.625 to 0.625
- proj_bias: float32 [2, 1408], P(None, 'row'), may hold values from -3 to 3
- up_weight: bfloat16 [2, 1408, 6144], P(None, 'row', 'col'), may hold values from -0.15625 to 0.15625
- up_bias: float32 [2, 6144], P(None, 'col'), may hold values from -3 to 3
- down_weight: bfloat16 [2, 6144, 1408], P(None, 'col', 'row'), may hold values from -0.078125 to 0.078125
- down_bias: float32 [2, 1408], P(None, 'row'), may hold values from -3 to 3
- norm_gain: float32 [2, 2, 1408], P(None, None, 'row'), may hold values from 0.25 to 1.75
- norm_shift: float32 [2, 2, 1408], P(None, None, 'row'), may hold values from -3 to 3
Outputs:
- out: float32 [8, 257, 1408], P(('dp', 'col'), None, 'row')
- tokens_grad: float32 [8, 257, 1408], P(('dp', 'col'), None, 'row')
- qkv_weight_grad: float32 [2, 1408, 3, 1408], P('dp', 'row', None, 'col')
- qv_bias_grad: float32 [2, 2, 1408], P('dp', None, 'col')
- proj_weight_grad: float32 [2, 1408, 1408], P('dp', 'col', 'row')
- proj_bias_grad: float32 [2, 1408], P('dp', 'row')
- up_weight_grad: float32 [2, 1408, 6144], P('dp', 'row', 'col')
- up_bias_grad: float32 [2, 6144], P('dp', 'col')
- down_weight_grad: float32 [2, 6144, 1408], P('dp', 'col', 'row')
- down_bias_grad: float32 [2, 1408], P('dp', 'row')
- norm_gain_grad: float32 [2, 2, 1408], P(None, None, 'row')
- norm_shift_grad: float32 [2, 2, 1408], P(None, None, 'row')
The draws below stay inside these ranges and needn't reach their ends.
All inputs are finite; a program needn't handle non-finite values.
Results may differ from the reference program's by a relative error of at most 0.03.
Values may be sent and summed in bfloat16 or wider, within the bound.
A program may use at most 128 MiB of HBM per device.

```python
import jax
import jax.numpy as jnp
from jax import lax

D = 1408
HEADS = 16
HEAD_DIM = 88
FF = 6144
SEQ = 257
LAYERS = 2
IMAGES = 8


def block_levels(key, dims, cuts, smallest, largest):
    def one(position, shards_of):
        heights = jax.random.uniform(jax.random.fold_in(jax.random.fold_in(key, 6), position), (shards_of,), jnp.float32, smallest / len(cuts), largest / len(cuts))
        return jnp.repeat(jnp.exp(heights), dims[position] // shards_of).reshape((-1,) + (1,) * (len(dims) - position - 1))

    factor_of = one(*cuts[0])
    for cut in cuts[1:]:
        factor_of = factor_of * one(*cut)
    return factor_of


def centred(own_key, extent, width, limit, cuts=(), dtype=jnp.bfloat16):
    entries = jax.random.normal(own_key, extent, jnp.float32) * width
    if len(cuts) > 0:
        entries = block_levels(own_key, extent, cuts, -0.22, 0.18) * entries
    return jnp.clip(entries, min=-limit, max=limit).astype(dtype)


def setup_inputs(seed: int = 0) -> dict:
    key_list = jax.random.split(jax.random.key(seed), 13)
    tokens = centred(key_list[0], (IMAGES, SEQ, D), 1.0, 6.0, ((0, 8), (2, 4)))
    cotangent = centred(key_list[1], (IMAGES, SEQ, D), 1.0, 6.0, ((0, 8), (2, 4)))
    qkv_weight = centred(key_list[2], (LAYERS, D, 3, D), D ** -0.5, 0.15625, ((1, 4), (3, 4)))
    qv_bias = centred(key_list[3], (LAYERS, 2, D), 0.5, 3.0, ((2, 4),), jnp.float32)
    proj_weight = centred(key_list[4], (LAYERS, D, D), (D // 16) ** -0.5, 0.625, ((1, 4), (2, 4)))
    proj_bias = centred(key_list[5], (LAYERS, D), 0.5, 3.0, ((1, 4),), jnp.float32)
    up_weight = centred(key_list[6], (LAYERS, D, FF), D ** -0.5, 0.15625, ((1, 4), (2, 4)))
    up_bias = centred(key_list[7], (LAYERS, FF), 0.5, 3.0, ((1, 4),), jnp.float32)
    down_weight = centred(key_list[8], (LAYERS, FF, D), FF ** -0.5, 0.078125, ((1, 4), (2, 4)))
    down_bias = centred(key_list[9], (LAYERS, D), 0.5, 3.0, ((1, 4),), jnp.float32)
    norm_gain = jnp.clip(1.0 + 0.15 * jax.random.normal(key_list[10], (LAYERS, 2, D), jnp.float32), 0.25, 1.75)
    norm_shift = centred(key_list[11], (LAYERS, 2, D), 0.5, 3.0, ((2, 4),), jnp.float32)
    return {"tokens": tokens, "cotangent": cotangent, "qkv_weight": qkv_weight, "qv_bias": qv_bias, "proj_weight": proj_weight, "proj_bias": proj_bias, "up_weight": up_weight, "up_bias": up_bias, "down_weight": down_weight, "down_bias": down_bias, "norm_gain": norm_gain, "norm_shift": norm_shift}


@jax.custom_vjp
def low(v):
    return lax.optimization_barrier(v.astype(jnp.bfloat16)).astype(jnp.float32)

@jax.custom_vjp
def low_back(v):
    return v

def low_keep(v):
    return (low(v), None)

def low_pass(kept, grad):
    return (grad,)

def back_keep(v):
    return (v, None)

def back_low(kept, grad):
    return (low(grad),)
low.defvjp(low_keep, low_pass)
low_back.defvjp(back_keep, back_low)
EPSILON = 1e-06

def product(left, right):
    return jnp.dot(left, right, precision=lax.Precision.HIGHEST, preferred_element_type=jnp.float32)

def layer_norm(stream, factor, shift):
    centre = lax.optimization_barrier(jnp.mean(stream, axis=-1, keepdims=True))
    spread = lax.optimization_barrier(jnp.mean(stream * stream, axis=-1, keepdims=True)) - centre * centre
    return (stream - centre) * lax.rsqrt(spread + EPSILON) * factor + shift

def attend_image(triple):
    pieces = triple.reshape(SEQ, 3, HEADS, HEAD_DIM)
    scaling = HEAD_DIM ** (-0.5)
    scores = low_back(scaling * jnp.einsum('qhd,khd->hqk', pieces[:, 0], pieces[:, 1], precision=lax.Precision.HIGHEST))
    probs = low(jax.nn.softmax(scores, axis=-1))
    attended = jnp.einsum('hqk,khd->qhd', probs, pieces[:, 2], precision=lax.Precision.HIGHEST)
    return attended.reshape(SEQ, HEADS * HEAD_DIM)

def residual_block(stream, qkv_w, qv_b, proj_w, proj_b, up_w, up_b, down_w, down_b, factors, shifts):
    normed = low(layer_norm(stream, factors[0], shifts[0]))
    offsets = jnp.concatenate([qv_b[0], jnp.zeros_like(qv_b[0]), qv_b[1]])
    triple = low(low_back(product(normed, qkv_w.reshape(D, 3 * D)) + offsets))
    attended = lax.map(jax.checkpoint(attend_image), triple.reshape(-1, SEQ, 3 * D))
    attended = low(low_back(attended.reshape(-1, D)))
    stream = stream + low_back(product(attended, proj_w) + proj_b)
    normed = low(layer_norm(stream, factors[1], shifts[1]))
    before = low_back(product(normed, up_w) + up_b)
    activated = low(jax.nn.gelu(before, approximate=False))
    return stream + low_back(product(activated, down_w) + down_b)

def reference(tokens, cotangent, qkv_weight, qv_bias, proj_weight, proj_bias, up_weight, up_bias, down_weight, down_bias, norm_gain, norm_shift):

    def forward(stream, qkv_all, qv_all, proj_all, proj_off, up_all, up_off, down_all, down_off, gain_all, shift_all):
        stream = stream.reshape(IMAGES * SEQ, D)
        for layer_index in range(LAYERS):
            stream = residual_block(stream, qkv_all[layer_index], qv_all[layer_index], proj_all[layer_index], proj_off[layer_index], up_all[layer_index], up_off[layer_index], down_all[layer_index], down_off[layer_index], gain_all[layer_index], shift_all[layer_index])
        return stream.reshape(IMAGES, SEQ, D)
    inputs = (tokens, qkv_weight, qv_bias, proj_weight, proj_bias, up_weight, up_bias, down_weight, down_bias, norm_gain, norm_shift)
    primals = tuple((argument.astype(jnp.float32) for argument in inputs))
    result, pullback = jax.vjp(forward, *primals)
    gradients = pullback(cotangent.astype(jnp.float32))
    return (result, gradients[0], gradients[1], gradients[2], gradients[3], gradients[4], gradients[5], gradients[6], gradients[7], gradients[8], gradients[9], gradients[10])
```

```python
from functools import partial

import jax
import jax.numpy as jnp
from jax import lax
from jax.experimental import pallas as pl
from jax.experimental.pallas import tpu as pltpu
from jax.sharding import PartitionSpec as P

D = 1408
HEAD_DIM = 88
SEQ = 257
LAYERS = 2
EPSILON = 1e-06
MESH = pl.DeviceIdType.MESH
BF = jnp.bfloat16
F32 = jnp.float32

ROWS = 272
STEP = 64
CHUNK = 80
BLK = 352
PAD = 384
HALF = 768
N = 4


def dot(a, b):
    return jnp.dot(a, b, preferred_element_type=F32)


def dot_t(a, b):
    return lax.dot_general(a, b, (((1,), (1,)), ((), ())), preferred_element_type=F32)


def t_dot(a, b):
    return lax.dot_general(a, b, (((0,), (0,)), ((), ())), preferred_element_type=F32)


def span(index):
    return pl.ds(STEP * index, STEP if index < N - 1 else CHUNK)


def head_span(head):
    low, high = HEAD_DIM * head, HEAD_DIM * (head + 1)
    return low, high, low // 128 * 128, -(-high // 128) * 128


def kernel(
    tok_hbm, cot_hbm, w_hbm, vec_ref, qb_ref, ub_ref,
    out_hbm, tg_hbm, g_hbm, vsum, csum,
    w, x1, x2, triple, att, lse, hid, slope, std, inv,
    gtop, gmid, lt, part, recv, st, gst, tmp, tin, cin, oblk, pin, pv,
    gb, da, g3, acc, sbuf, prx, keep, ici, fin,
    wloc, wsend, wrecv, psend, precv, vs, vr, toks, tokr, cots, cotr,
    zs, zr, rss, rsr, outs, outr, tgs, tgr, cs_s, cs_r, credit, gis, gir, fins, finr,
):
    d, r, c = lax.axis_index("dp"), lax.axis_index("row"), lax.axis_index("col")
    other = 1 - d
    near = (r + 1 - 2 * lax.rem(r, 2), lax.rem(r + 2, N), N - 1 - r)
    last = c == N - 1

    def remote(src, dst, ssem, rsem, dev):
        return pltpu.make_async_remote_copy(
            src, dst, ssem, rsem, device_id=dev, device_id_type=MESH
        )

    def rblk(index):
        return pl.ds(pl.multiple_of(index * BLK, 16), BLK)

    recv[...] = jnp.zeros_like(recv)
    tin[...] = jnp.zeros_like(tin)
    cin[...] = jnp.zeros_like(cin)
    vsum[...] = jnp.zeros_like(vsum)
    barrier = pltpu.get_barrier_semaphore()
    for k in range(N * N):
        pl.semaphore_signal(
            barrier, inc=1,
            device_id=(d, lax.rem(r + k // N, N), lax.rem(c + k % N, N)), device_id_type=MESH,
        )
    pl.semaphore_signal(barrier, inc=1, device_id=(other, r, c), device_id_type=MESH)
    pl.semaphore_wait(barrier, N * N + 1)

    for k in range(3):
        remote(vec_ref, pin.at[r], vs.at[k], vr.at[k], (d, near[k], c)).start()
    own_vec = pltpu.make_async_copy(vec_ref, pin.at[r], vr.at[3])
    own_vec.start()

    def spread(src, dst, ssem, rsem, start):
        for ct in range(N):
            mine = jnp.logical_and(r == c, c == ct)
            size = STEP if ct < N - 1 else CHUNK
            source, target = src.at[span(ct)], dst.at[r, pl.ds(0, size)]

            @pl.when(mine)
            def _():
                if start:
                    pltpu.make_async_copy(source, target, rsem.at[r]).start()

            @pl.when(jnp.logical_not(mine))
            def _():
                copy = remote(source, target, ssem.at[ct], rsem.at[r], (d, c, ct))
                if start:
                    copy.start()
                else:
                    copy.wait_send()

    def spread_wait(src, dst, rsem):
        def at_size(ct):
            size = STEP if ct < N - 1 else CHUNK
            for rs in range(N):
                pltpu.make_async_copy(
                    src.at[span(ct)], dst.at[rs, pl.ds(0, size)], rsem.at[rs]
                ).wait()

        @pl.when(last)
        def _():
            at_size(N - 1)

        @pl.when(jnp.logical_not(last))
        def _():
            at_size(0)

    spread(tok_hbm, tin, toks, tokr, True)

    def local_w(l, b):
        return pltpu.make_async_copy(w_hbm.at[l, b], w.at[l, b, rblk(r)], wloc.at[l, b])

    def send_w(l, i, k):
        b = 2 * i + d
        return remote(
            w_hbm.at[l, b], w.at[l, b, rblk(r)], wsend.at[l, i, k], wrecv.at[l, i, k],
            (d, near[k], c),
        )

    def share_w(l, i, k):
        b = 2 * i + d
        rows = w.at[l, b, rblk(near[k])]
        return remote(rows, rows, psend.at[l, i, k], precv.at[l, i, k], (other, r, c))

    for b in range(6):
        local_w(0, b).start()
    for l in range(LAYERS):
        for i in range(3):
            for k in range(3):
                send_w(l, i, k).start()
            if l == 0 and i == 0:
                spread(cot_hbm, cin, cots, cotr, True)
    for b in range(6):
        local_w(1, b).start()

    def forward_w(l, i):
        for k in range(3):
            send_w(l, i, k).wait_recv()
            share_w(l, i, k).start()

    def need_w(l, i):
        local_w(l, 2 * i).wait()
        local_w(l, 2 * i + 1).wait()
        for k in range(3):
            b = 2 * i + other
            rows = w.at[l, b, rblk(near[k])]
            pltpu.make_async_copy(rows, rows, precv.at[l, i, k]).wait()

    def gather_start(x):
        for cs in range(N):

            @pl.when(c == cs)
            def _():
                for ct in range(N):
                    if ct != cs:
                        rows = x.at[span(cs)]
                        remote(rows, rows, zs.at[ct], zr.at[cs], (d, r, ct)).start()

    def gather_wait(x):
        for cs in range(N):
            rows = x.at[span(cs)]

            @pl.when(c != cs)
            def _():
                pltpu.make_async_copy(rows, rows, zr.at[cs]).wait()

            @pl.when(c == cs)
            def _():
                for ct in range(N):
                    if ct != cs:
                        remote(rows, rows, zs.at[ct], zr.at[cs], (d, r, ct)).wait_send()

    def scatter_copy(ct):
        size = STEP if ct < N - 1 else CHUNK
        return remote(
            part.at[span(ct)], recv.at[c, pl.ds(0, size)], rss.at[ct], rsr.at[c], (d, r, ct)
        )

    def scatter_start():
        for ct in range(N):

            @pl.when(c != ct)
            def _():
                scatter_copy(ct).start()

            @pl.when(c == ct)
            def _():
                size = STEP if ct < N - 1 else CHUNK
                recv[ct, 0:size, :] = part[span(ct), :]

    def scatter_wait():
        for cs in range(N):
            for big in (False, True):
                size = CHUNK if big else STEP
                rows = recv.at[cs, pl.ds(0, size)]

                @pl.when(jnp.logical_and(c != cs, last if big else jnp.logical_not(last)))
                def _():
                    pltpu.make_async_copy(rows, rows, rsr.at[cs]).wait()

            @pl.when(c != cs)
            def _():
                scatter_copy(cs).wait_send()

    def received(rows):
        total = recv[0, rows, :].astype(F32)
        for cs in range(1, N):
            total = total + recv[cs, rows, :].astype(F32)
        return total

    def vector(row):
        return pv[pl.ds(row, 1), :]

    def own_rows(x, t, value):
        @pl.when(jnp.logical_or(t < 4, last))
        def _():
            x[pl.ds(pl.multiple_of(STEP * c + 16 * t, 16), 16), :] = value

    valid = jnp.where(last, SEQ - STEP * (N - 1), STEP)

    def masked(t, value):
        index = lax.broadcasted_iota(jnp.int32, (16, 1), 0) + 16 * t
        return jnp.where(index < valid, value, 0.0)

    def norm_forward(l, j, x, extra):
        def body(t, _):
            rows = pl.ds(pl.multiple_of(16 * t, 16), 16)
            v = extra(rows)
            st[rows, :] = v
            centre = jnp.sum(v, axis=1, keepdims=True) / D
            spread_ = jnp.sum(v * v, axis=1, keepdims=True) / D - centre * centre
            scale = lax.rsqrt(spread_ + EPSILON)
            standard = (v - centre) * scale
            std[l, j, rows, :] = standard
            inv[l, j, rows, :] = jnp.broadcast_to(scale, (16, 128))
            value = standard * vector(6 * l + j) + vector(6 * l + 2 + j)
            own_rows(x, t, value.astype(BF))
            return 0

        lax.fori_loop(0, CHUNK // 16, body, 0)

    def norm_backward(l, j, x, bias_row):
        def body(t, _):
            rows = pl.ds(pl.multiple_of(16 * t, 16), 16)
            e = received(rows)
            standard = std[l, j, rows, :]
            gain_term = masked(t, e * standard)
            vsum[pl.ds(6 * l + j, 1), :] += jnp.sum(gain_term, axis=0, keepdims=True)
            vsum[pl.ds(6 * l + 2 + j, 1), :] += jnp.sum(masked(t, e), axis=0, keepdims=True)
            f = e * vector(6 * l + j)
            first = jnp.sum(f, axis=1, keepdims=True) / D
            second = jnp.sum(f * standard, axis=1, keepdims=True) / D
            scale = inv[l, j, rows, 0:1]
            grad = gst[rows, :] + scale * (f - first - standard * second)
            gst[rows, :] = grad
            if x is not None:
                low = grad.astype(BF)
                own_rows(x, t, low)
                vsum[pl.ds(bias_row, 1), :] += jnp.sum(
                    masked(t, low.astype(F32)), axis=0, keepdims=True
                )
            return 0

        lax.fori_loop(0, CHUNK // 16, body, 0)

    def tiles(count, body):
        lax.fori_loop(0, count, lambda n, _: (body(n), 0)[1], 0)

    def features(body):
        tiles(5, lambda n: body(pl.multiple_of(n * 256, 256), 256))
        body(1280, 128)

    def assemble(src, dst):
        for k in range(N):
            dst[:, BLK * k : BLK * (k + 1)] = src[k, :, 0:BLK].astype(F32)

    for k in range(3):
        remote(vec_ref, pin.at[r], vs.at[k], vr.at[k], (d, near[k], c)).wait_recv()
    own_vec.wait()
    assemble(pin, pv)
    spread_wait(tok_hbm, tin, tokr)
    assemble(tin, st)

    lane = lax.broadcasted_iota(jnp.int32, (1, PAD), 1)
    key_ok = lax.broadcasted_iota(jnp.int32, (1, ROWS), 1) < SEQ
    scaling = HEAD_DIM**-0.5

    def head_mask(head):
        low, high, s0, s1 = head_span(head)
        lanes = lane[:, s0:s1]
        return jnp.logical_and(lanes >= low, lanes < high).astype(BF), s0, s1

    def attend(l):
        acc[0] = jnp.zeros((ROWS, PAD), F32)
        for head in range(4):
            mask, s0, s1 = head_mask(head)
            q = triple[l, 0, :, s0:s1] * mask
            scores = dot_t(q, triple[l, 1, :, s0:s1]) * scaling
            scores = jnp.where(key_ok, scores, -1e30)
            peak = jnp.max(scores, axis=1, keepdims=True)
            total = peak + jnp.log(jnp.sum(jnp.exp(scores - peak), axis=1, keepdims=True))
            lse[l, :, head : head + 1] = total
            probs = jnp.exp(scores - total).astype(BF)
            acc[0, :, s0:s1] += dot(probs, triple[l, 2, :, s0:s1] * mask)
        att[l] = acc[0].astype(BF)

    def forward(l, _):
        def take(rows):
            return st[rows, :]

        norm_forward(l, 0, x1.at[l], take)
        gather_start(x1.at[l])

        @pl.when(l == 0)
        def _():
            forward_w(0, 0)

        gather_wait(x1.at[l])
        need_w(l, 0)

        def qkv(s):
            lanes = pl.ds(pl.multiple_of(lax.rem(s, 2) * PAD, 128), PAD)
            value = dot(x1[l], w[l, s // 2, :, lanes]) + qb_ref[l, pl.ds(s, 1), :]
            triple[l, s] = value.astype(BF)

        tiles(3, qkv)
        attend(l)

        def proj(start, size):
            value = dot_t(att[l], w[l, 1, pl.ds(start, size), PAD : 2 * PAD])
            part[:, pl.ds(start, size)] = value.astype(BF)

        features(proj)
        scatter_start()
        forward_w(l, 1)
        scatter_wait()
        norm_forward(
            l, 1, x2.at[l], lambda rows: st[rows, :] + received(rows) + vector(6 * l + 4)
        )
        gather_start(x2.at[l])
        forward_w(l, 2)
        need_w(l, 1)
        gather_wait(x2.at[l])

        for h in range(2):

            def up(n):
                lanes = pl.ds(pl.multiple_of(n * 256, 256), 256)
                before = dot(x2[l], w[l, 2 + h, :, lanes]) + ub_ref[l, pl.ds(h, 1), lanes]
                half = before * (0.5**0.5)
                cdf = 0.5 + 0.5 * lax.erf(half)
                hid[l, h, :, lanes] = (before * cdf).astype(BF)
                density = jnp.exp(-half * half) * 0.3989422804014327
                slope[l, h, :, lanes] = (cdf + before * density).astype(slope.dtype)

            tiles(3, up)
        need_w(l, 2)

        def down(start, size):
            rows = pl.ds(start, size)
            value = dot_t(hid[l, 0], w[l, 4, rows, :]) + dot_t(hid[l, 1], w[l, 5, rows, :])
            part[:, pl.ds(start, size)] = value.astype(BF)

        features(down)
        scatter_start()

        @pl.when(l == 0)
        def _():
            forward_w(1, 0)

        scatter_wait()
        def settle(t, _):
            rows = pl.ds(pl.multiple_of(16 * t, 16), 16)
            st[rows, :] = st[rows, :] + received(rows) + vector(6 * l + 5)
            return 0

        lax.fori_loop(0, CHUNK // 16, settle, 0)
        return 0

    lax.fori_loop(0, LAYERS, forward, 0)

    def give(src, dst, ssem, rsem, start):
        for k in range(N):
            for cs in range(N):
                size = STEP if cs < N - 1 else CHUNK
                source, target = src.at[k, pl.ds(0, size)], dst.at[span(cs)]
                mine = jnp.logical_and(r == k, c == r)

                @pl.when(jnp.logical_and(c == cs, mine))
                def _():
                    if start:
                        pltpu.make_async_copy(source, target, rsem.at[cs]).start()

                @pl.when(jnp.logical_and(c == cs, jnp.logical_not(mine)))
                def _():
                    copy = remote(source, target, ssem.at[k], rsem.at[cs], (d, k, r))
                    if start:
                        copy.start()
                    else:
                        copy.wait_send()

    def give_wait(dst, rsem):
        for cs in range(N):
            rows = dst.at[span(cs)]
            pltpu.make_async_copy(rows, rows, rsem.at[cs]).wait()

    for k in range(N):
        oblk[k] = st[:, BLK * k : BLK * (k + 1)]
    give(oblk, out_hbm, outs, outr, True)

    spread_wait(cot_hbm, cin, cotr)
    assemble(cin, gst)

    def top_rows(t, _):
        rows = pl.ds(pl.multiple_of(16 * t, 16), 16)
        low = gst[rows, :].astype(BF)
        own_rows(gtop, t, low)
        vsum[pl.ds(6 * (LAYERS - 1) + 5, 1), :] += jnp.sum(
            masked(t, low.astype(F32)), axis=0, keepdims=True
        )
        return 0

    lax.fori_loop(0, CHUNK // 16, top_rows, 0)

    def transpose(src, index):
        def body(n):
            lanes = pl.ds(pl.multiple_of(n * 128, 128), 128)
            lt[index, lanes, :] = src[:, lanes].T

        tiles(D // 128, body)

    def piece(k):
        return remote(sbuf.at[k], prx.at[k], cs_s.at[k], cs_r.at[k], (other, r, c))

    def block_tile(i, b, k, left, right):
        rows = rblk(k)
        if i == 0:
            lanes = []
            for j in range(2):
                s = 2 * b + j
                lanes.append(dot(lt[left(s), rows, :], right(s)))
            return lanes
        return [dot(lt[left(b), rows, :], right(b))]

    def store_tile(ref, values):
        start = 0
        for value in values:
            ref[:, start : start + value.shape[1]] = value.astype(BF)
            start += value.shape[1]

    def pair(i, slot, left, right, wait_credit):
        if wait_credit is not None:

            @pl.when(wait_credit)
            def _():
                pl.semaphore_wait(credit, 1)

        def send_tile(k):
            store_tile(sbuf.at[k], block_tile(i, other, k, left, right))
            piece(k).start()

        tiles(N, send_tile)

        def keep_tile(k):
            store_tile(keep.at[slot, k], block_tile(i, d, k, left, right))

        tiles(N, keep_tile)

        def out_copy(k):
            return remote(
                keep.at[slot, near[k]], ici.at[i, k], gis.at[i, k], gir.at[i, k], (d, near[k], c)
            )

        def add(k):
            rows = prx.at[k]
            pltpu.make_async_copy(rows, rows, cs_r.at[k]).wait()
            keep[slot, k] = (keep[slot, k].astype(F32) + prx[k].astype(F32)).astype(BF)

        for k in range(3):
            add(near[k])
            out_copy(k).start()
        add(r)
        for k in range(N):
            piece(k).wait_send()
        pl.semaphore_signal(credit, inc=1, device_id=(other, r, c), device_id_type=MESH)

    def finish(l, i, slot):
        for k in range(3):
            arrived = ici.at[i, k]
            pltpu.make_async_copy(arrived, arrived, gir.at[i, k]).wait()

        def body(t, _):
            rows = pl.ds(pl.multiple_of(16 * t, 16), 16)
            total = keep[slot, r, rows, :].astype(F32)
            for k in range(3):
                total = total + ici[i, k, rows, :].astype(F32)
            fin[rows, :] = total
            return 0

        lax.fori_loop(0, BLK // 16, body, 0)
        target = g_hbm.at[2 * i + d]

        @pl.when(l == d)
        def _():
            copy = pltpu.make_async_copy(fin, target, fins.at[0])
            copy.start()
            copy.wait()

        @pl.when(l != d)
        def _():
            copy = remote(fin, target, fins.at[0], finr.at[i], (other, r, c))
            copy.start()
            copy.wait_send()

        for k in range(3):
            remote(
                keep.at[slot, near[k]], ici.at[i, k], gis.at[i, k], gir.at[i, k], (d, near[k], c)
            ).wait_send()

    def attend_back(l):
        for s in range(3):
            acc[s] = jnp.zeros((ROWS, PAD), F32)
        for head in range(4):
            mask, s0, s1 = head_mask(head)
            q = triple[l, 0, :, s0:s1] * mask
            keys = triple[l, 1, :, s0:s1]
            scores = dot_t(q, keys) * scaling
            scores = jnp.where(key_ok, scores, -1e30)
            probs = jnp.exp(scores - lse[l, :, head : head + 1])
            probs_low = probs.astype(BF)
            grad_heads = da[:, s0:s1] * mask
            acc[2, :, s0:s1] += t_dot(probs_low, grad_heads)
            grad_probs = dot_t(grad_heads, triple[l, 2, :, s0:s1])
            inner = jnp.sum(grad_probs * probs, axis=1, keepdims=True)
            grad_scores = (probs * (grad_probs - inner)).astype(BF)
            acc[0, :, s0:s1] += dot(grad_scores, keys * mask)
            acc[1, :, s0:s1] += t_dot(grad_scores, q)
        for s in range(3):
            value = acc[s] * scaling if s < 2 else acc[s]
            g3[s] = value.astype(BF)
        g3[3] = att[l]

    def backward(step, _):
        l = LAYERS - 1 - step
        gather_start(gtop)

        @pl.when(step > 0)
        def _():
            finish(l + 1, 0, 0)

        gather_wait(gtop)

        for h in range(2):

            def hidden(n):
                lanes = pl.ds(pl.multiple_of(n * 256, 256), 256)
                value = dot(gtop[...], w[l, 4 + h, :, lanes]) * slope[l, h, :, lanes].astype(F32)
                low = value.astype(BF)
                gb[h, :, lanes] = low
                csum[l, pl.ds(2 + h, 1), lanes] = jnp.sum(
                    low.astype(F32), axis=0, keepdims=True
                )

            tiles(3, hidden)

        def back_up(start, size):
            rows = pl.ds(start, size)
            value = dot_t(gb[0], w[l, 2, rows, :]) + dot_t(gb[1], w[l, 3, rows, :])
            part[:, pl.ds(start, size)] = value.astype(BF)

        features(back_up)
        scatter_start()
        transpose(gtop, 0)
        pair(2, 0, lambda b: 0, lambda b: hid[l, b], step > 0)
        scatter_wait()
        norm_backward(l, 1, gmid, 6 * l + 4)
        gather_start(gmid)
        transpose(x2.at[l], 1)
        pair(1, 1, lambda b: 1, lambda b: gb[b], step >= 0)
        gather_wait(gmid)
        da[...] = dot(gmid[...], w[l, 1, :, PAD : 2 * PAD]).astype(BF)
        attend_back(l)
        for s in range(3):
            row, start = (0, PAD * s) if s < 2 else (1, 0)
            csum[l, row : row + 1, start : start + PAD] = jnp.sum(
                g3[s].astype(F32), axis=0, keepdims=True
            )

        def back_qkv(start, size):
            rows = pl.ds(start, size)
            value = dot_t(g3[0], w[l, 0, rows, 0:PAD])
            value = value + dot_t(g3[1], w[l, 0, rows, PAD : 2 * PAD])
            value = value + dot_t(g3[2], w[l, 1, rows, 0:PAD])
            part[:, pl.ds(start, size)] = value.astype(BF)

        features(back_qkv)
        scatter_start()
        finish(l, 2, 0)
        finish(l, 1, 1)
        transpose(x1.at[l], 0)
        transpose(gmid, 1)
        pair(0, 0, lambda s: s // 3, lambda s: g3[s], step >= 0)
        scatter_wait()
        norm_backward(l, 0, gtop, jnp.where(l > 0, 6 * l - 1, 12))
        return 0

    lax.fori_loop(0, LAYERS, backward, 0)

    for k in range(N):
        tmp[k] = gst[:, BLK * k : BLK * (k + 1)]
    give(tmp, tg_hbm, tgs, tgr, True)
    finish(0, 0, 0)

    pl.semaphore_wait(credit, 1)
    give(oblk, out_hbm, outs, outr, False)
    give_wait(out_hbm, outr)
    give(tmp, tg_hbm, tgs, tgr, False)
    give_wait(tg_hbm, tgr)
    spread(tok_hbm, tin, toks, tokr, False)
    spread(cot_hbm, cin, cots, cotr, False)
    for i in range(3):
        arrived = g_hbm.at[2 * i + other]
        pltpu.make_async_copy(arrived, arrived, finr.at[i]).wait()
    for k in range(3):
        remote(vec_ref, pin.at[r], vs.at[k], vr.at[k], (d, near[k], c)).wait_send()
    for l in range(LAYERS):
        for i in range(3):
            for k in range(3):
                send_w(l, i, k).wait_send()
                share_w(l, i, k).wait_send()


def fused(tok, cot, wcat, vec, qb, ub):
    dma = pltpu.SemaphoreType.DMA
    vmem = pltpu.VMEM
    whole = pl.BlockSpec(memory_space=pltpu.VMEM)
    anywhere = pl.BlockSpec(memory_space=pl.ANY)
    scratch = [
        vmem((LAYERS, 6, D, HALF), BF),
        vmem((LAYERS, ROWS, D), BF),
        vmem((LAYERS, ROWS, D), BF),
        vmem((LAYERS, 3, ROWS, PAD), BF),
        vmem((LAYERS, ROWS, PAD), BF),
        vmem((LAYERS, ROWS, 128), F32),
        vmem((LAYERS, 2, ROWS, HALF), BF),
        vmem((LAYERS, 2, ROWS, HALF), BF),
        vmem((LAYERS, 2, CHUNK, D), F32),
        vmem((LAYERS, 2, CHUNK, 128), F32),
        vmem((ROWS, D), BF),
        vmem((ROWS, D), BF),
        vmem((2, D, ROWS), BF),
        vmem((ROWS, D), BF),
        vmem((N, CHUNK, D), BF),
        vmem((CHUNK, D), F32),
        vmem((CHUNK, D), F32),
        vmem((N, CHUNK, BLK), F32),
        vmem((N, CHUNK, BLK), BF),
        vmem((N, CHUNK, BLK), BF),
        vmem((N, CHUNK, BLK), F32),
        vmem((N, 16, BLK), F32),
        vmem((16, D), F32),
        vmem((2, ROWS, HALF), BF),
        vmem((ROWS, PAD), BF),
        vmem((4, ROWS, PAD), BF),
        vmem((3, ROWS, PAD), F32),
        vmem((N, BLK, HALF), BF),
        vmem((N, BLK, HALF), BF),
        vmem((2, N, BLK, HALF), BF),
        vmem((3, 3, BLK, HALF), BF),
        vmem((BLK, HALF), F32),
        dma((LAYERS, 6)),
        dma((LAYERS, 3, 3)), dma((LAYERS, 3, 3)),
        dma((LAYERS, 3, 3)), dma((LAYERS, 3, 3)),
        dma((3,)), dma((4,)),
        dma((N,)), dma((N,)), dma((N,)), dma((N,)),
        dma((N,)), dma((N,)), dma((N,)), dma((N,)),
        dma((N,)), dma((N,)), dma((N,)), dma((N,)),
        dma((N,)), dma((N,)), pltpu.SemaphoreType.REGULAR,
        dma((3, 3)), dma((3, 3)), dma((1,)), dma((3,)),
    ]
    shape = jax.ShapeDtypeStruct
    return pl.pallas_call(
        kernel,
        out_shape=(
            shape((ROWS, BLK), F32),
            shape((ROWS, BLK), F32),
            shape((6, BLK, HALF), F32),
            shape((16, D), F32),
            shape((LAYERS, 4, HALF), F32),
        ),
        in_specs=[anywhere, anywhere, anywhere, whole, whole, whole],
        out_specs=(anywhere, anywhere, anywhere, whole, whole),
        scratch_shapes=scratch,
        compiler_params=pltpu.CompilerParams(
            collective_id=0, has_side_effects=True, vmem_limit_bytes=67_043_328
        ),
    )(tok, cot, wcat, vec, qb, ub)


def widen(values, axis=-1, to=PAD):
    axis = axis % values.ndim
    pads = [(0, 0)] * values.ndim
    pads[axis] = (0, to - values.shape[axis])
    return jnp.pad(values, pads)


def per_device_fused(
    tokens, cotangent, qkv_weight, qv_bias, proj_weight, proj_bias,
    up_weight, up_bias, down_weight, down_bias, norm_gain, norm_shift,
):
    row, dp = lax.axis_index("row"), lax.axis_index("dp")
    tok = widen(tokens[0], 0, ROWS)
    cot = widen(cotangent[0], 0, ROWS)
    q, k, v = (widen(qkv_weight[:, :, s]) for s in range(3))
    proj = widen(proj_weight.transpose(0, 2, 1))
    down = down_weight.transpose(0, 2, 1)
    wcat = jnp.stack(
        [
            jnp.concatenate([q, k], 2),
            jnp.concatenate([v, proj], 2),
            up_weight[:, :, :HALF],
            up_weight[:, :, HALF:],
            down[:, :, :HALF],
            down[:, :, HALF:],
        ],
        axis=1,
    )
    vec = jnp.concatenate(
        [norm_gain, norm_shift, proj_bias[:, None], down_bias[:, None]], axis=1
    ).reshape(12, BLK)
    vec = widen(vec, 0, 16)
    zero = jnp.zeros_like(qv_bias[:, 0])
    qb = widen(jnp.stack([qv_bias[:, 0], zero, qv_bias[:, 1]], axis=1))
    ub = up_bias.reshape(LAYERS, 2, HALF)
    out, tg, grads, vsum, csum = fused(tok, cot, wcat, vec, qb, ub)
    vsum = lax.psum(vsum, ("dp", "row", "col"))
    csum = lax.psum(csum, ("dp", "row"))
    mine = lax.dynamic_slice(vsum[:12], (0, row * BLK), (12, BLK)).reshape(LAYERS, 6, BLK)
    layer = lax.dynamic_slice(mine, (dp, 0, 0), (1, 6, BLK))
    cols = lax.dynamic_slice(csum, (dp, 0, 0), (1, 4, HALF))
    qkv_grad = jnp.stack(
        [grads[0, :, :BLK], grads[0, :, PAD : PAD + BLK], grads[1, :, :BLK]], axis=1
    )
    return (
        out[None, :SEQ],
        tg[None, :SEQ],
        qkv_grad[None],
        jnp.stack([cols[:, 0, :BLK], cols[:, 1, :BLK]], axis=1),
        grads[1, :, PAD : PAD + BLK].T[None],
        layer[:, 4],
        jnp.concatenate([grads[2], grads[3]], axis=1)[None],
        cols[:, 2:].reshape(1, 2 * HALF),
        jnp.concatenate([grads[4].T, grads[5].T], axis=0)[None],
        layer[:, 5],
        mine[:, 0:2],
        mine[:, 2:4],
    )


NORMAL = (((1,), (0,)), ((), ()))
LAST_BOTH = (((1,), (1,)), ((), ()))
FIRST_BOTH = (((0,), (0,)), ((), ()))


def gather_tokens(values):
    return lax.all_gather(values, "col", axis=0, tiled=True)


def gather_blocks(values):
    return lax.all_gather(values, "row", axis=0, tiled=True)


def gather_grad_blocks(values):
    return lax.all_gather(values, "row", axis=0, tiled=True)


def width_totals(first_sum, second_sum):
    return lax.psum((first_sum, second_sum), "row")


def gather_whole(triple_w, up_w, proj_w, down_w):
    row_whole = (triple_w, up_w, proj_w, down_w)
    col_whole = (proj_w, down_w, triple_w, up_w)
    return (row_whole, col_whole)


def row_product(gathered, matrix, contract):
    return lax.psum_scatter(
        lax.dot_general(gathered, matrix, contract, preferred_element_type=jnp.float32).astype(
            jnp.bfloat16
        ),
        "row",
        scatter_dimension=0,
        tiled=True,
    ).astype(jnp.float32)


def col_product(gathered, matrix, contract):
    return lax.psum_scatter(
        lax.dot_general(gathered, matrix, contract, preferred_element_type=jnp.float32).astype(
            jnp.bfloat16
        ),
        "col",
        scatter_dimension=0,
        tiled=True,
    ).astype(jnp.float32)


def norm_forward(stream, factor, shift):
    totals, squares = width_totals(jnp.sum(stream, axis=1), jnp.sum(stream * stream, axis=1))
    centre = totals / D
    spread = squares / D - centre * centre
    centred = stream - centre[:, None]
    scaling = lax.rsqrt(spread + EPSILON)
    standard = centred * scaling[:, None]
    return (standard * factor + shift, standard, scaling)


def norm_backward(grad_norm, standard, scaling, factor):
    factor_grad = jnp.sum(grad_norm * standard, axis=0)
    shift_grad = jnp.sum(grad_norm, axis=0)
    grad_standard = grad_norm * factor
    first_sum, second_sum = width_totals(
        jnp.sum(grad_standard, axis=1), jnp.sum(grad_standard * standard, axis=1)
    )
    grad_stream = scaling[:, None] * (
        grad_standard - first_sum[:, None] / D - standard * (second_sum[:, None] / D)
    )
    return (grad_stream, factor_grad, shift_grad)


def split_triple(triple_out, width):
    images = triple_out.shape[0] // SEQ
    head_count = width // HEAD_DIM
    pieces = triple_out.reshape(images, SEQ, 3, head_count, HEAD_DIM)
    return (pieces[:, :, 0], pieces[:, :, 1], pieces[:, :, 2])


def attend_forward(triple_out, width):
    queries, key_rows, values = split_triple(triple_out, width)
    scaling = HEAD_DIM ** (-0.5)
    scores = (
        jnp.einsum("bqhd,bkhd->bhqk", queries, key_rows, preferred_element_type=jnp.float32)
        * scaling
    )
    row_peak = jnp.max(scores, axis=-1, keepdims=True)
    log_totals = row_peak + jnp.log(jnp.sum(jnp.exp(scores - row_peak), axis=-1, keepdims=True))
    probs_low = jnp.exp(scores - log_totals).astype(jnp.bfloat16)
    attended = jnp.einsum("bhqk,bkhd->bqhd", probs_low, values, preferred_element_type=jnp.float32)
    return (attended.reshape(triple_out.shape[0], width).astype(jnp.bfloat16), log_totals)


def attend_backward(triple_out, log_totals, grad_attended, width):
    queries, key_rows, values = split_triple(triple_out, width)
    scaling = HEAD_DIM ** (-0.5)
    scores = (
        jnp.einsum("bqhd,bkhd->bhqk", queries, key_rows, preferred_element_type=jnp.float32)
        * scaling
    )
    probs = jnp.exp(scores - log_totals)
    probs_low = probs.astype(jnp.bfloat16)
    grad_heads = grad_attended.reshape(values.shape)
    grad_values = jnp.einsum(
        "bhqk,bqhd->bkhd", probs_low, grad_heads, preferred_element_type=jnp.float32
    )
    grad_probs = jnp.einsum(
        "bqhd,bkhd->bhqk", grad_heads, values, preferred_element_type=jnp.float32
    )
    grad_scores = (
        probs * (grad_probs - jnp.sum(grad_probs * probs, axis=-1, keepdims=True))
    ).astype(jnp.bfloat16)
    grad_queries = (
        jnp.einsum("bhqk,bkhd->bqhd", grad_scores, key_rows, preferred_element_type=jnp.float32)
        * scaling
    )
    grad_keys = (
        jnp.einsum("bhqk,bqhd->bkhd", grad_scores, queries, preferred_element_type=jnp.float32)
        * scaling
    )
    stacked = jnp.stack([grad_queries, grad_keys, grad_values], axis=2)
    return stacked.reshape(triple_out.shape[0], 3 * width).astype(jnp.bfloat16)


def layer_forward(stream, weights):
    qkv_w, qv_b, proj_w, proj_b, up_w, up_b, down_w, down_b, factors, shifts = weights
    width = qkv_w.shape[2]
    triple_w = qkv_w.reshape(qkv_w.shape[0], 3 * width)
    row_whole, col_whole = gather_whole(triple_w, up_w, proj_w, down_w)
    first_norm, first_standard, first_scaling = norm_forward(stream, factors[0], shifts[0])
    first_rows = gather_tokens(first_norm.astype(jnp.bfloat16))
    offsets = jnp.concatenate([qv_b[0], jnp.zeros_like(qv_b[0]), qv_b[1]])
    triple_out = (row_product(first_rows, triple_w, NORMAL) + offsets).astype(jnp.bfloat16)
    attended, log_totals = attend_forward(triple_out, width)
    head_rows = gather_blocks(attended)
    stream_mid = stream + col_product(head_rows, proj_w, NORMAL) + proj_b
    second_norm, second_standard, second_scaling = norm_forward(stream_mid, factors[1], shifts[1])
    second_rows = gather_tokens(second_norm.astype(jnp.bfloat16))
    before = row_product(second_rows, up_w, NORMAL) + up_b
    activated = jax.nn.gelu(before, approximate=False).astype(jnp.bfloat16)
    hidden_rows = gather_blocks(activated)
    branch_out = col_product(hidden_rows, down_w, NORMAL)
    stream_out = stream_mid + branch_out + down_b
    saved = (
        first_rows,
        first_standard,
        first_scaling,
        triple_out,
        log_totals,
        head_rows,
        second_rows,
        second_standard,
        second_scaling,
        before,
        hidden_rows,
        row_whole,
        col_whole,
    )
    return (stream_out, saved)


def layer_backward(grad_out, saved, weights):
    qkv_w, qv_b, proj_w, proj_b, up_w, up_b, down_w, down_b, factors, shifts = weights
    (
        first_rows,
        first_standard,
        first_scaling,
        triple_out,
        log_totals,
        head_rows,
        second_rows,
        second_standard,
        second_scaling,
        before,
        hidden_rows,
        row_whole,
        col_whole,
    ) = saved
    width = qkv_w.shape[2]
    triple_w = qkv_w.reshape(qkv_w.shape[0], 3 * width)
    grad_rows = gather_tokens(grad_out.astype(jnp.bfloat16))
    down_grad = lax.dot_general(
        hidden_rows, grad_rows, FIRST_BOTH, preferred_element_type=jnp.float32
    )
    down_off_grad = jnp.sum(grad_rows, axis=0, dtype=jnp.float32)
    grad_active = row_product(grad_rows, down_w, LAST_BOTH)
    _, slope_pull = jax.vjp(partial(jax.nn.gelu, approximate=False), before)
    grad_before = slope_pull(grad_active)[0].astype(jnp.bfloat16)
    before_rows = gather_grad_blocks(grad_before)
    up_grad = lax.dot_general(
        second_rows, before_rows, FIRST_BOTH, preferred_element_type=jnp.float32
    )
    up_off_grad = jnp.sum(before_rows, axis=0, dtype=jnp.float32)
    grad_second = col_product(before_rows, up_w, LAST_BOTH)
    grad_mid, second_factor_grad, second_shift_grad = norm_backward(
        grad_second, second_standard, second_scaling, factors[1]
    )
    grad_mid = grad_mid + grad_out
    mid_rows = gather_tokens(grad_mid.astype(jnp.bfloat16))
    proj_grad = lax.dot_general(head_rows, mid_rows, FIRST_BOTH, preferred_element_type=jnp.float32)
    proj_off_grad = jnp.sum(mid_rows, axis=0, dtype=jnp.float32)
    grad_attended = row_product(mid_rows, proj_w, LAST_BOTH).astype(jnp.bfloat16)
    grad_triple = attend_backward(triple_out, log_totals, grad_attended, width)
    triple_rows = gather_grad_blocks(grad_triple)
    triple_grad = lax.dot_general(
        first_rows, triple_rows, FIRST_BOTH, preferred_element_type=jnp.float32
    )
    column_sums = jnp.sum(triple_rows, axis=0, dtype=jnp.float32).reshape(3, width)
    qv_grad = jnp.stack([column_sums[0], column_sums[2]])
    grad_first = col_product(triple_rows, triple_w, LAST_BOTH)
    grad_in, first_factor_grad, first_shift_grad = norm_backward(
        grad_first, first_standard, first_scaling, factors[0]
    )
    grad_in = grad_in + grad_mid
    factor_grads = jnp.stack([first_factor_grad, second_factor_grad])
    shift_grads = jnp.stack([first_shift_grad, second_shift_grad])
    layer_grads = (
        triple_grad.reshape(qkv_w.shape),
        qv_grad,
        proj_grad,
        proj_off_grad,
        up_grad,
        up_off_grad,
        down_grad,
        down_off_grad,
        factor_grads,
        shift_grads,
    )
    return (grad_in, layer_grads)


def per_device_plain(
    tokens,
    cotangent,
    qkv_weight,
    qv_bias,
    proj_weight,
    proj_bias,
    up_weight,
    up_bias,
    down_weight,
    down_bias,
    norm_gain,
    norm_shift,
):
    image_count, seq_len, width_row = tokens.shape
    stream = tokens.reshape(image_count * seq_len, width_row).astype(jnp.float32)
    layer_params = []
    saved_list = []
    for layer_index in range(LAYERS):
        params = (
            qkv_weight[layer_index],
            qv_bias[layer_index],
            proj_weight[layer_index],
            proj_bias[layer_index],
            up_weight[layer_index],
            up_bias[layer_index],
            down_weight[layer_index],
            down_bias[layer_index],
            norm_gain[layer_index],
            norm_shift[layer_index],
        )
        layer_params.append(params)
        stream, saved = layer_forward(stream, params)
        saved_list.append(saved)
    grad_stream = cotangent.reshape(image_count * seq_len, width_row).astype(jnp.float32)
    per_layer = [None] * LAYERS
    for layer_index in reversed(range(LAYERS)):
        grad_stream, layer_grads = layer_backward(
            grad_stream, saved_list[layer_index], layer_params[layer_index]
        )
        per_layer[layer_index] = layer_grads
    stacked = tuple(
        (jnp.stack([layer_grads[position] for layer_grads in per_layer]) for position in range(10))
    )
    summed = (
        lax.psum_scatter(
            stacked[0].astype(jnp.bfloat16), "dp", scatter_dimension=0, tiled=True
        ).astype(jnp.float32),
        lax.psum_scatter(
            stacked[1].astype(jnp.bfloat16), "dp", scatter_dimension=0, tiled=True
        ).astype(jnp.float32),
        lax.psum_scatter(
            stacked[2].astype(jnp.bfloat16), "dp", scatter_dimension=0, tiled=True
        ).astype(jnp.float32),
        lax.psum_scatter(
            stacked[3].astype(jnp.bfloat16), "dp", scatter_dimension=0, tiled=True
        ).astype(jnp.float32),
        lax.psum_scatter(
            stacked[4].astype(jnp.bfloat16), "dp", scatter_dimension=0, tiled=True
        ).astype(jnp.float32),
        lax.psum_scatter(
            stacked[5].astype(jnp.bfloat16), "dp", scatter_dimension=0, tiled=True
        ).astype(jnp.float32),
        lax.psum_scatter(
            stacked[6].astype(jnp.bfloat16), "dp", scatter_dimension=0, tiled=True
        ).astype(jnp.float32),
        lax.psum_scatter(
            stacked[7].astype(jnp.bfloat16), "dp", scatter_dimension=0, tiled=True
        ).astype(jnp.float32),
    )
    norm_sums = lax.psum((stacked[8], stacked[9]), ("dp", "col"))
    result = stream.reshape(image_count, seq_len, width_row)
    tokens_grad = grad_stream.reshape(image_count, seq_len, width_row)
    return (
        result,
        tokens_grad,
        summed[0],
        summed[1],
        summed[2],
        summed[3],
        summed[4],
        summed[5],
        summed[6],
        summed[7],
        norm_sums[0],
        norm_sums[1],
    )


def solution(mesh):
    placed = (
        P(("dp", "col"), None, "row"),
        P(("dp", "col"), None, "row"),
        P(None, "row", None, "col"),
        P(None, None, "col"),
        P(None, "col", "row"),
        P(None, "row"),
        P(None, "row", "col"),
        P(None, "col"),
        P(None, "col", "row"),
        P(None, "row"),
        P(None, None, "row"),
        P(None, None, "row"),
    )
    sizes = (mesh.shape["dp"], mesh.shape["row"], mesh.shape["col"])
    return jax.shard_map(
        per_device_fused if sizes == (2, N, N) else per_device_plain,
        mesh=mesh,
        in_specs=placed,
        out_specs=(
            P(("dp", "col"), None, "row"),
            P(("dp", "col"), None, "row"),
            P("dp", "row", None, "col"),
            P("dp", None, "col"),
            P("dp", "col", "row"),
            P("dp", "row"),
            P("dp", "row", "col"),
            P("dp", "col"),
            P("dp", "col", "row"),
            P("dp", "row"),
            P(None, None, "row"),
            P(None, None, "row"),
        ),
        check_vma=False,
    )
```

```python
from functools import partial

import jax
import jax.numpy as jnp
from jax import lax
from jax.experimental import pallas as pl
from jax.experimental.pallas import tpu as pltpu
from jax.sharding import PartitionSpec as P

D = 1408
HEAD_DIM = 88
SEQ = 257
LAYERS = 2
EPSILON = 1e-06
MESH = pl.DeviceIdType.MESH
BF = jnp.bfloat16
F32 = jnp.float32

ROWS = 272
STEP = 64
CHUNK = 80
BLK = 352
PAD = 384
HALF = 768
N = 4


def dot(a, b):
    return jnp.dot(a, b, preferred_element_type=F32)


def dot_t(a, b):
    return lax.dot_general(a, b, (((1,), (1,)), ((), ())), preferred_element_type=F32)


def t_dot(a, b):
    return lax.dot_general(a, b, (((0,), (0,)), ((), ())), preferred_element_type=F32)


def span(index):
    return pl.ds(STEP * index, STEP if index < N - 1 else CHUNK)


def head_span(head):
    low, high = HEAD_DIM * head, HEAD_DIM * (head + 1)
    return low, high, low // 128 * 128, -(-high // 128) * 128


def kernel(
    tok_hbm, cot_hbm, wa_hbm, up_hbm, down_hbm, vec_ref, qb_ref, ub_ref,
    out_hbm, tg_hbm, ga_hbm, gu_hbm, gd_hbm, vout, cout,
    wa, wm, x1, x2, triple, att, lse, hid, slope, std, inv,
    gtop, gmid, lt, part, recv, st, gst, tin, cin, oblk, pin, pv,
    gb, da, g3, acc, sbuf, prx, keep, ici, fin, part2, recv2,
    vsum, csum, vb, vx, vz, vd, cx, cd,
    wloc, wsend, wrecv, psend, precv, vs, vr, toks, tokr, cots, cotr,
    zs, zr, rss, rsr, outs, outr, tgs, tgr, cs_s, cs_r, credit, gis, gir, fins, finr,
    zs2, zr2, rss2, rsr2, vxs, vxr, vzs, vzr, vds, cxs, cxr, cds,
):
    d, r, c = lax.axis_index("dp"), lax.axis_index("row"), lax.axis_index("col")
    other = 1 - d
    near = (r + 1 - 2 * lax.rem(r, 2), lax.rem(r + 2, N), N - 1 - r)
    last = c == N - 1

    def remote(src, dst, ssem, rsem, dev):
        return pltpu.make_async_remote_copy(
            src, dst, ssem, rsem, device_id=dev, device_id_type=MESH
        )

    def rblk(index):
        return pl.ds(pl.multiple_of(index * BLK, 16), BLK)

    recv[...] = jnp.zeros_like(recv)
    recv2[...] = jnp.zeros_like(recv2)
    tin[...] = jnp.zeros_like(tin)
    cin[...] = jnp.zeros_like(cin)
    vsum[...] = jnp.zeros_like(vsum)
    csum[...] = jnp.zeros_like(csum)
    barrier = pltpu.get_barrier_semaphore()
    for k in range(N * N):
        pl.semaphore_signal(
            barrier, inc=1,
            device_id=(d, lax.rem(r + k // N, N), lax.rem(c + k % N, N)), device_id_type=MESH,
        )
    pl.semaphore_signal(barrier, inc=1, device_id=(other, r, c), device_id_type=MESH)
    pl.semaphore_wait(barrier, N * N + 1)

    for k in range(3):
        remote(vec_ref, pin.at[r], vs.at[k], vr.at[k], (d, near[k], c)).start()
    own_vec = pltpu.make_async_copy(vec_ref, pin.at[r], vr.at[3])
    own_vec.start()

    def spread(src, dst, ssem, rsem, start):
        for ct in range(N):
            mine = jnp.logical_and(r == c, c == ct)
            size = STEP if ct < N - 1 else CHUNK
            source, target = src.at[span(ct)], dst.at[r, pl.ds(0, size)]

            @pl.when(mine)
            def _():
                if start:
                    pltpu.make_async_copy(source, target, rsem.at[r]).start()

            @pl.when(jnp.logical_not(mine))
            def _():
                copy = remote(source, target, ssem.at[ct], rsem.at[r], (d, c, ct))
                if start:
                    copy.start()
                else:
                    copy.wait_send()

    def spread_wait(src, dst, rsem):
        def at_size(ct):
            size = STEP if ct < N - 1 else CHUNK
            for rs in range(N):
                pltpu.make_async_copy(
                    src.at[span(ct)], dst.at[rs, pl.ds(0, size)], rsem.at[rs]
                ).wait()

        @pl.when(last)
        def _():
            at_size(N - 1)

        @pl.when(jnp.logical_not(last))
        def _():
            at_size(0)

    spread(tok_hbm, tin, toks, tokr, True)

    def source_w(l, i, which):
        if i == 0:
            return wa_hbm.at[l, pl.ds(2 * which, 2)]
        lanes = pl.ds(pl.multiple_of(HALF * which, 128), HALF)
        return (up_hbm if i == 1 else down_hbm).at[l, :, lanes]

    def rows_w(l, i, which, block):
        if i == 0:
            return wa.at[l, pl.ds(2 * which, 2), rblk(block), :]
        return wm.at[l, 2 * (i - 1) + which, rblk(block), :]

    def local_w(l, i, which):
        return pltpu.make_async_copy(
            source_w(l, i, which), rows_w(l, i, which, r), wloc.at[l, i, which]
        )

    def send_w(l, i, k):
        return remote(
            source_w(l, i, d), rows_w(l, i, d, r), wsend.at[l, i, k], wrecv.at[l, i, k],
            (d, near[k], c),
        )

    def share_w(l, i, k):
        rows = rows_w(l, i, d, near[k])
        return remote(rows, rows, psend.at[l, i, k], precv.at[l, i, k], (other, r, c))

    for l in range(LAYERS):
        for i in range(3):
            for k in range(3):
                send_w(l, i, k).start()
            for which in range(2):
                local_w(l, i, which).start()
            if l == 0 and i == 0:
                spread(cot_hbm, cin, cots, cotr, True)

    def forward_w(l, i):
        for k in range(3):
            send_w(l, i, k).wait_recv()
            share_w(l, i, k).start()

    def need_w(l, i):
        for which in range(2):
            local_w(l, i, which).wait()
        for k in range(3):
            rows = rows_w(l, i, other, near[k])
            pltpu.make_async_copy(rows, rows, precv.at[l, i, k]).wait()

    def gather_start(x, zs=zs, zr=zr):
        for cs in range(N):

            @pl.when(c == cs)
            def _():
                for ct in range(N):
                    if ct != cs:
                        rows = x.at[span(cs)]
                        remote(rows, rows, zs.at[ct], zr.at[cs], (d, r, ct)).start()

    def gather_wait(x, zs=zs, zr=zr):
        for cs in range(N):
            rows = x.at[span(cs)]

            @pl.when(c != cs)
            def _():
                pltpu.make_async_copy(rows, rows, zr.at[cs]).wait()

            @pl.when(c == cs)
            def _():
                for ct in range(N):
                    if ct != cs:
                        remote(rows, rows, zs.at[ct], zr.at[cs], (d, r, ct)).wait_send()

    def scatter_copy(ct, part, recv, rss, rsr):
        size = STEP if ct < N - 1 else CHUNK
        return remote(
            part.at[span(ct)], recv.at[c, pl.ds(0, size)], rss.at[ct], rsr.at[c], (d, r, ct)
        )

    main = (part, recv, rss, rsr)
    side = (part2, recv2, rss2, rsr2)

    def scatter_start(path=main):
        for ct in range(N):

            @pl.when(c != ct)
            def _():
                scatter_copy(ct, *path).start()

            @pl.when(c == ct)
            def _():
                size = STEP if ct < N - 1 else CHUNK
                path[1][ct, 0:size, :] = path[0][span(ct), :]

    def scatter_wait(path=main):
        for cs in range(N):
            for big in (False, True):
                size = CHUNK if big else STEP
                rows = path[1].at[cs, pl.ds(0, size)]

                @pl.when(jnp.logical_and(c != cs, last if big else jnp.logical_not(last)))
                def _():
                    pltpu.make_async_copy(rows, rows, path[3].at[cs]).wait()

            @pl.when(c != cs)
            def _():
                scatter_copy(cs, *path).wait_send()

    def received(rows, recv=recv):
        total = recv[0, rows, :].astype(F32)
        for cs in range(1, N):
            total = total + recv[cs, rows, :].astype(F32)
        return total

    def vector(row):
        return pv[pl.ds(row, 1), :]

    def own_rows(x, t, value):
        @pl.when(jnp.logical_or(t < 4, last))
        def _():
            x[pl.ds(pl.multiple_of(STEP * c + 16 * t, 16), 16), :] = value

    valid = jnp.where(last, SEQ - STEP * (N - 1), STEP)

    def masked(t, value):
        index = lax.broadcasted_iota(jnp.int32, (16, 1), 0) + 16 * t
        return jnp.where(index < valid, value, 0.0)

    def norm_forward(l, j, x, extra):
        def body(t, _):
            rows = pl.ds(pl.multiple_of(16 * t, 16), 16)
            v = extra(rows)
            st[rows, :] = v
            centre = jnp.sum(v, axis=1, keepdims=True) / D
            spread_ = jnp.sum(v * v, axis=1, keepdims=True) / D - centre * centre
            scale = lax.rsqrt(spread_ + EPSILON)
            standard = (v - centre) * scale
            std[l, j, rows, :] = standard
            inv[l, j, rows, :] = jnp.broadcast_to(scale, (16, 128))
            value = standard * vector(6 * l + j) + vector(6 * l + 2 + j)
            own_rows(x, t, value.astype(BF))
            return 0

        lax.fori_loop(0, CHUNK // 16, body, 0)

    def norm_backward(l, j, x, bias_row):
        def body(t, _):
            rows = pl.ds(pl.multiple_of(16 * t, 16), 16)
            e = received(rows)
            standard = std[l, j, rows, :]
            gain_term = masked(t, e * standard)
            vsum[pl.ds(6 * l + j, 1), :] += jnp.sum(gain_term, axis=0, keepdims=True)
            vsum[pl.ds(6 * l + 2 + j, 1), :] += jnp.sum(masked(t, e), axis=0, keepdims=True)
            f = e * vector(6 * l + j)
            first = jnp.sum(f, axis=1, keepdims=True) / D
            second = jnp.sum(f * standard, axis=1, keepdims=True) / D
            scale = inv[l, j, rows, 0:1]
            grad = gst[rows, :] + scale * (f - first - standard * second)
            gst[rows, :] = grad
            if x is not None:
                low = grad.astype(BF)
                own_rows(x, t, low)
                vsum[pl.ds(bias_row, 1), :] += jnp.sum(
                    masked(t, low.astype(F32)), axis=0, keepdims=True
                )
            return 0

        lax.fori_loop(0, CHUNK // 16, body, 0)

    def tiles(count, body):
        lax.fori_loop(0, count, lambda n, _: (body(n), 0)[1], 0)

    def features(body):
        tiles(5, lambda n: body(pl.multiple_of(n * 256, 256), 256))
        body(1280, 128)

    def assemble(src, dst):
        for k in range(N):
            dst[:, BLK * k : BLK * (k + 1)] = src[k, :, 0:BLK].astype(F32)

    for k in range(3):
        remote(vec_ref, pin.at[r], vs.at[k], vr.at[k], (d, near[k], c)).wait_recv()
    own_vec.wait()
    assemble(pin, pv)
    spread_wait(tok_hbm, tin, tokr)
    assemble(tin, st)

    lane = lax.broadcasted_iota(jnp.int32, (1, PAD), 1)
    key_ok = lax.broadcasted_iota(jnp.int32, (1, ROWS), 1) < SEQ
    scaling = HEAD_DIM**-0.5

    def head_mask(head):
        low, high, s0, s1 = head_span(head)
        lanes = lane[:, s0:s1]
        return jnp.logical_and(lanes >= low, lanes < high).astype(BF), s0, s1

    def attend(l):
        acc[0] = jnp.zeros((ROWS, PAD), F32)
        for head in range(4):
            mask, s0, s1 = head_mask(head)
            q = triple[l, 0, :, s0:s1] * mask
            scores = dot_t(q, triple[l, 1, :, s0:s1]) * scaling
            scores = jnp.where(key_ok, scores, -1e30)
            peak = jnp.max(scores, axis=1, keepdims=True)
            total = peak + jnp.log(jnp.sum(jnp.exp(scores - peak), axis=1, keepdims=True))
            lse[l, :, head : head + 1] = total
            probs = jnp.exp(scores - total).astype(BF)
            acc[0, :, s0:s1] += dot(probs, triple[l, 2, :, s0:s1] * mask)
        att[l] = acc[0].astype(BF)

    def down(l, target):
        def body(start, size):
            rows = pl.ds(start, size)
            value = dot_t(hid[l, 0], wm[l, 2, rows, :]) + dot_t(hid[l, 1], wm[l, 3, rows, :])
            target[:, rows] = value.astype(BF)

        return body

    def settle(l, recv):
        def body(t, _):
            rows = pl.ds(pl.multiple_of(16 * t, 16), 16)
            st[rows, :] = st[rows, :] + received(rows, recv) + vector(6 * l + 5)
            return 0

        return body

    def top_rows(t, _):
        rows = pl.ds(pl.multiple_of(16 * t, 16), 16)
        low = gst[rows, :].astype(BF)
        own_rows(gtop, t, low)
        vsum[pl.ds(6 * (LAYERS - 1) + 5, 1), :] += jnp.sum(
            masked(t, low.astype(F32)), axis=0, keepdims=True
        )
        return 0

    def forward(l, _):
        def take(rows):
            return st[rows, :]

        norm_forward(l, 0, x1.at[l], take)
        gather_start(x1.at[l])

        @pl.when(l == 0)
        def _():
            forward_w(0, 0)

        gather_wait(x1.at[l])

        @pl.when(l == 0)
        def _():
            spread_wait(cot_hbm, cin, cotr)
            assemble(cin, gst)
            lax.fori_loop(0, CHUNK // 16, top_rows, 0)
            gather_start(gtop, zs2, zr2)

        need_w(l, 0)

        def qkv(s):
            value = dot(x1[l], wa[l, s]) + qb_ref[l, pl.ds(s, 1), :]
            triple[l, s] = value.astype(BF)

        tiles(3, qkv)
        attend(l)

        def proj(start, size):
            value = dot_t(att[l], wa[l, 3, pl.ds(start, size), :])
            part[:, pl.ds(start, size)] = value.astype(BF)

        features(proj)
        scatter_start()
        forward_w(l, 1)
        scatter_wait()
        norm_forward(
            l, 1, x2.at[l], lambda rows: st[rows, :] + received(rows) + vector(6 * l + 4)
        )
        gather_start(x2.at[l])
        forward_w(l, 2)
        need_w(l, 1)
        gather_wait(x2.at[l])

        for h in range(2):

            def up(n):
                lanes = pl.ds(pl.multiple_of(n * 256, 256), 256)
                before = dot(x2[l], wm[l, h, :, lanes]) + ub_ref[l, pl.ds(h, 1), lanes]
                half = before * (0.5**0.5)
                cdf = 0.5 + 0.5 * lax.erf(half)
                hid[l, h, :, lanes] = (before * cdf).astype(BF)
                density = jnp.exp(-half * half) * 0.3989422804014327
                slope[l, h, :, lanes] = (cdf + before * density).astype(slope.dtype)

            tiles(3, up)
        need_w(l, 2)

        @pl.when(l == 0)
        def _():
            features(down(l, part))
            scatter_start()
            forward_w(1, 0)
            scatter_wait()
            lax.fori_loop(0, CHUNK // 16, settle(l, recv), 0)

        return 0

    lax.fori_loop(0, LAYERS, forward, 0)

    def give(src, dst, ssem, rsem, start):
        for k in range(N):
            for cs in range(N):
                size = STEP if cs < N - 1 else CHUNK
                source, target = src.at[k, pl.ds(0, size)], dst.at[span(cs)]
                mine = jnp.logical_and(r == k, c == r)

                @pl.when(jnp.logical_and(c == cs, mine))
                def _():
                    if start:
                        pltpu.make_async_copy(source, target, rsem.at[cs]).start()

                @pl.when(jnp.logical_and(c == cs, jnp.logical_not(mine)))
                def _():
                    copy = remote(source, target, ssem.at[k], rsem.at[cs], (d, k, r))
                    if start:
                        copy.start()
                    else:
                        copy.wait_send()

    def give_wait(dst, rsem):
        for cs in range(N):
            rows = dst.at[span(cs)]
            pltpu.make_async_copy(rows, rows, rsem.at[cs]).wait()

    def transpose(src, index):
        def body(n):
            lanes = pl.ds(pl.multiple_of(n * 128, 128), 128)
            lt[index, lanes, :] = src[:, lanes].T

        tiles(D // 128, body)

    def piece(k):
        return remote(sbuf.at[k], prx.at[k], cs_s.at[k], cs_r.at[k], (other, r, c))

    def block_tile(i, b, k, left, right):
        rows = rblk(k)
        if i == 0:
            lanes = []
            for j in range(2):
                s = 2 * b + j
                lanes.append(dot(lt[left(s), rows, :], right(s)))
            return lanes
        return [dot(lt[left(b), rows, :], right(b))]

    def store_tile(ref, values):
        start = 0
        for value in values:
            ref[:, start : start + value.shape[1]] = value.astype(BF)
            start += value.shape[1]

    def pair(i, slot, left, right, wait_credit):
        if wait_credit is not None:

            @pl.when(wait_credit)
            def _():
                pl.semaphore_wait(credit, 1)

        def send_tile(k):
            store_tile(sbuf.at[k], block_tile(i, other, k, left, right))
            piece(k).start()

        tiles(N, send_tile)

        def keep_tile(k):
            store_tile(keep.at[slot, k], block_tile(i, d, k, left, right))

        tiles(N, keep_tile)

        def out_copy(k):
            return remote(
                keep.at[slot, near[k]], ici.at[i, k], gis.at[i, k], gir.at[i, k], (d, near[k], c)
            )

        def add(k):
            rows = prx.at[k]
            pltpu.make_async_copy(rows, rows, cs_r.at[k]).wait()
            keep[slot, k] = (keep[slot, k].astype(F32) + prx[k].astype(F32)).astype(BF)

        for k in range(3):
            add(near[k])
            out_copy(k).start()
        add(r)
        for k in range(N):
            piece(k).wait_send()
        pl.semaphore_signal(credit, inc=1, device_id=(other, r, c), device_id_type=MESH)

    def result(i, which, j):
        if i == 0:
            return ga_hbm.at[2 * which + j]
        lanes = pl.ds(pl.multiple_of(HALF * which + PAD * j, 128), PAD)
        return (gu_hbm if i == 1 else gd_hbm).at[:, lanes]

    def finish(l, i, slot):
        for k in range(3):
            arrived = ici.at[i, k]
            pltpu.make_async_copy(arrived, arrived, gir.at[i, k]).wait()

        def body(t, _):
            rows = pl.ds(pl.multiple_of(16 * t, 16), 16)
            total = keep[slot, r, rows, :].astype(F32)
            for k in range(3):
                total = total + ici[i, k, rows, :].astype(F32)
            fin[0, rows, :] = total[:, 0:PAD]
            fin[1, rows, :] = total[:, PAD : 2 * PAD]
            return 0

        lax.fori_loop(0, BLK // 16, body, 0)

        @pl.when(l == d)
        def _():
            copies = [
                pltpu.make_async_copy(fin.at[j], result(i, d, j), fins.at[j]) for j in range(2)
            ]
            for copy in copies:
                copy.start()
            for copy in copies:
                copy.wait()

        @pl.when(l != d)
        def _():
            copies = [
                remote(fin.at[j], result(i, d, j), fins.at[j], finr.at[i, j], (other, r, c))
                for j in range(2)
            ]
            for copy in copies:
                copy.start()
            for copy in copies:
                copy.wait_send()

        for k in range(3):
            remote(
                keep.at[slot, near[k]], ici.at[i, k], gis.at[i, k], gir.at[i, k], (d, near[k], c)
            ).wait_send()

    def attend_back(l):
        for s in range(3):
            acc[s] = jnp.zeros((ROWS, PAD), F32)
        for head in range(4):
            mask, s0, s1 = head_mask(head)
            q = triple[l, 0, :, s0:s1] * mask
            keys = triple[l, 1, :, s0:s1]
            scores = dot_t(q, keys) * scaling
            scores = jnp.where(key_ok, scores, -1e30)
            probs = jnp.exp(scores - lse[l, :, head : head + 1])
            probs_low = probs.astype(BF)
            grad_heads = da[:, s0:s1] * mask
            acc[2, :, s0:s1] += t_dot(probs_low, grad_heads)
            grad_probs = dot_t(grad_heads, triple[l, 2, :, s0:s1])
            inner = jnp.sum(grad_probs * probs, axis=1, keepdims=True)
            grad_scores = (probs * (grad_probs - inner)).astype(BF)
            acc[0, :, s0:s1] += dot(grad_scores, keys * mask)
            acc[1, :, s0:s1] += t_dot(grad_scores, q)
        for s in range(3):
            value = acc[s] * scaling if s < 2 else acc[s]
            g3[s] = value.astype(BF)
        g3[3] = att[l]

    def backward(step, _):
        l = LAYERS - 1 - step

        @pl.when(step == 0)
        def _():
            gather_wait(gtop, zs2, zr2)

        @pl.when(step > 0)
        def _():
            gather_start(gtop)
            finish(l + 1, 0, 0)
            gather_wait(gtop)

        for h in range(2):

            def hidden(n):
                lanes = pl.ds(pl.multiple_of(n * 256, 256), 256)
                value = dot(gtop[...], wm[l, 2 + h, :, lanes]) * slope[l, h, :, lanes].astype(F32)
                low = value.astype(BF)
                gb[h, :, lanes] = low
                csum[l, pl.ds(2 + h, 1), lanes] = jnp.sum(
                    low.astype(F32), axis=0, keepdims=True
                )

            tiles(3, hidden)

        def back_up(start, size):
            rows = pl.ds(start, size)
            value = dot_t(gb[0], wm[l, 0, rows, :]) + dot_t(gb[1], wm[l, 1, rows, :])
            part[:, pl.ds(start, size)] = value.astype(BF)

        features(back_up)
        scatter_start()
        transpose(gtop, 0)
        pair(2, 0, lambda b: 0, lambda b: hid[l, b], step > 0)
        scatter_wait()
        norm_backward(l, 1, gmid, 6 * l + 4)
        gather_start(gmid)
        transpose(x2.at[l], 1)
        pair(1, 1, lambda b: 1, lambda b: gb[b], step >= 0)
        @pl.when(step == 0)
        def _():
            features(down(l, part2))

        gather_wait(gmid)

        @pl.when(step == 0)
        def _():
            scatter_start(side)

        da[...] = dot(gmid[...], wa[l, 3]).astype(BF)
        attend_back(l)
        for s in range(3):
            if s != 1:
                csum[l, s // 2 : s // 2 + 1, 0:PAD] = jnp.sum(
                    g3[s].astype(F32), axis=0, keepdims=True
                )

        def back_qkv(start, size):
            rows = pl.ds(start, size)
            value = dot_t(g3[0], wa[l, 0, rows, :])
            value = value + dot_t(g3[1], wa[l, 1, rows, :])
            value = value + dot_t(g3[2], wa[l, 2, rows, :])
            part[:, pl.ds(start, size)] = value.astype(BF)

        features(back_qkv)
        scatter_start()
        finish(l, 2, 0)
        finish(l, 1, 1)
        transpose(x1.at[l], 0)
        transpose(gmid, 1)
        pair(0, 0, lambda s: s // 3, lambda s: g3[s], step >= 0)
        scatter_wait()
        norm_backward(l, 0, gtop, jnp.where(l > 0, 6 * l - 1, 12))

        @pl.when(step == 0)
        def _():
            scatter_wait(side)
            lax.fori_loop(0, CHUNK // 16, settle(l, recv2), 0)
            for k in range(N):
                oblk[k] = st[:, BLK * k : BLK * (k + 1)]
            give(oblk, out_hbm, outs, outr, True)

        return 0

    lax.fori_loop(0, LAYERS, backward, 0)

    give(oblk, out_hbm, outs, outr, False)
    give_wait(out_hbm, outr)
    for k in range(N):
        oblk[k] = gst[:, BLK * k : BLK * (k + 1)]
    give(oblk, tg_hbm, tgs, tgr, True)

    def c_copy(k):
        return remote(csum, cx.at[k], cxs.at[k], cxr.at[k], (d, near[k], c))

    def v_copy(k):
        return remote(vb.at[near[k]], vx.at[k], vxs.at[k], vxr.at[k], (d, near[k], c))

    def z_copy(k):
        return remote(
            vz.at[c], vz.at[c], vzs.at[k], vzr.at[c], (d, r, lax.rem(c + k + 1, N))
        )

    for k in range(N):
        vb[k] = vsum[:, BLK * k : BLK * (k + 1)]
    for k in range(3):
        v_copy(k).start()
        c_copy(k).start()
    total = vb[r]
    for k in range(3):
        v_copy(k).wait_recv()
        total = total + vx[k]
    vz[c] = total
    for k in range(3):
        z_copy(k).start()
    for k in range(3):
        c_copy(k).wait()
    for l in range(LAYERS):
        csum[l] = csum[l] + cx[0, l] + cx[1, l] + cx[2, l]
    c_half = remote(csum.at[other], cd, cds.at[0], cds.at[1], (other, r, c))
    c_half.start()
    for cs in range(N):

        @pl.when(c != cs)
        def _():
            pltpu.make_async_copy(vz.at[cs], vz.at[cs], vzr.at[cs]).wait()

    total = vz[0]
    for cs in range(1, N):
        total = total + vz[cs]
    vd[0] = total
    v_half = remote(vd.at[0], vd.at[1], vds.at[0], vds.at[1], (other, r, c))
    v_half.start()
    finish(0, 0, 0)
    c_half.wait()
    cout[...] = csum[d] + cd[...]
    v_half.wait()
    vout[...] = vd[0] + vd[1]
    for k in range(3):
        v_copy(k).wait_send()
        z_copy(k).wait_send()

    pl.semaphore_wait(credit, 1)
    give(oblk, tg_hbm, tgs, tgr, False)
    give_wait(tg_hbm, tgr)
    spread(tok_hbm, tin, toks, tokr, False)
    spread(cot_hbm, cin, cots, cotr, False)
    for i in range(3):
        for j in range(2):
            arrived = result(i, other, j)
            pltpu.make_async_copy(arrived, arrived, finr.at[i, j]).wait()
    for k in range(3):
        remote(vec_ref, pin.at[r], vs.at[k], vr.at[k], (d, near[k], c)).wait_send()
    for l in range(LAYERS):
        for i in range(3):
            for k in range(3):
                send_w(l, i, k).wait_send()
                share_w(l, i, k).wait_send()


def fused(*operands):
    dma = pltpu.SemaphoreType.DMA
    vmem = pltpu.VMEM
    whole = pl.BlockSpec(memory_space=pltpu.VMEM)
    anywhere = pl.BlockSpec(memory_space=pl.ANY)
    scratch = [
        vmem((LAYERS, 4, D, PAD), BF),
        vmem((LAYERS, 4, D, HALF), BF),
        vmem((LAYERS, ROWS, D), BF),
        vmem((LAYERS, ROWS, D), BF),
        vmem((LAYERS, 3, ROWS, PAD), BF),
        vmem((LAYERS, ROWS, PAD), BF),
        vmem((LAYERS, ROWS, 128), F32),
        vmem((LAYERS, 2, ROWS, HALF), BF),
        vmem((LAYERS, 2, ROWS, HALF), BF),
        vmem((LAYERS, 2, CHUNK, D), F32),
        vmem((LAYERS, 2, CHUNK, 128), F32),
        vmem((ROWS, D), BF),
        vmem((ROWS, D), BF),
        vmem((2, D, ROWS), BF),
        vmem((ROWS, D), BF),
        vmem((N, CHUNK, D), BF),
        vmem((CHUNK, D), F32),
        vmem((CHUNK, D), F32),
        vmem((N, CHUNK, BLK), BF),
        vmem((N, CHUNK, BLK), BF),
        vmem((N, CHUNK, BLK), F32),
        vmem((N, 16, BLK), F32),
        vmem((16, D), F32),
        vmem((2, ROWS, HALF), BF),
        vmem((ROWS, PAD), BF),
        vmem((4, ROWS, PAD), BF),
        vmem((3, ROWS, PAD), F32),
        vmem((N, BLK, HALF), BF),
        vmem((N, BLK, HALF), BF),
        vmem((2, N, BLK, HALF), BF),
        vmem((3, 3, BLK, HALF), BF),
        vmem((2, BLK, PAD), F32),
        vmem((ROWS, D), BF),
        vmem((N, CHUNK, D), BF),
        vmem((16, D), F32),
        vmem((LAYERS, 4, HALF), F32),
        vmem((N, 16, BLK), F32),
        vmem((3, 16, BLK), F32),
        vmem((N, 16, BLK), F32),
        vmem((2, 16, BLK), F32),
        vmem((3, LAYERS, 4, HALF), F32),
        vmem((4, HALF), F32),
        dma((LAYERS, 3, 2)),
        dma((LAYERS, 3, 3)), dma((LAYERS, 3, 3)),
        dma((LAYERS, 3, 3)), dma((LAYERS, 3, 3)),
        dma((3,)), dma((4,)),
        dma((N,)), dma((N,)), dma((N,)), dma((N,)),
        dma((N,)), dma((N,)), dma((N,)), dma((N,)),
        dma((N,)), dma((N,)), dma((N,)), dma((N,)),
        dma((N,)), dma((N,)), pltpu.SemaphoreType.REGULAR,
        dma((3, 3)), dma((3, 3)), dma((2,)), dma((3, 2)),
        dma((N,)), dma((N,)), dma((N,)), dma((N,)),
        dma((3,)), dma((3,)), dma((3,)), dma((N,)), dma((2,)),
        dma((3,)), dma((3,)), dma((2,)),
    ]
    shape = jax.ShapeDtypeStruct
    return pl.pallas_call(
        kernel,
        out_shape=(
            shape((ROWS, BLK), F32),
            shape((ROWS, BLK), F32),
            shape((4, BLK, PAD), F32),
            shape((BLK, 2 * HALF), F32),
            shape((BLK, 2 * HALF), F32),
            shape((16, BLK), F32),
            shape((4, HALF), F32),
        ),
        in_specs=[anywhere] * 5 + [whole] * 3,
        out_specs=(anywhere,) * 5 + (whole, whole),
        scratch_shapes=scratch,
        compiler_params=pltpu.CompilerParams(
            collective_id=0, has_side_effects=True, vmem_limit_bytes=67_043_328
        ),
    )(*operands)


def widen(values, axis=-1, to=PAD):
    axis = axis % values.ndim
    pads = [(0, 0)] * values.ndim
    pads[axis] = (0, to - values.shape[axis])
    return jnp.pad(values, pads)


def per_device_fused(
    tokens, cotangent, qkv_weight, qv_bias, proj_weight, proj_bias,
    up_weight, up_bias, down_weight, down_bias, norm_gain, norm_shift,
):
    dp = lax.axis_index("dp")
    tok = widen(tokens[0], 0, ROWS)
    cot = widen(cotangent[0], 0, ROWS)
    heads = jnp.concatenate(
        [qkv_weight.transpose(0, 2, 1, 3), proj_weight.transpose(0, 2, 1)[:, None]], axis=1
    )
    vec = jnp.concatenate(
        [norm_gain, norm_shift, proj_bias[:, None], down_bias[:, None]], axis=1
    ).reshape(12, BLK)
    vec = widen(vec, 0, 16)
    zero = jnp.zeros_like(qv_bias[:, 0])
    qb = widen(jnp.stack([qv_bias[:, 0], zero, qv_bias[:, 1]], axis=1))
    ub = up_bias.reshape(LAYERS, 2, HALF)
    down = down_weight.transpose(0, 2, 1)
    out, tg, ga, gu, gd, vout, cout = fused(tok, cot, widen(heads), up_weight, down, vec, qb, ub)
    both = vout[:12].reshape(LAYERS, 6, BLK)
    layer = lax.dynamic_slice(both, (dp, 0, 0), (1, 6, BLK))
    return (
        out[None, :SEQ],
        tg[None, :SEQ],
        ga[:3, :, :BLK].transpose(1, 0, 2)[None],
        cout[None, 0:2, :BLK],
        ga[3, :, :BLK].T[None],
        layer[:, 4],
        gu[None],
        cout[2:].reshape(1, 2 * HALF),
        gd.T[None],
        layer[:, 5],
        both[:, 0:2],
        both[:, 2:4],
    )


NORMAL = (((1,), (0,)), ((), ()))
LAST_BOTH = (((1,), (1,)), ((), ()))
FIRST_BOTH = (((0,), (0,)), ((), ()))


def gather_tokens(values):
    return lax.all_gather(values, "col", axis=0, tiled=True)


def gather_blocks(values):
    return lax.all_gather(values, "row", axis=0, tiled=True)


def gather_grad_blocks(values):
    return lax.all_gather(values, "row", axis=0, tiled=True)


def width_totals(first_sum, second_sum):
    return lax.psum((first_sum, second_sum), "row")


def gather_whole(triple_w, up_w, proj_w, down_w):
    row_whole = (triple_w, up_w, proj_w, down_w)
    col_whole = (proj_w, down_w, triple_w, up_w)
    return (row_whole, col_whole)


def row_product(gathered, matrix, contract):
    return lax.psum_scatter(
        lax.dot_general(gathered, matrix, contract, preferred_element_type=jnp.float32).astype(
            jnp.bfloat16
        ),
        "row",
        scatter_dimension=0,
        tiled=True,
    ).astype(jnp.float32)


def col_product(gathered, matrix, contract):
    return lax.psum_scatter(
        lax.dot_general(gathered, matrix, contract, preferred_element_type=jnp.float32).astype(
            jnp.bfloat16
        ),
        "col",
        scatter_dimension=0,
        tiled=True,
    ).astype(jnp.float32)


def norm_forward(stream, factor, shift):
    totals, squares = width_totals(jnp.sum(stream, axis=1), jnp.sum(stream * stream, axis=1))
    centre = totals / D
    spread = squares / D - centre * centre
    centred = stream - centre[:, None]
    scaling = lax.rsqrt(spread + EPSILON)
    standard = centred * scaling[:, None]
    return (standard * factor + shift, standard, scaling)


def norm_backward(grad_norm, standard, scaling, factor):
    factor_grad = jnp.sum(grad_norm * standard, axis=0)
    shift_grad = jnp.sum(grad_norm, axis=0)
    grad_standard = grad_norm * factor
    first_sum, second_sum = width_totals(
        jnp.sum(grad_standard, axis=1), jnp.sum(grad_standard * standard, axis=1)
    )
    grad_stream = scaling[:, None] * (
        grad_standard - first_sum[:, None] / D - standard * (second_sum[:, None] / D)
    )
    return (grad_stream, factor_grad, shift_grad)


def split_triple(triple_out, width):
    images = triple_out.shape[0] // SEQ
    head_count = width // HEAD_DIM
    pieces = triple_out.reshape(images, SEQ, 3, head_count, HEAD_DIM)
    return (pieces[:, :, 0], pieces[:, :, 1], pieces[:, :, 2])


def attend_forward(triple_out, width):
    queries, key_rows, values = split_triple(triple_out, width)
    scaling = HEAD_DIM ** (-0.5)
    scores = (
        jnp.einsum("bqhd,bkhd->bhqk", queries, key_rows, preferred_element_type=jnp.float32)
        * scaling
    )
    row_peak = jnp.max(scores, axis=-1, keepdims=True)
    log_totals = row_peak + jnp.log(jnp.sum(jnp.exp(scores - row_peak), axis=-1, keepdims=True))
    probs_low = jnp.exp(scores - log_totals).astype(jnp.bfloat16)
    attended = jnp.einsum("bhqk,bkhd->bqhd", probs_low, values, preferred_element_type=jnp.float32)
    return (attended.reshape(triple_out.shape[0], width).astype(jnp.bfloat16), log_totals)


def attend_backward(triple_out, log_totals, grad_attended, width):
    queries, key_rows, values = split_triple(triple_out, width)
    scaling = HEAD_DIM ** (-0.5)
    scores = (
        jnp.einsum("bqhd,bkhd->bhqk", queries, key_rows, preferred_element_type=jnp.float32)
        * scaling
    )
    probs = jnp.exp(scores - log_totals)
    probs_low = probs.astype(jnp.bfloat16)
    grad_heads = grad_attended.reshape(values.shape)
    grad_values = jnp.einsum(
        "bhqk,bqhd->bkhd", probs_low, grad_heads, preferred_element_type=jnp.float32
    )
    grad_probs = jnp.einsum(
        "bqhd,bkhd->bhqk", grad_heads, values, preferred_element_type=jnp.float32
    )
    grad_scores = (
        probs * (grad_probs - jnp.sum(grad_probs * probs, axis=-1, keepdims=True))
    ).astype(jnp.bfloat16)
    grad_queries = (
        jnp.einsum("bhqk,bkhd->bqhd", grad_scores, key_rows, preferred_element_type=jnp.float32)
        * scaling
    )
    grad_keys = (
        jnp.einsum("bhqk,bqhd->bkhd", grad_scores, queries, preferred_element_type=jnp.float32)
        * scaling
    )
    stacked = jnp.stack([grad_queries, grad_keys, grad_values], axis=2)
    return stacked.reshape(triple_out.shape[0], 3 * width).astype(jnp.bfloat16)


def layer_forward(stream, weights):
    qkv_w, qv_b, proj_w, proj_b, up_w, up_b, down_w, down_b, factors, shifts = weights
    width = qkv_w.shape[2]
    triple_w = qkv_w.reshape(qkv_w.shape[0], 3 * width)
    row_whole, col_whole = gather_whole(triple_w, up_w, proj_w, down_w)
    first_norm, first_standard, first_scaling = norm_forward(stream, factors[0], shifts[0])
    first_rows = gather_tokens(first_norm.astype(jnp.bfloat16))
    offsets = jnp.concatenate([qv_b[0], jnp.zeros_like(qv_b[0]), qv_b[1]])
    triple_out = (row_product(first_rows, triple_w, NORMAL) + offsets).astype(jnp.bfloat16)
    attended, log_totals = attend_forward(triple_out, width)
    head_rows = gather_blocks(attended)
    stream_mid = stream + col_product(head_rows, proj_w, NORMAL) + proj_b
    second_norm, second_standard, second_scaling = norm_forward(stream_mid, factors[1], shifts[1])
    second_rows = gather_tokens(second_norm.astype(jnp.bfloat16))
    before = row_product(second_rows, up_w, NORMAL) + up_b
    activated = jax.nn.gelu(before, approximate=False).astype(jnp.bfloat16)
    hidden_rows = gather_blocks(activated)
    branch_out = col_product(hidden_rows, down_w, NORMAL)
    stream_out = stream_mid + branch_out + down_b
    saved = (
        first_rows,
        first_standard,
        first_scaling,
        triple_out,
        log_totals,
        head_rows,
        second_rows,
        second_standard,
        second_scaling,
        before,
        hidden_rows,
        row_whole,
        col_whole,
    )
    return (stream_out, saved)


def layer_backward(grad_out, saved, weights):
    qkv_w, qv_b, proj_w, proj_b, up_w, up_b, down_w, down_b, factors, shifts = weights
    (
        first_rows,
        first_standard,
        first_scaling,
        triple_out,
        log_totals,
        head_rows,
        second_rows,
        second_standard,
        second_scaling,
        before,
        hidden_rows,
        row_whole,
        col_whole,
    ) = saved
    width = qkv_w.shape[2]
    triple_w = qkv_w.reshape(qkv_w.shape[0], 3 * width)
    grad_rows = gather_tokens(grad_out.astype(jnp.bfloat16))
    down_grad = lax.dot_general(
        hidden_rows, grad_rows, FIRST_BOTH, preferred_element_type=jnp.float32
    )
    down_off_grad = jnp.sum(grad_rows, axis=0, dtype=jnp.float32)
    grad_active = row_product(grad_rows, down_w, LAST_BOTH)
    _, slope_pull = jax.vjp(partial(jax.nn.gelu, approximate=False), before)
    grad_before = slope_pull(grad_active)[0].astype(jnp.bfloat16)
    before_rows = gather_grad_blocks(grad_before)
    up_grad = lax.dot_general(
        second_rows, before_rows, FIRST_BOTH, preferred_element_type=jnp.float32
    )
    up_off_grad = jnp.sum(before_rows, axis=0, dtype=jnp.float32)
    grad_second = col_product(before_rows, up_w, LAST_BOTH)
    grad_mid, second_factor_grad, second_shift_grad = norm_backward(
        grad_second, second_standard, second_scaling, factors[1]
    )
    grad_mid = grad_mid + grad_out
    mid_rows = gather_tokens(grad_mid.astype(jnp.bfloat16))
    proj_grad = lax.dot_general(head_rows, mid_rows, FIRST_BOTH, preferred_element_type=jnp.float32)
    proj_off_grad = jnp.sum(mid_rows, axis=0, dtype=jnp.float32)
    grad_attended = row_product(mid_rows, proj_w, LAST_BOTH).astype(jnp.bfloat16)
    grad_triple = attend_backward(triple_out, log_totals, grad_attended, width)
    triple_rows = gather_grad_blocks(grad_triple)
    triple_grad = lax.dot_general(
        first_rows, triple_rows, FIRST_BOTH, preferred_element_type=jnp.float32
    )
    column_sums = jnp.sum(triple_rows, axis=0, dtype=jnp.float32).reshape(3, width)
    qv_grad = jnp.stack([column_sums[0], column_sums[2]])
    grad_first = col_product(triple_rows, triple_w, LAST_BOTH)
    grad_in, first_factor_grad, first_shift_grad = norm_backward(
        grad_first, first_standard, first_scaling, factors[0]
    )
    grad_in = grad_in + grad_mid
    factor_grads = jnp.stack([first_factor_grad, second_factor_grad])
    shift_grads = jnp.stack([first_shift_grad, second_shift_grad])
    layer_grads = (
        triple_grad.reshape(qkv_w.shape),
        qv_grad,
        proj_grad,
        proj_off_grad,
        up_grad,
        up_off_grad,
        down_grad,
        down_off_grad,
        factor_grads,
        shift_grads,
    )
    return (grad_in, layer_grads)


def per_device_plain(
    tokens,
    cotangent,
    qkv_weight,
    qv_bias,
    proj_weight,
    proj_bias,
    up_weight,
    up_bias,
    down_weight,
    down_bias,
    norm_gain,
    norm_shift,
):
    image_count, seq_len, width_row = tokens.shape
    stream = tokens.reshape(image_count * seq_len, width_row).astype(jnp.float32)
    layer_params = []
    saved_list = []
    for layer_index in range(LAYERS):
        params = (
            qkv_weight[layer_index],
            qv_bias[layer_index],
            proj_weight[layer_index],
            proj_bias[layer_index],
            up_weight[layer_index],
            up_bias[layer_index],
            down_weight[layer_index],
            down_bias[layer_index],
            norm_gain[layer_index],
            norm_shift[layer_index],
        )
        layer_params.append(params)
        stream, saved = layer_forward(stream, params)
        saved_list.append(saved)
    grad_stream = cotangent.reshape(image_count * seq_len, width_row).astype(jnp.float32)
    per_layer = [None] * LAYERS
    for layer_index in reversed(range(LAYERS)):
        grad_stream, layer_grads = layer_backward(
            grad_stream, saved_list[layer_index], layer_params[layer_index]
        )
        per_layer[layer_index] = layer_grads
    stacked = tuple(
        (jnp.stack([layer_grads[position] for layer_grads in per_layer]) for position in range(10))
    )
    summed = (
        lax.psum_scatter(
            stacked[0].astype(jnp.bfloat16), "dp", scatter_dimension=0, tiled=True
        ).astype(jnp.float32),
        lax.psum_scatter(
            stacked[1].astype(jnp.bfloat16), "dp", scatter_dimension=0, tiled=True
        ).astype(jnp.float32),
        lax.psum_scatter(
            stacked[2].astype(jnp.bfloat16), "dp", scatter_dimension=0, tiled=True
        ).astype(jnp.float32),
        lax.psum_scatter(
            stacked[3].astype(jnp.bfloat16), "dp", scatter_dimension=0, tiled=True
        ).astype(jnp.float32),
        lax.psum_scatter(
            stacked[4].astype(jnp.bfloat16), "dp", scatter_dimension=0, tiled=True
        ).astype(jnp.float32),
        lax.psum_scatter(
            stacked[5].astype(jnp.bfloat16), "dp", scatter_dimension=0, tiled=True
        ).astype(jnp.float32),
        lax.psum_scatter(
            stacked[6].astype(jnp.bfloat16), "dp", scatter_dimension=0, tiled=True
        ).astype(jnp.float32),
        lax.psum_scatter(
            stacked[7].astype(jnp.bfloat16), "dp", scatter_dimension=0, tiled=True
        ).astype(jnp.float32),
    )
    norm_sums = lax.psum((stacked[8], stacked[9]), ("dp", "col"))
    result = stream.reshape(image_count, seq_len, width_row)
    tokens_grad = grad_stream.reshape(image_count, seq_len, width_row)
    return (
        result,
        tokens_grad,
        summed[0],
        summed[1],
        summed[2],
        summed[3],
        summed[4],
        summed[5],
        summed[6],
        summed[7],
        norm_sums[0],
        norm_sums[1],
    )


def solution(mesh):
    placed = (
        P(("dp", "col"), None, "row"),
        P(("dp", "col"), None, "row"),
        P(None, "row", None, "col"),
        P(None, None, "col"),
        P(None, "col", "row"),
        P(None, "row"),
        P(None, "row", "col"),
        P(None, "col"),
        P(None, "col", "row"),
        P(None, "row"),
        P(None, None, "row"),
        P(None, None, "row"),
    )
    sizes = (mesh.shape["dp"], mesh.shape["row"], mesh.shape["col"])
    return jax.shard_map(
        per_device_fused if sizes == (2, N, N) else per_device_plain,
        mesh=mesh,
        in_specs=placed,
        out_specs=(
            P(("dp", "col"), None, "row"),
            P(("dp", "col"), None, "row"),
            P("dp", "row", None, "col"),
            P("dp", None, "col"),
            P("dp", "col", "row"),
            P("dp", "row"),
            P("dp", "row", "col"),
            P("dp", "col"),
            P("dp", "col", "row"),
            P("dp", "row"),
            P(None, None, "row"),
            P(None, None, "row"),
        ),
        check_vma=False,
    )
```

```python
from functools import partial

import jax
import jax.numpy as jnp
from jax import lax
from jax.experimental import pallas as pl
from jax.experimental.pallas import tpu as pltpu
from jax.sharding import PartitionSpec as P

D = 1408
HEAD_DIM = 88
SEQ = 257
LAYERS = 2
EPSILON = 1e-06
MESH = pl.DeviceIdType.MESH
BF = jnp.bfloat16
F32 = jnp.float32

ROWS = 272
STEP = 64
CHUNK = 80
LAST = 72
BLK = 352
PAD = 384
HALF = 768
N = 4


def dot(a, b):
    return jnp.dot(a, b, preferred_element_type=F32)


def dot_t(a, b):
    return lax.dot_general(a, b, (((1,), (1,)), ((), ())), preferred_element_type=F32)


def t_dot(a, b):
    return lax.dot_general(a, b, (((0,), (0,)), ((), ())), preferred_element_type=F32)


def span(index):
    return pl.ds(STEP * index, STEP if index < N - 1 else LAST)


def head_span(head):
    low, high = HEAD_DIM * head, HEAD_DIM * (head + 1)
    return low, high, low // 128 * 128, -(-high // 128) * 128


def kernel(
    tok_hbm, cot_hbm, wa_hbm, up_hbm, down_hbm, vec_ref, qb_ref, ub_ref,
    out_hbm, tg_hbm, ga_hbm, gu_hbm, gd_hbm, vout, cout,
    wa, wm, x1, x2, triple, att, lse, hid, slope, std, inv,
    gtop, gmid, lt, part, recv, st, gst, tin, cin, oblk, mid, pin, pv,
    gb, da, g3, acc, sbuf, prx, keep, ici, fin, hop, recv2,
    vsum, csum, vb, vx, vz, vd, cx, cd,
    wloc, wsend, wrecv, fsend, frecv, psend, precv, vs, vr, m1s, m1r, m2s, m2r,
    zs, zr, rss, rsr, cs_s, cs_r, credit, gis, gir, fins, finr, hs, hr,
    zs2, zr2, rss2, rsr2, vxs, vxr, vzs, vzr, vds, cxs, cxr, cds,
):
    d, r, c = lax.axis_index("dp"), lax.axis_index("row"), lax.axis_index("col")
    other = 1 - d
    near = (r + 1 - 2 * lax.rem(r, 2), lax.rem(r + 2, N), N - 1 - r)
    last = c == N - 1

    def remote(src, dst, ssem, rsem, dev):
        return pltpu.make_async_remote_copy(
            src, dst, ssem, rsem, device_id=dev, device_id_type=MESH
        )

    def rblk(index):
        return pl.ds(pl.multiple_of(index * BLK, 16), BLK)

    def rhalf(index, part_):
        return pl.ds(pl.multiple_of(index * BLK + part_ * (BLK // 2), 16), BLK // 2)

    recv[...] = jnp.zeros_like(recv)
    recv2[...] = jnp.zeros_like(recv2)
    for array in (x1.at[0], x1.at[1], x2.at[0], x2.at[1], gtop, gmid):
        array[ROWS - 16 :, :] = jnp.zeros((16, D), BF)
    tin[...] = jnp.zeros_like(tin)
    cin[...] = jnp.zeros_like(cin)
    vsum[...] = jnp.zeros_like(vsum)
    csum[...] = jnp.zeros_like(csum)
    barrier = pltpu.get_barrier_semaphore()
    for k in range(N * N):
        pl.semaphore_signal(
            barrier, inc=1,
            device_id=(d, lax.rem(r + k // N, N), lax.rem(c + k % N, N)), device_id_type=MESH,
        )
    pl.semaphore_signal(barrier, inc=1, device_id=(other, r, c), device_id_type=MESH)
    pl.semaphore_wait(barrier, N * N + 1)

    for k in range(3):
        remote(vec_ref, pin.at[r], vs.at[k], vr.at[k], (d, near[k], c)).start()
    own_vec = pltpu.make_async_copy(vec_ref, pin.at[r], vr.at[3])
    own_vec.start()

    def by_size(body):
        @pl.when(last)
        def _():
            body(LAST)

        @pl.when(jnp.logical_not(last))
        def _():
            body(STEP)

    def come_start(u, src):
        for ct in range(N):
            size = STEP if ct < N - 1 else LAST
            source, target = src.at[span(ct)], mid.at[u, c, pl.ds(0, size)]

            @pl.when(c == ct)
            def _():
                pltpu.make_async_copy(source, target, m1r.at[u, c]).start()

            @pl.when(c != ct)
            def _():
                remote(source, target, m1s.at[u, ct], m1r.at[u, c], (d, r, ct)).start()

    def come_pass(u, dst):
        def sized(size):
            rows = pl.ds(0, size)
            for p in range(N):
                source, target = mid.at[u, p, rows], dst.at[r, rows]
                pltpu.make_async_copy(source, source, m1r.at[u, p]).wait()

                @pl.when(r == p)
                def _():
                    pltpu.make_async_copy(source, target, m2r.at[u, r]).start()

                @pl.when(r != p)
                def _():
                    remote(source, target, m2s.at[u, p], m2r.at[u, r], (d, p, c)).start()

        by_size(sized)

    def come_wait(u, dst):
        def sized(size):
            for rs in range(N):
                rows = dst.at[rs, pl.ds(0, size)]
                pltpu.make_async_copy(rows, rows, m2r.at[u, rs]).wait()

        by_size(sized)

    def go_start(u):
        def sized(size):
            rows = pl.ds(0, size)
            for k in range(N):
                source, target = oblk.at[k, rows], mid.at[u, r, rows]

                @pl.when(r == k)
                def _():
                    pltpu.make_async_copy(source, target, m1r.at[u, r]).start()

                @pl.when(r != k)
                def _():
                    remote(source, target, m1s.at[u, k], m1r.at[u, r], (d, k, c)).start()

        by_size(sized)

    def go_pass(u, dst):
        def sized(size):
            for p in range(N):
                source = mid.at[u, p, pl.ds(0, size)]
                target = dst.at[pl.ds(pl.multiple_of(STEP * c, 16), size)]
                pltpu.make_async_copy(source, source, m1r.at[u, p]).wait()

                @pl.when(c == p)
                def _():
                    pltpu.make_async_copy(source, target, m2r.at[u, c]).start()

                @pl.when(c != p)
                def _():
                    remote(source, target, m2s.at[u, p], m2r.at[u, c], (d, r, p)).start()

        by_size(sized)

    def go_wait(u, dst):
        for cs in range(N):
            rows = dst.at[span(cs)]
            pltpu.make_async_copy(rows, rows, m2r.at[u, cs]).wait()

    def sent(u):
        for ct in range(N):
            size = STEP if ct < N - 1 else LAST
            rows = mid.at[u, 0, pl.ds(0, size)]

            if u < 2:

                @pl.when(c != ct)
                def _():
                    remote(rows, rows, m1s.at[u, ct], m1r.at[u, 0], (d, r, ct)).wait_send()

            def second(size):
                rows = mid.at[u, 0, pl.ds(0, size)]
                first_row = u < 2

                @pl.when((r != ct) if first_row else (c != ct))
                def _():
                    remote(rows, rows, m2s.at[u, ct], m2r.at[u, 0], (d, r, c)).wait_send()

                if not first_row:

                    @pl.when(r != ct)
                    def _():
                        remote(rows, rows, m1s.at[u, ct], m1r.at[u, 0], (d, ct, c)).wait_send()

            by_size(second)

    come_start(0, tok_hbm)

    def source_w(l, i, which):
        if i == 0:
            return wa_hbm.at[l, pl.ds(2 * which, 2)]
        lanes = pl.ds(pl.multiple_of(HALF * which, 128), HALF)
        return (up_hbm if i == 1 else down_hbm).at[l, :, lanes]

    def rows_w(l, i, which, block):
        if i == 0:
            return wa.at[l, pl.ds(2 * which, 2), block, :]
        return wm.at[l, 2 * (i - 1) + which, block, :]

    def local_w(l, i, which):
        return pltpu.make_async_copy(
            source_w(l, i, which), rows_w(l, i, which, rblk(r)), wloc.at[l, i, which]
        )

    def send_w(l, i, k):
        return remote(
            source_w(l, i, d), rows_w(l, i, d, rblk(r)), wsend.at[l, i, k], wrecv.at[l, i, k],
            (d, near[k], c),
        )

    def pass_w(l, i, k):
        rows = rows_w(l, i, d, rhalf(near[k], k))
        return remote(rows, rows, fsend.at[l, i, k], frecv.at[l, i, k], (d, near[1 - k], c))

    def share_w(l, i, k):
        rows = rows_w(l, i, d, rblk(near[k]))
        return remote(rows, rows, psend.at[l, i, k], precv.at[l, i, k], (other, r, c))

    def direct_w(l, i):
        for k in range(2):
            send_w(l, i, k).start()

    def stage_w(l, i):
        for k in range(2):
            send_w(l, i, k).wait_recv()
            pass_w(l, i, k).start()
        for k in range(2):
            share_w(l, i, k).start()

    def close_w(l, i):
        for k in range(2):
            rows = rows_w(l, i, d, rhalf(near[2], k))
            pltpu.make_async_copy(rows, rows, frecv.at[l, i, k]).wait()
        share_w(l, i, 2).start()

    def need_w(l, i):
        for which in range(2):
            local_w(l, i, which).wait()
        for k in range(3):
            rows = rows_w(l, i, other, rblk(near[k]))
            pltpu.make_async_copy(rows, rows, precv.at[l, i, k]).wait()

    direct_w(0, 0)
    come_start(1, cot_hbm)
    come_pass(0, tin)
    for l in range(LAYERS):
        for i in range(3):
            for which in range(2):
                local_w(l, i, which).start()

    def gather_start(x, zs=zs, zr=zr):
        for cs in range(N):

            @pl.when(c == cs)
            def _():
                for ct in range(N):
                    if ct != cs:
                        rows = x.at[span(cs)]
                        remote(rows, rows, zs.at[ct], zr.at[cs], (d, r, ct)).start()

    def gather_wait(x, zs=zs, zr=zr):
        for cs in range(N):
            rows = x.at[span(cs)]

            @pl.when(c != cs)
            def _():
                pltpu.make_async_copy(rows, rows, zr.at[cs]).wait()

            @pl.when(c == cs)
            def _():
                for ct in range(N):
                    if ct != cs:
                        remote(rows, rows, zs.at[ct], zr.at[cs], (d, r, ct)).wait_send()

    def scatter_copy(ct, part, recv, rss, rsr):
        size = STEP if ct < N - 1 else LAST
        return remote(
            part.at[span(ct)], recv.at[c, pl.ds(0, size)], rss.at[ct], rsr.at[c], (d, r, ct)
        )

    main = (part, recv, rss, rsr)
    side = (x2.at[LAYERS - 1], recv2, rss2, rsr2)

    def scatter_start(path=main):
        for ct in range(N):

            @pl.when(c != ct)
            def _():
                scatter_copy(ct, *path).start()

            @pl.when(c == ct)
            def _():
                size = STEP if ct < N - 1 else LAST
                path[1][ct, 0:size, :] = path[0][span(ct), :]

    def scatter_wait(path=main):
        for cs in range(N):
            for big in (False, True):
                size = LAST if big else STEP
                rows = path[1].at[cs, pl.ds(0, size)]

                @pl.when(jnp.logical_and(c != cs, last if big else jnp.logical_not(last)))
                def _():
                    pltpu.make_async_copy(rows, rows, path[3].at[cs]).wait()

            @pl.when(c != cs)
            def _():
                scatter_copy(cs, *path).wait_send()

    def received(rows, recv=recv):
        total = recv[0, rows, :].astype(F32)
        for cs in range(1, N):
            total = total + recv[cs, rows, :].astype(F32)
        return total

    def vector(row):
        return pv[pl.ds(row, 1), :]

    def own_rows(x, t, value):
        @pl.when(jnp.logical_or(t < 4, last))
        def _():
            x[pl.ds(pl.multiple_of(STEP * c + 16 * t, 16), 16), :] = value

    valid = jnp.where(last, SEQ - STEP * (N - 1), STEP)

    def masked(t, value):
        index = lax.broadcasted_iota(jnp.int32, (16, 1), 0) + 16 * t
        return jnp.where(index < valid, value, 0.0)

    def norm_forward(l, j, x, extra):
        def body(t, _):
            rows = pl.ds(pl.multiple_of(16 * t, 16), 16)
            v = extra(rows)
            st[rows, :] = v
            centre = jnp.sum(v, axis=1, keepdims=True) / D
            spread_ = jnp.sum(v * v, axis=1, keepdims=True) / D - centre * centre
            scale = lax.rsqrt(spread_ + EPSILON)
            standard = (v - centre) * scale
            std[l, j, rows, :] = standard
            inv[l, j, rows, :] = jnp.broadcast_to(scale, (16, 128))
            value = standard * vector(6 * l + j) + vector(6 * l + 2 + j)
            own_rows(x, t, value.astype(BF))
            return 0

        lax.fori_loop(0, CHUNK // 16, body, 0)

    def norm_backward(l, j, x, bias_row):
        def body(t, _):
            rows = pl.ds(pl.multiple_of(16 * t, 16), 16)
            e = received(rows)
            standard = std[l, j, rows, :]
            gain_term = masked(t, e * standard)
            vsum[pl.ds(6 * l + j, 1), :] += jnp.sum(gain_term, axis=0, keepdims=True)
            vsum[pl.ds(6 * l + 2 + j, 1), :] += jnp.sum(masked(t, e), axis=0, keepdims=True)
            f = e * vector(6 * l + j)
            first = jnp.sum(f, axis=1, keepdims=True) / D
            second = jnp.sum(f * standard, axis=1, keepdims=True) / D
            scale = inv[l, j, rows, 0:1]
            grad = gst[rows, :] + scale * (f - first - standard * second)
            gst[rows, :] = grad
            if x is not None:
                low = grad.astype(BF)
                own_rows(x, t, low)
                vsum[pl.ds(bias_row, 1), :] += jnp.sum(
                    masked(t, low.astype(F32)), axis=0, keepdims=True
                )
            return 0

        lax.fori_loop(0, CHUNK // 16, body, 0)

    def tiles(count, body):
        lax.fori_loop(0, count, lambda n, _: (body(n), 0)[1], 0)

    def features(body):
        tiles(5, lambda n: body(pl.multiple_of(n * 256, 256), 256))
        body(1280, 128)

    def assemble(src, dst):
        for k in range(N):
            dst[:, BLK * k : BLK * (k + 1)] = src[k, :, 0:BLK].astype(F32)

    for k in range(3):
        remote(vec_ref, pin.at[r], vs.at[k], vr.at[k], (d, near[k], c)).wait_recv()
    own_vec.wait()
    assemble(pin, pv)
    come_wait(0, tin)
    come_pass(1, cin)
    assemble(tin, st)

    lane = lax.broadcasted_iota(jnp.int32, (1, PAD), 1)
    key_ok = lax.broadcasted_iota(jnp.int32, (1, ROWS), 1) < SEQ
    scaling = HEAD_DIM**-0.5

    def head_mask(head):
        low, high, s0, s1 = head_span(head)
        lanes = lane[:, s0:s1]
        return jnp.logical_and(lanes >= low, lanes < high).astype(BF), s0, s1

    def attend(l):
        acc[0] = jnp.zeros((ROWS, PAD), F32)
        for head in range(4):
            mask, s0, s1 = head_mask(head)
            q = triple[l, 0, :, s0:s1] * mask
            scores = dot_t(q, triple[l, 1, :, s0:s1]) * scaling
            scores = jnp.where(key_ok, scores, -1e30)
            peak = jnp.max(scores, axis=1, keepdims=True)
            total = peak + jnp.log(jnp.sum(jnp.exp(scores - peak), axis=1, keepdims=True))
            lse[l, :, head : head + 1] = total
            probs = jnp.exp(scores - total).astype(BF)
            acc[0, :, s0:s1] += dot(probs, triple[l, 2, :, s0:s1] * mask)
        att[l] = acc[0].astype(BF)

    def down(l, target):
        def body(start, size):
            rows = pl.ds(start, size)
            value = dot_t(hid[l, 0], wm[l, 2, rows, :]) + dot_t(hid[l, 1], wm[l, 3, rows, :])
            target[:, rows] = value.astype(BF)

        return body

    def settle(l, recv):
        def body(t, _):
            rows = pl.ds(pl.multiple_of(16 * t, 16), 16)
            st[rows, :] = st[rows, :] + received(rows, recv) + vector(6 * l + 5)
            return 0

        return body

    def top_rows(t, _):
        rows = pl.ds(pl.multiple_of(16 * t, 16), 16)
        low = gst[rows, :].astype(BF)
        own_rows(gtop, t, low)
        vsum[pl.ds(6 * (LAYERS - 1) + 5, 1), :] += jnp.sum(
            masked(t, low.astype(F32)), axis=0, keepdims=True
        )
        return 0

    def forward(l, _):
        def take(rows):
            return st[rows, :]

        norm_forward(l, 0, x1.at[l], take)
        gather_start(x1.at[l])

        @pl.when(l == 0)
        def _():
            stage_w(0, 0)
            direct_w(0, 1)
            direct_w(0, 2)

        close_w(l, 0)
        gather_wait(x1.at[l])

        @pl.when(l == 0)
        def _():
            come_wait(1, cin)
            assemble(cin, gst)
            lax.fori_loop(0, CHUNK // 16, top_rows, 0)
            gather_start(gtop, zs2, zr2)

        need_w(l, 0)

        def qkv(s):
            value = dot(x1[l], wa[l, s]) + qb_ref[l, pl.ds(s, 1), :]
            triple[l, s] = value.astype(BF)

        tiles(3, qkv)
        attend(l)

        def proj(start, size):
            value = dot_t(att[l], wa[l, 3, pl.ds(start, size), :])
            part[:, pl.ds(start, size)] = value.astype(BF)

        features(proj)
        scatter_start()
        stage_w(l, 1)

        @pl.when(l == 0)
        def _():
            direct_w(1, 0)

        scatter_wait()
        norm_forward(
            l, 1, x2.at[l], lambda rows: st[rows, :] + received(rows) + vector(6 * l + 4)
        )
        gather_start(x2.at[l])
        close_w(l, 1)
        stage_w(l, 2)

        @pl.when(l == 0)
        def _():
            direct_w(1, 1)

        need_w(l, 1)
        gather_wait(x2.at[l])

        for h in range(2):

            def up(n):
                lanes = pl.ds(pl.multiple_of(n * 256, 256), 256)
                before = dot(x2[l], wm[l, h, :, lanes]) + ub_ref[l, pl.ds(h, 1), lanes]
                half = before * (0.5**0.5)
                cdf = 0.5 + 0.5 * lax.erf(half)
                hid[l, h, :, lanes] = (before * cdf).astype(BF)
                density = jnp.exp(-half * half) * 0.3989422804014327
                slope[l, h, :, lanes] = (cdf + before * density).astype(slope.dtype)

            tiles(3, up)
        close_w(l, 2)
        need_w(l, 2)

        @pl.when(l == 0)
        def _():
            features(down(l, part))
            scatter_start()
            stage_w(1, 0)
            direct_w(1, 2)
            scatter_wait()
            lax.fori_loop(0, CHUNK // 16, settle(l, recv), 0)

        return 0

    lax.fori_loop(0, LAYERS, forward, 0)

    def transpose(src, index):
        def body(n):
            lanes = pl.ds(pl.multiple_of(n * 128, 128), 128)
            lt[index, lanes, :] = src[:, lanes].T

        tiles(D // 128, body)

    def piece(turn, k):
        return remote(
            sbuf.at[lax.rem(k, 2)], prx.at[turn, k], cs_s.at[k], cs_r.at[turn, k], (other, r, c)
        )

    def block_tile(ref, i, b, k, left, right):
        rows = rblk(k)
        for j in range(2):
            lanes = pl.ds(PAD * j, PAD)
            if i == 0:
                s = 2 * b + j
                value = dot(lt[left(s), rows, :], right(s))
            else:
                value = dot(lt[left(b), rows, :], right(b)[:, lanes])
            ref[:, lanes] = value.astype(BF)

    def strips(count, body):
        def strip(t, _):
            body(pl.ds(pl.multiple_of(16 * t, 16), 16))
            return 0

        lax.fori_loop(0, count // 16, strip, 0)

    def make(i, slot, turn, left, right, wait_credit):
        @pl.when(wait_credit)
        def _():
            pl.semaphore_wait(credit, 1)

        def send_tile(k):
            @pl.when(k >= 2)
            def _():
                piece(turn, k - 2).wait_send()

            block_tile(sbuf.at[lax.rem(k, 2)], i, other, k, left, right)
            piece(turn, k).start()

        tiles(N, send_tile)

        def keep_tile(k):
            block_tile(keep.at[slot, k], i, d, k, left, right)

        tiles(N, keep_tile)
        for k in (2, 3):
            piece(turn, k).wait_send()

    def half_copy(i, slot, k):
        half = pl.ds(k * (BLK // 2), BLK // 2)
        return remote(
            keep.at[slot, near[2], half], hop.at[i, k], hs.at[i, k], hr.at[i, k], (d, near[k], c)
        )

    def block_copy(i, slot, k):
        return remote(
            keep.at[slot, near[k]], ici.at[i, k], gis.at[i, k], gir.at[i, k], (d, near[k], c)
        )

    def merge(i, slot, turn):
        def add(k):
            rows = prx.at[turn, k]
            pltpu.make_async_copy(rows, rows, cs_r.at[turn, k]).wait()

            def strip(rows):
                value = keep[slot, k, rows, :].astype(F32) + prx[turn, k, rows, :].astype(F32)
                keep[slot, k, rows, :] = value.astype(BF)

            strips(BLK, strip)

        add(near[2])
        for k in range(2):
            half_copy(i, slot, k).start()
        for k in (near[0], near[1], r):
            add(k)
        pl.semaphore_signal(credit, inc=1, device_id=(other, r, c), device_id_type=MESH)

    def relay(i, slot):
        for k in range(2):
            pltpu.make_async_copy(hop.at[i, k], hop.at[i, k], hr.at[i, k]).wait()
            block = near[1 - k]

            def strip(t, _):
                rows = pl.ds(pl.multiple_of(16 * t, 16), 16)
                half = pl.ds(pl.multiple_of(k * (BLK // 2) + 16 * t, 16), 16)
                value = keep[slot, block, half, :].astype(F32) + hop[i, k, rows, :].astype(F32)
                keep[slot, block, half, :] = value.astype(BF)
                return 0

            lax.fori_loop(0, BLK // 32, strip, 0)
            block_copy(i, slot, 1 - k).start()

    def result(i, which, j):
        if i == 0:
            return ga_hbm.at[2 * which + j]
        lanes = pl.ds(pl.multiple_of(HALF * which + PAD * j, 128), PAD)
        return (gu_hbm if i == 1 else gd_hbm).at[:, lanes]

    def finish(l, i, slot):
        for k in range(2):
            arrived = ici.at[i, k]
            pltpu.make_async_copy(arrived, arrived, gir.at[i, k]).wait()

        def body(t, _):
            rows = pl.ds(pl.multiple_of(16 * t, 16), 16)
            total = keep[slot, r, rows, :].astype(F32)
            for k in range(2):
                total = total + ici[i, k, rows, :].astype(F32)
            fin[0, rows, :] = total[:, 0:PAD]
            fin[1, rows, :] = total[:, PAD : 2 * PAD]
            return 0

        lax.fori_loop(0, BLK // 16, body, 0)

        @pl.when(l == d)
        def _():
            copies = [
                pltpu.make_async_copy(fin.at[j], result(i, d, j), fins.at[j]) for j in range(2)
            ]
            for copy in copies:
                copy.start()
            for copy in copies:
                copy.wait()

        @pl.when(l != d)
        def _():
            copies = [
                remote(fin.at[j], result(i, d, j), fins.at[j], finr.at[i, j], (other, r, c))
                for j in range(2)
            ]
            for copy in copies:
                copy.start()
            for copy in copies:
                copy.wait_send()

        for k in range(2):
            half_copy(i, slot, k).wait_send()
            block_copy(i, slot, k).wait_send()

    def attend_back(l):
        for s in range(3):
            acc[s] = jnp.zeros((ROWS, PAD), F32)
        for head in range(4):
            mask, s0, s1 = head_mask(head)
            q = triple[l, 0, :, s0:s1] * mask
            keys = triple[l, 1, :, s0:s1]
            scores = dot_t(q, keys) * scaling
            scores = jnp.where(key_ok, scores, -1e30)
            probs = jnp.exp(scores - lse[l, :, head : head + 1])
            probs_low = probs.astype(BF)
            grad_heads = da[:, s0:s1] * mask
            acc[2, :, s0:s1] += t_dot(probs_low, grad_heads)
            grad_probs = dot_t(grad_heads, triple[l, 2, :, s0:s1])
            inner = jnp.sum(grad_probs * probs, axis=1, keepdims=True)
            grad_scores = (probs * (grad_probs - inner)).astype(BF)
            acc[0, :, s0:s1] += dot(grad_scores, keys * mask)
            acc[1, :, s0:s1] += t_dot(grad_scores, q)
        for s in range(3):
            value = acc[s] * scaling if s < 2 else acc[s]
            g3[s] = value.astype(BF)
        g3[3] = att[l]

    def backward(step, _):
        l = LAYERS - 1 - step

        @pl.when(step == 0)
        def _():
            gather_wait(gtop, zs2, zr2)

        @pl.when(step > 0)
        def _():
            gather_start(gtop)
            merge(0, 0, lax.rem(step + 1, 2))
            finish(l + 1, 1, 1)
            gather_wait(gtop)

        for h in range(2):

            def hidden(n):
                lanes = pl.ds(pl.multiple_of(n * 256, 256), 256)
                value = dot(gtop[...], wm[l, 2 + h, :, lanes]) * slope[l, h, :, lanes].astype(F32)
                low = value.astype(BF)
                gb[h, :, lanes] = low
                csum[l, pl.ds(2 + h, 1), lanes] = jnp.sum(
                    low.astype(F32), axis=0, keepdims=True
                )

            tiles(3, hidden)

        @pl.when(step > 0)
        def _():
            relay(0, 0)
            go_pass(2, out_hbm)

        def back_up(start, size):
            rows = pl.ds(start, size)
            value = dot_t(gb[0], wm[l, 0, rows, :]) + dot_t(gb[1], wm[l, 1, rows, :])
            part[:, pl.ds(start, size)] = value.astype(BF)

        features(back_up)
        scatter_start()
        transpose(gtop, 0)

        @pl.when(step > 0)
        def _():
            finish(l + 1, 0, 0)

        make(2, 0, lax.rem(step, 2), lambda b: 0, lambda b: hid.at[l, b], step > 0)
        scatter_wait()
        norm_backward(l, 1, gmid, 6 * l + 4)
        gather_start(gmid)
        merge(2, 0, lax.rem(step, 2))
        transpose(x2.at[l], 1)
        make(1, 1, lax.rem(step + 1, 2), lambda b: 1, lambda b: gb.at[b], step > 0)

        @pl.when(step == 0)
        def _():
            features(down(l, x2.at[LAYERS - 1]))

        relay(2, 0)
        gather_wait(gmid)

        @pl.when(step == 0)
        def _():
            scatter_start(side)

        merge(1, 1, lax.rem(step + 1, 2))
        da[...] = dot(gmid[...], wa[l, 3]).astype(BF)
        attend_back(l)
        relay(1, 1)
        for s in range(3):
            if s != 1:
                csum[l, s // 2 : s // 2 + 1, 0:PAD] = jnp.sum(
                    g3[s].astype(F32), axis=0, keepdims=True
                )

        def back_qkv(start, size):
            rows = pl.ds(start, size)
            value = dot_t(g3[0], wa[l, 0, rows, :])
            value = value + dot_t(g3[1], wa[l, 1, rows, :])
            value = value + dot_t(g3[2], wa[l, 2, rows, :])
            part[:, pl.ds(start, size)] = value.astype(BF)

        features(back_qkv)
        scatter_start()
        finish(l, 2, 0)
        transpose(x1.at[l], 0)
        transpose(gmid, 1)
        make(0, 0, lax.rem(step, 2), lambda s: s // 3, lambda s: g3[s], step >= 0)
        scatter_wait()
        norm_backward(l, 0, gtop, jnp.where(l > 0, 6 * l - 1, 12))

        @pl.when(step == 0)
        def _():
            scatter_wait(side)
            lax.fori_loop(0, CHUNK // 16, settle(l, recv2), 0)
            for k in range(N):
                oblk[k] = st[:, BLK * k : BLK * (k + 1)].astype(BF)
            go_start(2)

        return 0

    lax.fori_loop(0, LAYERS, backward, 0)

    merge(0, 0, (LAYERS - 1) % 2)
    go_wait(2, out_hbm)
    sent(2)
    for k in range(N):
        oblk[k] = gst[:, BLK * k : BLK * (k + 1)].astype(BF)
    go_start(3)

    def c_copy(k):
        return remote(csum, cx.at[k], cxs.at[k], cxr.at[k], (d, near[k], c))

    def v_copy(k):
        return remote(vb.at[near[k]], vx.at[k], vxs.at[k], vxr.at[k], (d, near[k], c))

    def z_copy(k):
        return remote(
            vz.at[c], vz.at[c], vzs.at[k], vzr.at[c], (d, r, lax.rem(c + k + 1, N))
        )

    for k in range(N):
        vb[k] = vsum[:, BLK * k : BLK * (k + 1)]
    for k in range(3):
        v_copy(k).start()
        c_copy(k).start()
    go_pass(3, tg_hbm)
    relay(0, 0)
    total = vb[r]
    for k in range(3):
        v_copy(k).wait_recv()
        total = total + vx[k]
    vz[c] = total
    for k in range(3):
        z_copy(k).start()
    for k in range(3):
        c_copy(k).wait()
    for l in range(LAYERS):
        csum[l] = csum[l] + cx[0, l] + cx[1, l] + cx[2, l]
    c_half = remote(csum.at[other], cd, cds.at[0], cds.at[1], (other, r, c))
    c_half.start()
    for cs in range(N):

        @pl.when(c != cs)
        def _():
            pltpu.make_async_copy(vz.at[cs], vz.at[cs], vzr.at[cs]).wait()

    total = vz[0]
    for cs in range(1, N):
        total = total + vz[cs]
    vd[0] = total
    v_half = remote(vd.at[0], vd.at[1], vds.at[0], vds.at[1], (other, r, c))
    v_half.start()
    finish(0, 1, 1)
    finish(0, 0, 0)
    c_half.wait()
    cout[...] = csum[d] + cd[...]
    v_half.wait()
    vout[...] = vd[0] + vd[1]
    for k in range(3):
        v_copy(k).wait_send()
        z_copy(k).wait_send()

    pl.semaphore_wait(credit, 2)
    go_wait(3, tg_hbm)
    for u in (0, 1, 3):
        sent(u)
    for i in range(3):
        for j in range(2):
            arrived = result(i, other, j)
            pltpu.make_async_copy(arrived, arrived, finr.at[i, j]).wait()
    for k in range(3):
        remote(vec_ref, pin.at[r], vs.at[k], vr.at[k], (d, near[k], c)).wait_send()
    for l in range(LAYERS):
        for i in range(3):
            for k in range(2):
                send_w(l, i, k).wait_send()
                pass_w(l, i, k).wait_send()
            for k in range(3):
                share_w(l, i, k).wait_send()


def fused(*operands):
    dma = pltpu.SemaphoreType.DMA
    vmem = pltpu.VMEM
    whole = pl.BlockSpec(memory_space=pltpu.VMEM)
    anywhere = pl.BlockSpec(memory_space=pl.ANY)
    scratch = [
        vmem((LAYERS, 4, D, PAD), BF),
        vmem((LAYERS, 4, D, HALF), BF),
        vmem((LAYERS, ROWS, D), BF),
        vmem((LAYERS, ROWS, D), BF),
        vmem((LAYERS, 3, ROWS, PAD), BF),
        vmem((LAYERS, ROWS, PAD), BF),
        vmem((LAYERS, ROWS, 128), F32),
        vmem((LAYERS, 2, ROWS, HALF), BF),
        vmem((LAYERS, 2, ROWS, HALF), BF),
        vmem((LAYERS, 2, CHUNK, D), F32),
        vmem((LAYERS, 2, CHUNK, 128), F32),
        vmem((ROWS, D), BF),
        vmem((ROWS, D), BF),
        vmem((2, D, ROWS), BF),
        vmem((ROWS, D), BF),
        vmem((N, CHUNK, D), BF),
        vmem((CHUNK, D), F32),
        vmem((CHUNK, D), F32),
        vmem((N, CHUNK, BLK), BF),
        vmem((N, CHUNK, BLK), BF),
        vmem((N, CHUNK, BLK), BF),
        vmem((4, N, CHUNK, BLK), BF),
        vmem((N, 16, BLK), F32),
        vmem((16, D), F32),
        vmem((2, ROWS, HALF), BF),
        vmem((ROWS, PAD), BF),
        vmem((4, ROWS, PAD), BF),
        vmem((3, ROWS, PAD), F32),
        vmem((2, BLK, HALF), BF),
        vmem((2, N, BLK, HALF), BF),
        vmem((2, N, BLK, HALF), BF),
        vmem((3, 2, BLK, HALF), BF),
        vmem((2, BLK, PAD), F32),
        vmem((3, 2, BLK // 2, HALF), BF),
        vmem((N, CHUNK, D), BF),
        vmem((16, D), F32),
        vmem((LAYERS, 4, HALF), F32),
        vmem((N, 16, BLK), F32),
        vmem((3, 16, BLK), F32),
        vmem((N, 16, BLK), F32),
        vmem((2, 16, BLK), F32),
        vmem((3, LAYERS, 4, HALF), F32),
        vmem((4, HALF), F32),
        dma((LAYERS, 3, 2)),
        dma((LAYERS, 3, 2)), dma((LAYERS, 3, 2)),
        dma((LAYERS, 3, 2)), dma((LAYERS, 3, 2)),
        dma((LAYERS, 3, 3)), dma((LAYERS, 3, 3)),
        dma((3,)), dma((4,)),
        dma((4, N)), dma((4, N)), dma((4, N)), dma((4, N)),
        dma((N,)), dma((N,)), dma((N,)), dma((N,)),
        dma((N,)), dma((2, N)), pltpu.SemaphoreType.REGULAR,
        dma((3, 2)), dma((3, 2)), dma((2,)), dma((3, 2)),
        dma((3, 2)), dma((3, 2)),
        dma((N,)), dma((N,)), dma((N,)), dma((N,)),
        dma((3,)), dma((3,)), dma((3,)), dma((N,)), dma((2,)),
        dma((3,)), dma((3,)), dma((2,)),
    ]
    shape = jax.ShapeDtypeStruct
    return pl.pallas_call(
        kernel,
        out_shape=(
            shape((ROWS, BLK), BF),
            shape((ROWS, BLK), BF),
            shape((4, BLK, PAD), F32),
            shape((BLK, 2 * HALF), F32),
            shape((BLK, 2 * HALF), F32),
            shape((16, BLK), F32),
            shape((4, HALF), F32),
        ),
        in_specs=[anywhere] * 5 + [whole] * 3,
        out_specs=(anywhere,) * 5 + (whole, whole),
        scratch_shapes=scratch,
        compiler_params=pltpu.CompilerParams(
            collective_id=0, has_side_effects=True, vmem_limit_bytes=67_043_328
        ),
    )(*operands)


def widen(values, axis=-1, to=PAD):
    axis = axis % values.ndim
    pads = [(0, 0)] * values.ndim
    pads[axis] = (0, to - values.shape[axis])
    return jnp.pad(values, pads)


def per_device_fused(
    tokens, cotangent, qkv_weight, qv_bias, proj_weight, proj_bias,
    up_weight, up_bias, down_weight, down_bias, norm_gain, norm_shift,
):
    dp = lax.axis_index("dp")
    tok = widen(tokens[0], 0, ROWS)
    cot = widen(cotangent[0], 0, ROWS)
    heads = jnp.concatenate(
        [qkv_weight.transpose(0, 2, 1, 3), proj_weight.transpose(0, 2, 1)[:, None]], axis=1
    )
    vec = jnp.concatenate(
        [norm_gain, norm_shift, proj_bias[:, None], down_bias[:, None]], axis=1
    ).reshape(12, BLK)
    vec = widen(vec, 0, 16)
    zero = jnp.zeros_like(qv_bias[:, 0])
    qb = widen(jnp.stack([qv_bias[:, 0], zero, qv_bias[:, 1]], axis=1))
    ub = up_bias.reshape(LAYERS, 2, HALF)
    down = down_weight.transpose(0, 2, 1)
    out, tg, ga, gu, gd, vout, cout = fused(tok, cot, widen(heads), up_weight, down, vec, qb, ub)
    both = vout[:12].reshape(LAYERS, 6, BLK)
    layer = lax.dynamic_slice(both, (dp, 0, 0), (1, 6, BLK))
    return (
        out[None, :SEQ].astype(F32),
        tg[None, :SEQ].astype(F32),
        ga[:3, :, :BLK].transpose(1, 0, 2)[None],
        cout[None, 0:2, :BLK],
        ga[3, :, :BLK].T[None],
        layer[:, 4],
        gu[None],
        cout[2:].reshape(1, 2 * HALF),
        gd.T[None],
        layer[:, 5],
        both[:, 0:2],
        both[:, 2:4],
    )


NORMAL = (((1,), (0,)), ((), ()))
LAST_BOTH = (((1,), (1,)), ((), ()))
FIRST_BOTH = (((0,), (0,)), ((), ()))


def gather_tokens(values):
    return lax.all_gather(values, "col", axis=0, tiled=True)


def gather_blocks(values):
    return lax.all_gather(values, "row", axis=0, tiled=True)


def gather_grad_blocks(values):
    return lax.all_gather(values, "row", axis=0, tiled=True)


def width_totals(first_sum, second_sum):
    return lax.psum((first_sum, second_sum), "row")


def gather_whole(triple_w, up_w, proj_w, down_w):
    row_whole = (triple_w, up_w, proj_w, down_w)
    col_whole = (proj_w, down_w, triple_w, up_w)
    return (row_whole, col_whole)


def row_product(gathered, matrix, contract):
    return lax.psum_scatter(
        lax.dot_general(gathered, matrix, contract, preferred_element_type=jnp.float32).astype(
            jnp.bfloat16
        ),
        "row",
        scatter_dimension=0,
        tiled=True,
    ).astype(jnp.float32)


def col_product(gathered, matrix, contract):
    return lax.psum_scatter(
        lax.dot_general(gathered, matrix, contract, preferred_element_type=jnp.float32).astype(
            jnp.bfloat16
        ),
        "col",
        scatter_dimension=0,
        tiled=True,
    ).astype(jnp.float32)


def norm_forward(stream, factor, shift):
    totals, squares = width_totals(jnp.sum(stream, axis=1), jnp.sum(stream * stream, axis=1))
    centre = totals / D
    spread = squares / D - centre * centre
    centred = stream - centre[:, None]
    scaling = lax.rsqrt(spread + EPSILON)
    standard = centred * scaling[:, None]
    return (standard * factor + shift, standard, scaling)


def norm_backward(grad_norm, standard, scaling, factor):
    factor_grad = jnp.sum(grad_norm * standard, axis=0)
    shift_grad = jnp.sum(grad_norm, axis=0)
    grad_standard = grad_norm * factor
    first_sum, second_sum = width_totals(
        jnp.sum(grad_standard, axis=1), jnp.sum(grad_standard * standard, axis=1)
    )
    grad_stream = scaling[:, None] * (
        grad_standard - first_sum[:, None] / D - standard * (second_sum[:, None] / D)
    )
    return (grad_stream, factor_grad, shift_grad)


def split_triple(triple_out, width):
    images = triple_out.shape[0] // SEQ
    head_count = width // HEAD_DIM
    pieces = triple_out.reshape(images, SEQ, 3, head_count, HEAD_DIM)
    return (pieces[:, :, 0], pieces[:, :, 1], pieces[:, :, 2])


def attend_forward(triple_out, width):
    queries, key_rows, values = split_triple(triple_out, width)
    scaling = HEAD_DIM ** (-0.5)
    scores = (
        jnp.einsum("bqhd,bkhd->bhqk", queries, key_rows, preferred_element_type=jnp.float32)
        * scaling
    )
    row_peak = jnp.max(scores, axis=-1, keepdims=True)
    log_totals = row_peak + jnp.log(jnp.sum(jnp.exp(scores - row_peak), axis=-1, keepdims=True))
    probs_low = jnp.exp(scores - log_totals).astype(jnp.bfloat16)
    attended = jnp.einsum("bhqk,bkhd->bqhd", probs_low, values, preferred_element_type=jnp.float32)
    return (attended.reshape(triple_out.shape[0], width).astype(jnp.bfloat16), log_totals)


def attend_backward(triple_out, log_totals, grad_attended, width):
    queries, key_rows, values = split_triple(triple_out, width)
    scaling = HEAD_DIM ** (-0.5)
    scores = (
        jnp.einsum("bqhd,bkhd->bhqk", queries, key_rows, preferred_element_type=jnp.float32)
        * scaling
    )
    probs = jnp.exp(scores - log_totals)
    probs_low = probs.astype(jnp.bfloat16)
    grad_heads = grad_attended.reshape(values.shape)
    grad_values = jnp.einsum(
        "bhqk,bqhd->bkhd", probs_low, grad_heads, preferred_element_type=jnp.float32
    )
    grad_probs = jnp.einsum(
        "bqhd,bkhd->bhqk", grad_heads, values, preferred_element_type=jnp.float32
    )
    grad_scores = (
        probs * (grad_probs - jnp.sum(grad_probs * probs, axis=-1, keepdims=True))
    ).astype(jnp.bfloat16)
    grad_queries = (
        jnp.einsum("bhqk,bkhd->bqhd", grad_scores, key_rows, preferred_element_type=jnp.float32)
        * scaling
    )
    grad_keys = (
        jnp.einsum("bhqk,bqhd->bkhd", grad_scores, queries, preferred_element_type=jnp.float32)
        * scaling
    )
    stacked = jnp.stack([grad_queries, grad_keys, grad_values], axis=2)
    return stacked.reshape(triple_out.shape[0], 3 * width).astype(jnp.bfloat16)


def layer_forward(stream, weights):
    qkv_w, qv_b, proj_w, proj_b, up_w, up_b, down_w, down_b, factors, shifts = weights
    width = qkv_w.shape[2]
    triple_w = qkv_w.reshape(qkv_w.shape[0], 3 * width)
    row_whole, col_whole = gather_whole(triple_w, up_w, proj_w, down_w)
    first_norm, first_standard, first_scaling = norm_forward(stream, factors[0], shifts[0])
    first_rows = gather_tokens(first_norm.astype(jnp.bfloat16))
    offsets = jnp.concatenate([qv_b[0], jnp.zeros_like(qv_b[0]), qv_b[1]])
    triple_out = (row_product(first_rows, triple_w, NORMAL) + offsets).astype(jnp.bfloat16)
    attended, log_totals = attend_forward(triple_out, width)
    head_rows = gather_blocks(attended)
    stream_mid = stream + col_product(head_rows, proj_w, NORMAL) + proj_b
    second_norm, second_standard, second_scaling = norm_forward(stream_mid, factors[1], shifts[1])
    second_rows = gather_tokens(second_norm.astype(jnp.bfloat16))
    before = row_product(second_rows, up_w, NORMAL) + up_b
    activated = jax.nn.gelu(before, approximate=False).astype(jnp.bfloat16)
    hidden_rows = gather_blocks(activated)
    branch_out = col_product(hidden_rows, down_w, NORMAL)
    stream_out = stream_mid + branch_out + down_b
    saved = (
        first_rows,
        first_standard,
        first_scaling,
        triple_out,
        log_totals,
        head_rows,
        second_rows,
        second_standard,
        second_scaling,
        before,
        hidden_rows,
        row_whole,
        col_whole,
    )
    return (stream_out, saved)


def layer_backward(grad_out, saved, weights):
    qkv_w, qv_b, proj_w, proj_b, up_w, up_b, down_w, down_b, factors, shifts = weights
    (
        first_rows,
        first_standard,
        first_scaling,
        triple_out,
        log_totals,
        head_rows,
        second_rows,
        second_standard,
        second_scaling,
        before,
        hidden_rows,
        row_whole,
        col_whole,
    ) = saved
    width = qkv_w.shape[2]
    triple_w = qkv_w.reshape(qkv_w.shape[0], 3 * width)
    grad_rows = gather_tokens(grad_out.astype(jnp.bfloat16))
    down_grad = lax.dot_general(
        hidden_rows, grad_rows, FIRST_BOTH, preferred_element_type=jnp.float32
    )
    down_off_grad = jnp.sum(grad_rows, axis=0, dtype=jnp.float32)
    grad_active = row_product(grad_rows, down_w, LAST_BOTH)
    _, slope_pull = jax.vjp(partial(jax.nn.gelu, approximate=False), before)
    grad_before = slope_pull(grad_active)[0].astype(jnp.bfloat16)
    before_rows = gather_grad_blocks(grad_before)
    up_grad = lax.dot_general(
        second_rows, before_rows, FIRST_BOTH, preferred_element_type=jnp.float32
    )
    up_off_grad = jnp.sum(before_rows, axis=0, dtype=jnp.float32)
    grad_second = col_product(before_rows, up_w, LAST_BOTH)
    grad_mid, second_factor_grad, second_shift_grad = norm_backward(
        grad_second, second_standard, second_scaling, factors[1]
    )
    grad_mid = grad_mid + grad_out
    mid_rows = gather_tokens(grad_mid.astype(jnp.bfloat16))
    proj_grad = lax.dot_general(head_rows, mid_rows, FIRST_BOTH, preferred_element_type=jnp.float32)
    proj_off_grad = jnp.sum(mid_rows, axis=0, dtype=jnp.float32)
    grad_attended = row_product(mid_rows, proj_w, LAST_BOTH).astype(jnp.bfloat16)
    grad_triple = attend_backward(triple_out, log_totals, grad_attended, width)
    triple_rows = gather_grad_blocks(grad_triple)
    triple_grad = lax.dot_general(
        first_rows, triple_rows, FIRST_BOTH, preferred_element_type=jnp.float32
    )
    column_sums = jnp.sum(triple_rows, axis=0, dtype=jnp.float32).reshape(3, width)
    qv_grad = jnp.stack([column_sums[0], column_sums[2]])
    grad_first = col_product(triple_rows, triple_w, LAST_BOTH)
    grad_in, first_factor_grad, first_shift_grad = norm_backward(
        grad_first, first_standard, first_scaling, factors[0]
    )
    grad_in = grad_in + grad_mid
    factor_grads = jnp.stack([first_factor_grad, second_factor_grad])
    shift_grads = jnp.stack([first_shift_grad, second_shift_grad])
    layer_grads = (
        triple_grad.reshape(qkv_w.shape),
        qv_grad,
        proj_grad,
        proj_off_grad,
        up_grad,
        up_off_grad,
        down_grad,
        down_off_grad,
        factor_grads,
        shift_grads,
    )
    return (grad_in, layer_grads)


def per_device_plain(
    tokens,
    cotangent,
    qkv_weight,
    qv_bias,
    proj_weight,
    proj_bias,
    up_weight,
    up_bias,
    down_weight,
    down_bias,
    norm_gain,
    norm_shift,
):
    image_count, seq_len, width_row = tokens.shape
    stream = tokens.reshape(image_count * seq_len, width_row).astype(jnp.float32)
    layer_params = []
    saved_list = []
    for layer_index in range(LAYERS):
        params = (
            qkv_weight[layer_index],
            qv_bias[layer_index],
            proj_weight[layer_index],
            proj_bias[layer_index],
            up_weight[layer_index],
            up_bias[layer_index],
            down_weight[layer_index],
            down_bias[layer_index],
            norm_gain[layer_index],
            norm_shift[layer_index],
        )
        layer_params.append(params)
        stream, saved = layer_forward(stream, params)
        saved_list.append(saved)
    grad_stream = cotangent.reshape(image_count * seq_len, width_row).astype(jnp.float32)
    per_layer = [None] * LAYERS
    for layer_index in reversed(range(LAYERS)):
        grad_stream, layer_grads = layer_backward(
            grad_stream, saved_list[layer_index], layer_params[layer_index]
        )
        per_layer[layer_index] = layer_grads
    stacked = tuple(
        (jnp.stack([layer_grads[position] for layer_grads in per_layer]) for position in range(10))
    )
    summed = (
        lax.psum_scatter(
            stacked[0].astype(jnp.bfloat16), "dp", scatter_dimension=0, tiled=True
        ).astype(jnp.float32),
        lax.psum_scatter(
            stacked[1].astype(jnp.bfloat16), "dp", scatter_dimension=0, tiled=True
        ).astype(jnp.float32),
        lax.psum_scatter(
            stacked[2].astype(jnp.bfloat16), "dp", scatter_dimension=0, tiled=True
        ).astype(jnp.float32),
        lax.psum_scatter(
            stacked[3].astype(jnp.bfloat16), "dp", scatter_dimension=0, tiled=True
        ).astype(jnp.float32),
        lax.psum_scatter(
            stacked[4].astype(jnp.bfloat16), "dp", scatter_dimension=0, tiled=True
        ).astype(jnp.float32),
        lax.psum_scatter(
            stacked[5].astype(jnp.bfloat16), "dp", scatter_dimension=0, tiled=True
        ).astype(jnp.float32),
        lax.psum_scatter(
            stacked[6].astype(jnp.bfloat16), "dp", scatter_dimension=0, tiled=True
        ).astype(jnp.float32),
        lax.psum_scatter(
            stacked[7].astype(jnp.bfloat16), "dp", scatter_dimension=0, tiled=True
        ).astype(jnp.float32),
    )
    norm_sums = lax.psum((stacked[8], stacked[9]), ("dp", "col"))
    result = stream.reshape(image_count, seq_len, width_row)
    tokens_grad = grad_stream.reshape(image_count, seq_len, width_row)
    return (
        result,
        tokens_grad,
        summed[0],
        summed[1],
        summed[2],
        summed[3],
        summed[4],
        summed[5],
        summed[6],
        summed[7],
        norm_sums[0],
        norm_sums[1],
    )


def solution(mesh):
    placed = (
        P(("dp", "col"), None, "row"),
        P(("dp", "col"), None, "row"),
        P(None, "row", None, "col"),
        P(None, None, "col"),
        P(None, "col", "row"),
        P(None, "row"),
        P(None, "row", "col"),
        P(None, "col"),
        P(None, "col", "row"),
        P(None, "row"),
        P(None, None, "row"),
        P(None, None, "row"),
    )
    sizes = (mesh.shape["dp"], mesh.shape["row"], mesh.shape["col"])
    return jax.shard_map(
        per_device_fused if sizes == (2, N, N) else per_device_plain,
        mesh=mesh,
        in_specs=placed,
        out_specs=(
            P(("dp", "col"), None, "row"),
            P(("dp", "col"), None, "row"),
            P("dp", "row", None, "col"),
            P("dp", None, "col"),
            P("dp", "col", "row"),
            P("dp", "row"),
            P("dp", "row", "col"),
            P("dp", "col"),
            P("dp", "col", "row"),
            P("dp", "row"),
            P(None, None, "row"),
            P(None, None, "row"),
        ),
        check_vma=False,
    )
```

```python
from functools import partial

import jax
import jax.numpy as jnp
from jax import lax
from jax.experimental import pallas as pl
from jax.experimental.pallas import tpu as pltpu
from jax.sharding import PartitionSpec as P

D = 1408
HEAD_DIM = 88
SEQ = 257
LAYERS = 2
EPSILON = 1e-06
MESH = pl.DeviceIdType.MESH
BF = jnp.bfloat16
F32 = jnp.float32

ROWS = 272
STEP = 64
CHUNK = 80
LAST = 72
BLK = 352
PAD = 384
HALF = 768
N = 4


def dot(a, b):
    return jnp.dot(a, b, preferred_element_type=F32)


def dot_t(a, b):
    return lax.dot_general(a, b, (((1,), (1,)), ((), ())), preferred_element_type=F32)


def t_dot(a, b):
    return lax.dot_general(a, b, (((0,), (0,)), ((), ())), preferred_element_type=F32)


def span(index):
    return pl.ds(STEP * index, STEP if index < N - 1 else LAST)


def head_span(head):
    low, high = HEAD_DIM * head, HEAD_DIM * (head + 1)
    return low, high, low // 128 * 128, -(-high // 128) * 128


def kernel(
    tok_hbm, cot_hbm, wa_hbm, up_hbm, down_hbm, vec_ref, qb_ref, ub_ref,
    out_hbm, tg_hbm, ga_hbm, gu_hbm, gd_hbm, vout, cout,
    wa, wm, x1, x2, triple, att, lse, hid, slope, std, inv,
    gtop, gmid, lt, part, recv, st, gst, tin, cin, oblk, mid, pin, pv,
    gb, da, g3, acc, sbuf, prx, keep, ici, fin, hop, rb, rb2, recv2,
    vsum, csum, vb, vx, vz, vd, cx, cd,
    wloc, wsend, wrecv, fsend, frecv, psend, precv, vs, vr, m1s, m1r, m2s, m2r,
    zs, zr, rss, rsr, lr, cs_s, cs_r, credit, gis, gir, fins, finr, hs, hr,
    zs2, zr2, rss2, rsr2, lr2, vxs, vxr, vzs, vzr, vds, cxs, cxr, cds,
):
    d, r, c = lax.axis_index("dp"), lax.axis_index("row"), lax.axis_index("col")
    other = 1 - d
    near = (r + 1 - 2 * lax.rem(r, 2), lax.rem(r + 2, N), N - 1 - r)
    last = c == N - 1

    def remote(src, dst, ssem, rsem, dev):
        return pltpu.make_async_remote_copy(
            src, dst, ssem, rsem, device_id=dev, device_id_type=MESH
        )

    def rblk(index):
        return pl.ds(pl.multiple_of(index * BLK, 16), BLK)

    def rhalf(index, part_):
        return pl.ds(pl.multiple_of(index * BLK + part_ * (BLK // 2), 16), BLK // 2)

    recv[...] = jnp.zeros_like(recv)
    recv2[...] = jnp.zeros_like(recv2)
    for array in (x1.at[0], x1.at[1], x2.at[0], x2.at[1], gtop, gmid):
        array[ROWS - 16 :, :] = jnp.zeros((16, D), BF)
    tin[...] = jnp.zeros_like(tin)
    cin[...] = jnp.zeros_like(cin)
    vsum[...] = jnp.zeros_like(vsum)
    csum[...] = jnp.zeros_like(csum)
    barrier = pltpu.get_barrier_semaphore()
    for k in range(N * N):
        pl.semaphore_signal(
            barrier, inc=1,
            device_id=(d, lax.rem(r + k // N, N), lax.rem(c + k % N, N)), device_id_type=MESH,
        )
    pl.semaphore_signal(barrier, inc=1, device_id=(other, r, c), device_id_type=MESH)
    pl.semaphore_wait(barrier, N * N + 1)

    for k in range(3):
        remote(vec_ref, pin.at[r], vs.at[k], vr.at[k], (d, near[k], c)).start()
    own_vec = pltpu.make_async_copy(vec_ref, pin.at[r], vr.at[3])
    own_vec.start()

    def by_size(body):
        @pl.when(last)
        def _():
            body(LAST)

        @pl.when(jnp.logical_not(last))
        def _():
            body(STEP)

    def come_start(u, src):
        for ct in range(N):
            size = STEP if ct < N - 1 else LAST
            source, target = src.at[span(ct)], mid.at[u, c, pl.ds(0, size)]

            @pl.when(c == ct)
            def _():
                pltpu.make_async_copy(source, target, m1r.at[u, c]).start()

            @pl.when(c != ct)
            def _():
                remote(source, target, m1s.at[u, ct], m1r.at[u, c], (d, r, ct)).start()

    def come_pass(u, dst):
        def sized(size):
            rows = pl.ds(0, size)
            for p in range(N):
                source, target = mid.at[u, p, rows], dst.at[r, rows]
                pltpu.make_async_copy(source, source, m1r.at[u, p]).wait()

                @pl.when(r == p)
                def _():
                    pltpu.make_async_copy(source, target, m2r.at[u, r]).start()

                @pl.when(r != p)
                def _():
                    remote(source, target, m2s.at[u, p], m2r.at[u, r], (d, p, c)).start()

        by_size(sized)

    def come_wait(u, dst):
        def sized(size):
            for rs in range(N):
                rows = dst.at[rs, pl.ds(0, size)]
                pltpu.make_async_copy(rows, rows, m2r.at[u, rs]).wait()

        by_size(sized)

    def go_start(u):
        def sized(size):
            rows = pl.ds(0, size)
            for k in range(N):
                source, target = oblk.at[k, rows], mid.at[u, r, rows]

                @pl.when(r == k)
                def _():
                    pltpu.make_async_copy(source, target, m1r.at[u, r]).start()

                @pl.when(r != k)
                def _():
                    remote(source, target, m1s.at[u, k], m1r.at[u, r], (d, k, c)).start()

        by_size(sized)

    def go_pass(u, dst):
        def sized(size):
            for p in range(N):
                source = mid.at[u, p, pl.ds(0, size)]
                target = dst.at[pl.ds(pl.multiple_of(STEP * c, 16), size)]
                pltpu.make_async_copy(source, source, m1r.at[u, p]).wait()

                @pl.when(c == p)
                def _():
                    pltpu.make_async_copy(source, target, m2r.at[u, c]).start()

                @pl.when(c != p)
                def _():
                    remote(source, target, m2s.at[u, p], m2r.at[u, c], (d, r, p)).start()

        by_size(sized)

    def go_wait(u, dst):
        for cs in range(N):
            rows = dst.at[span(cs)]
            pltpu.make_async_copy(rows, rows, m2r.at[u, cs]).wait()

    def sent(u):
        for ct in range(N):
            size = STEP if ct < N - 1 else LAST
            rows = mid.at[u, 0, pl.ds(0, size)]

            if u < 2:

                @pl.when(c != ct)
                def _():
                    remote(rows, rows, m1s.at[u, ct], m1r.at[u, 0], (d, r, ct)).wait_send()

            def second(size):
                rows = mid.at[u, 0, pl.ds(0, size)]
                first_row = u < 2

                @pl.when((r != ct) if first_row else (c != ct))
                def _():
                    remote(rows, rows, m2s.at[u, ct], m2r.at[u, 0], (d, r, c)).wait_send()

                if not first_row:

                    @pl.when(r != ct)
                    def _():
                        remote(rows, rows, m1s.at[u, ct], m1r.at[u, 0], (d, ct, c)).wait_send()

            by_size(second)

    come_start(0, tok_hbm)

    def source_w(l, i, which, rows):
        if i == 0:
            return wa_hbm.at[l, pl.ds(2 * which, 2), rows, :]
        lanes = pl.ds(pl.multiple_of(HALF * which, 128), HALF)
        return (up_hbm if i == 1 else down_hbm).at[l, rows, lanes]

    def rows_w(l, i, which, block):
        if i == 0:
            return wa.at[l, pl.ds(2 * which, 2), block, :]
        return wm.at[l, 2 * (i - 1) + which, block, :]

    def local_w(l, i, which):
        return pltpu.make_async_copy(
            source_w(l, i, which, pl.ds(0, BLK)), rows_w(l, i, which, rblk(r)), wloc.at[l, i, which]
        )

    def send_w(l, i, k, h):
        return remote(
            source_w(l, i, d, pl.ds(h * (BLK // 2), BLK // 2)), rows_w(l, i, d, rhalf(r, h)),
            wsend.at[l, i, k, h], wrecv.at[l, i, k, h], (d, near[k], c),
        )

    def pass_w(l, i, k):
        rows = rows_w(l, i, d, rhalf(near[k], k))
        return remote(rows, rows, fsend.at[l, i, k], frecv.at[l, i, k], (d, near[1 - k], c))

    def share_w(l, i, k):
        rows = rows_w(l, i, d, rblk(near[k]))
        return remote(rows, rows, psend.at[l, i, k], precv.at[l, i, k], (other, r, c))

    def direct_w(l, i, parts=(0, 1)):
        for part_ in parts:
            for k in range(2):
                send_w(l, i, k, k if part_ == 0 else 1 - k).start()

    def stage_w(l, i):
        for k in range(2):
            send_w(l, i, k, k).wait_recv()
            pass_w(l, i, k).start()
        for k in range(2):
            send_w(l, i, k, 1 - k).wait_recv()
            share_w(l, i, k).start()

    def close_w(l, i):
        for k in range(2):
            rows = rows_w(l, i, d, rhalf(near[2], k))
            pltpu.make_async_copy(rows, rows, frecv.at[l, i, k]).wait()
        share_w(l, i, 2).start()

    def need_w(l, i):
        for which in range(2):
            local_w(l, i, which).wait()
        for k in range(3):
            rows = rows_w(l, i, other, rblk(near[k]))
            pltpu.make_async_copy(rows, rows, precv.at[l, i, k]).wait()

    direct_w(0, 0, (0,))
    come_pass(0, tin)
    direct_w(0, 0, (1,))
    come_start(1, cot_hbm)
    for l in range(LAYERS):
        for i in range(3):
            for which in range(2):
                local_w(l, i, which).start()

    def half_rows(cs, h):
        return pl.ds(STEP * cs + 32 * h, 32 if h == 0 or cs < N - 1 else LAST - 32)

    halves = ((0, 0), (1, 0), (0, 1), (1, 1))
    targets = ((2, 1), (2, 0), (1, 3), (1, 2))
    relays = ((1, 0, [(2 + far, h) for far, h in halves]), (2, 3, [(1 - far, h) for far, h in halves]))

    first_z, second_z = (zs, zr), (zs2, zr2)

    def gather_start(x, sems=first_z):
        zs, zr = sems
        for c0 in range(N):

            @pl.when(c == c0)
            def _():
                for n in range(4):
                    rows = x.at[half_rows(c0, n % 2)]
                    remote(
                        rows, rows, zs.at[n], zr.at[c0, n % 2], (d, r, targets[c0][n // 2])
                    ).start()

    def gather_pass(x, *steps, sems=first_z):
        zs, zr = sems
        for c0, far, order in relays:

            @pl.when(c == c0)
            def _():
                for n in steps:
                    cs, h = order[n]
                    rows = x.at[half_rows(cs, h)]
                    pltpu.make_async_copy(rows, rows, zr.at[cs, h]).wait()
                    remote(rows, rows, zs.at[4 + n], zr.at[cs, h], (d, r, far)).start()

    def gather_wait(x, sems=first_z):
        zs, zr = sems
        for c0 in range(N):
            passed = [order for at, _, order in relays if at == c0]

            @pl.when(c == c0)
            def _():
                for cs in range(N):
                    for h in range(2):
                        if cs != c0 and not (passed and (cs, h) in passed[0]):
                            rows = x.at[half_rows(cs, h)]
                            pltpu.make_async_copy(rows, rows, zr.at[cs, h]).wait()
                for n in range(4):
                    rows = x.at[half_rows(c0, n % 2)]
                    remote(rows, rows, zs.at[n], zr.at[c0, 0], (d, r, targets[c0][0])).wait_send()
                if passed:
                    for n, (cs, h) in enumerate(passed[0]):
                        rows = x.at[half_rows(cs, h)]
                        remote(rows, rows, zs.at[4 + n], zr.at[cs, h], (d, r, 0)).wait_send()

    sides = ((0, 1, (3, 2)), (3, 2, (0, 1)))
    inner = ((1, 0), (2, 3))

    def size_of(cs):
        return STEP if cs < N - 1 else LAST

    def cols(h):
        return pl.ds(0, HALF) if h == 0 else pl.ds(HALF, D - HALF)

    main = (part, rb, recv, rss, rsr, lr)
    side = (x2.at[LAYERS - 1], rb2, recv2, rss2, rsr2, lr2)

    def end_copy(n, h, middle, dest, path):
        part, rb, recv, rss, rsr, lr = path
        return remote(
            part.at[span(dest), cols(h)], rb.at[n, pl.ds(0, size_of(dest)), cols(h)],
            rss.at[2 * n + h], lr.at[n, h], (d, r, middle),
        )

    def single_copy(dest, h, path):
        part, rb, recv, rss, rsr, lr = path
        return remote(
            part.at[span(dest), cols(h)], recv.at[1, pl.ds(0, size_of(dest)), cols(h)],
            rss.at[4 + h], rsr.at[h], (d, r, dest),
        )

    def sum_copy(n, h, dest, path):
        part, rb, recv, rss, rsr, lr = path
        rows = pl.ds(0, size_of(dest))
        return remote(
            rb.at[n, rows, cols(h)], recv.at[2, rows, cols(h)], rss.at[6 + 2 * n + h],
            rsr.at[2 + h], (d, r, dest),
        )

    def add_start(h, path=main):
        for end, middle, dests in sides:

            @pl.when(c == end)
            def _():
                for n in range(2):
                    end_copy(n, h, middle, dests[n], path).start()
                single_copy(middle, h, path).start()

        for middle, end in inner:

            @pl.when(c == middle)
            def _():
                single_copy(end, h, path).start()

        for cs in range(N):

            @pl.when(c == cs)
            def _():
                path[2][0, 0 : size_of(cs), cols(h)] = path[0][span(cs), cols(h)]

    def add_pass(*steps, path=main):
        part, rb, recv, rss, rsr, lr = path
        for end, middle, dests in sides:

            @pl.when(c == middle)
            def _():
                for step in steps:
                    h, n = step // 2, step % 2
                    dest = dests[n]
                    size = size_of(dest)
                    rows = rb.at[n, pl.ds(0, size), cols(h)]
                    pltpu.make_async_copy(rows, rows, lr.at[n, h]).wait()
                    for start in range(0, size, 16):
                        width = min(16, size - start)
                        mine = part[pl.ds(STEP * dest + start, width), cols(h)]
                        value = rb[n, start : start + width, cols(h)].astype(F32)
                        rb[n, start : start + width, cols(h)] = (
                            value + mine.astype(F32)
                        ).astype(BF)
                    sum_copy(n, h, dest, path).start()

    def add_wait(path=main):
        part, rb, recv, rss, rsr, lr = path
        for cs in range(N):

            @pl.when(c == cs)
            def _():
                for k in (1, 2):
                    for h in range(2):
                        rows = recv.at[k, pl.ds(0, size_of(cs)), cols(h)]
                        pltpu.make_async_copy(rows, rows, rsr.at[2 * (k - 1) + h]).wait()

        for end, middle, dests in sides:

            @pl.when(c == end)
            def _():
                for h in range(2):
                    for n in range(2):
                        end_copy(n, h, middle, dests[n], path).wait_send()
                    single_copy(middle, h, path).wait_send()

            @pl.when(c == middle)
            def _():
                for h in range(2):
                    single_copy(end, h, path).wait_send()
                    for n in range(2):
                        sum_copy(n, h, dests[n], path).wait_send()

    def received(rows, recv=recv):
        total = recv[0, rows, :].astype(F32)
        for k in range(1, recv.shape[0]):
            total = total + recv[k, rows, :].astype(F32)
        return total

    def vector(row):
        return pv[pl.ds(row, 1), :]

    def own_rows(x, t, value):
        @pl.when(jnp.logical_or(t < 4, last))
        def _():
            x[pl.ds(pl.multiple_of(STEP * c + 16 * t, 16), 16), :] = value

    valid = jnp.where(last, SEQ - STEP * (N - 1), STEP)

    def masked(t, value):
        index = lax.broadcasted_iota(jnp.int32, (16, 1), 0) + 16 * t
        return jnp.where(index < valid, value, 0.0)

    def norm_forward(l, j, x, extra):
        def body(t, _):
            rows = pl.ds(pl.multiple_of(16 * t, 16), 16)
            v = extra(rows)
            st[rows, :] = v
            centre = jnp.sum(v, axis=1, keepdims=True) / D
            spread_ = jnp.sum(v * v, axis=1, keepdims=True) / D - centre * centre
            scale = lax.rsqrt(spread_ + EPSILON)
            standard = (v - centre) * scale
            std[l, j, rows, :] = standard
            inv[l, j, rows, :] = jnp.broadcast_to(scale, (16, 128))
            value = standard * vector(6 * l + j) + vector(6 * l + 2 + j)
            own_rows(x, t, value.astype(BF))
            return 0

        lax.fori_loop(0, CHUNK // 16, body, 0)

    def norm_backward(l, j, x, bias_row):
        def body(t, _):
            rows = pl.ds(pl.multiple_of(16 * t, 16), 16)
            e = received(rows)
            standard = std[l, j, rows, :]
            gain_term = masked(t, e * standard)
            vsum[pl.ds(6 * l + j, 1), :] += jnp.sum(gain_term, axis=0, keepdims=True)
            vsum[pl.ds(6 * l + 2 + j, 1), :] += jnp.sum(masked(t, e), axis=0, keepdims=True)
            f = e * vector(6 * l + j)
            first = jnp.sum(f, axis=1, keepdims=True) / D
            second = jnp.sum(f * standard, axis=1, keepdims=True) / D
            scale = inv[l, j, rows, 0:1]
            grad = gst[rows, :] + scale * (f - first - standard * second)
            gst[rows, :] = grad
            if x is not None:
                low = grad.astype(BF)
                own_rows(x, t, low)
                vsum[pl.ds(bias_row, 1), :] += jnp.sum(
                    masked(t, low.astype(F32)), axis=0, keepdims=True
                )
            return 0

        lax.fori_loop(0, CHUNK // 16, body, 0)

    def tiles(count, body):
        lax.fori_loop(0, count, lambda n, _: (body(n), 0)[1], 0)

    def features(body, start=None):
        tiles(3, lambda n: body(pl.multiple_of(n * 256, 256), 256))
        if start is not None:
            start(0)
        tiles(2, lambda n: body(pl.multiple_of(HALF + n * 256, 256), 256))
        body(1280, 128)
        if start is not None:
            start(1)

    def assemble(src, dst):
        for k in range(N):
            dst[:, BLK * k : BLK * (k + 1)] = src[k, :, 0:BLK].astype(F32)

    for k in range(3):
        remote(vec_ref, pin.at[r], vs.at[k], vr.at[k], (d, near[k], c)).wait_recv()
    own_vec.wait()
    assemble(pin, pv)
    come_wait(0, tin)
    come_pass(1, cin)
    assemble(tin, st)

    lane = lax.broadcasted_iota(jnp.int32, (1, PAD), 1)
    key_ok = lax.broadcasted_iota(jnp.int32, (1, ROWS), 1) < SEQ
    scaling = HEAD_DIM**-0.5

    def head_mask(head):
        low, high, s0, s1 = head_span(head)
        lanes = lane[:, s0:s1]
        return jnp.logical_and(lanes >= low, lanes < high).astype(BF), s0, s1

    def attend(l):
        acc[0] = jnp.zeros((ROWS, PAD), F32)
        for head in range(4):
            mask, s0, s1 = head_mask(head)
            q = triple[l, 0, :, s0:s1] * mask
            scores = dot_t(q, triple[l, 1, :, s0:s1]) * scaling
            scores = jnp.where(key_ok, scores, -1e30)
            peak = jnp.max(scores, axis=1, keepdims=True)
            total = peak + jnp.log(jnp.sum(jnp.exp(scores - peak), axis=1, keepdims=True))
            lse[l, :, head : head + 1] = total
            probs = jnp.exp(scores - total).astype(BF)
            acc[0, :, s0:s1] += dot(probs, triple[l, 2, :, s0:s1] * mask)
        att[l] = acc[0].astype(BF)

    def down(l, target):
        def body(start, size):
            rows = pl.ds(start, size)
            value = dot_t(hid[l, 0], wm[l, 2, rows, :]) + dot_t(hid[l, 1], wm[l, 3, rows, :])
            target[:, rows] = value.astype(BF)

        return body

    def settle(l, recv):
        def body(t, _):
            rows = pl.ds(pl.multiple_of(16 * t, 16), 16)
            st[rows, :] = st[rows, :] + received(rows, recv) + vector(6 * l + 5)
            return 0

        return body

    def top_rows(t, _):
        rows = pl.ds(pl.multiple_of(16 * t, 16), 16)
        low = gst[rows, :].astype(BF)
        own_rows(gtop, t, low)
        vsum[pl.ds(6 * (LAYERS - 1) + 5, 1), :] += jnp.sum(
            masked(t, low.astype(F32)), axis=0, keepdims=True
        )
        return 0

    def forward(l, _):
        def take(rows):
            return st[rows, :]

        norm_forward(l, 0, x1.at[l], take)
        gather_start(x1.at[l])

        @pl.when(l == 0)
        def _():
            stage_w(0, 0)
            direct_w(0, 1)

        gather_pass(x1.at[l], 0, 1, 2, 3)

        @pl.when(l == 0)
        def _():
            close_w(0, 0)

        gather_wait(x1.at[l])

        @pl.when(l == 0)
        def _():
            come_wait(1, cin)
            assemble(cin, gst)
            lax.fori_loop(0, CHUNK // 16, top_rows, 0)
            gather_start(gtop, second_z)

        need_w(l, 0)

        def qkv(s):
            value = dot(x1[l], wa[l, s]) + qb_ref[l, pl.ds(s, 1), :]
            triple[l, s] = value.astype(BF)

        tiles(3, qkv)
        attend(l)
        stage_w(l, 1)
        direct_w(l, 2)

        def proj(start, size):
            value = dot_t(att[l], wa[l, 3, pl.ds(start, size), :])
            part[:, pl.ds(start, size)] = value.astype(BF)

        features(proj, add_start)
        add_pass(0, 1, 2, 3)
        close_w(l, 1)
        add_wait()
        norm_forward(
            l, 1, x2.at[l], lambda rows: st[rows, :] + received(rows) + vector(6 * l + 4)
        )
        gather_start(x2.at[l])
        gather_pass(x2.at[l], 0, 1)
        stage_w(l, 2)

        @pl.when(l == 0)
        def _():
            direct_w(1, 0)

        gather_pass(x2.at[l], 2, 3)
        gather_wait(x2.at[l])
        close_w(l, 2)
        need_w(l, 1)

        @pl.when(l == 0)
        def _():
            gather_pass(gtop, 0, 1, 2, 3, sems=second_z)


        for h in range(2):

            def up(n):
                lanes = pl.ds(pl.multiple_of(n * 256, 256), 256)
                before = dot(x2[l], wm[l, h, :, lanes]) + ub_ref[l, pl.ds(h, 1), lanes]
                half = before * (0.5**0.5)
                cdf = 0.5 + 0.5 * lax.erf(half)
                hid[l, h, :, lanes] = (before * cdf).astype(BF)
                density = jnp.exp(-half * half) * 0.3989422804014327
                slope[l, h, :, lanes] = (cdf + before * density).astype(slope.dtype)

            tiles(3, up)
        need_w(l, 2)

        @pl.when(l == 0)
        def _():
            features(down(l, part), add_start)
            stage_w(1, 0)
            direct_w(1, 1)
            add_pass(0, 1, 2, 3)
            close_w(1, 0)
            add_wait()
            lax.fori_loop(0, CHUNK // 16, settle(l, recv), 0)

        return 0

    lax.fori_loop(0, LAYERS, forward, 0)

    def transpose(src, index):
        def body(n):
            lanes = pl.ds(pl.multiple_of(n * 128, 128), 128)
            lt[index, lanes, :] = src[:, lanes].T

        tiles(D // 128, body)

    def piece(turn, k):
        return remote(
            sbuf.at[lax.rem(k, 2)], prx.at[turn, k], cs_s.at[k], cs_r.at[turn, k], (other, r, c)
        )

    def block_tile(ref, i, b, k, left, right):
        rows = rblk(k)
        for j in range(2):
            lanes = pl.ds(PAD * j, PAD)
            if i == 0:
                s = 2 * b + j
                value = dot(lt[left(s), rows, :], right(s))
            else:
                value = dot(lt[left(b), rows, :], right(b)[:, lanes])
            ref[:, lanes] = value.astype(BF)

    def strips(count, body):
        def strip(t, _):
            body(pl.ds(pl.multiple_of(16 * t, 16), 16))
            return 0

        lax.fori_loop(0, count // 16, strip, 0)

    def make_send(i, turn, left, right, wait_credit):
        @pl.when(wait_credit)
        def _():
            pl.semaphore_wait(credit, 1)

        def send_tile(k):
            @pl.when(k >= 2)
            def _():
                piece(turn, k - 2).wait_send()

            block_tile(sbuf.at[lax.rem(k, 2)], i, other, k, left, right)
            piece(turn, k).start()

        tiles(N, send_tile)

    def make_keep(i, slot, turn, left, right, first):
        def keep_tile(k):
            block_tile(keep.at[slot, 2 * first + k], i, d, 2 * first + k, left, right)

        tiles(2, keep_tile)
        if first == 1:
            for k in (2, 3):
                piece(turn, k).wait_send()

    def half_copy(i, slot, k):
        half = pl.ds(k * (BLK // 2), BLK // 2)
        return remote(
            keep.at[slot, near[2], half], hop.at[i, k], hs.at[i, k], hr.at[i, k], (d, near[k], c)
        )

    def block_copy(i, slot, k):
        return remote(
            keep.at[slot, near[k]], ici.at[i, k], gis.at[i, k], gir.at[i, k], (d, near[k], c)
        )

    def merge(i, slot, turn):
        def add(k):
            rows = prx.at[turn, k]
            pltpu.make_async_copy(rows, rows, cs_r.at[turn, k]).wait()

            def strip(rows):
                value = keep[slot, k, rows, :].astype(F32) + prx[turn, k, rows, :].astype(F32)
                keep[slot, k, rows, :] = value.astype(BF)

            strips(BLK, strip)

        add(near[2])
        for k in range(2):
            half_copy(i, slot, k).start()
        for k in (near[0], near[1], r):
            add(k)
        pl.semaphore_signal(credit, inc=1, device_id=(other, r, c), device_id_type=MESH)

    def relay(i, slot):
        for k in range(2):
            pltpu.make_async_copy(hop.at[i, k], hop.at[i, k], hr.at[i, k]).wait()
            block = near[1 - k]

            def strip(t, _):
                rows = pl.ds(pl.multiple_of(16 * t, 16), 16)
                half = pl.ds(pl.multiple_of(k * (BLK // 2) + 16 * t, 16), 16)
                value = keep[slot, block, half, :].astype(F32) + hop[i, k, rows, :].astype(F32)
                keep[slot, block, half, :] = value.astype(BF)
                return 0

            lax.fori_loop(0, BLK // 32, strip, 0)
            block_copy(i, slot, 1 - k).start()

    def result(i, which, j):
        if i == 0:
            return ga_hbm.at[2 * which + j]
        lanes = pl.ds(pl.multiple_of(HALF * which + PAD * j, 128), PAD)
        return (gu_hbm if i == 1 else gd_hbm).at[:, lanes]

    def finish(l, i, slot):
        for k in range(2):
            arrived = ici.at[i, k]
            pltpu.make_async_copy(arrived, arrived, gir.at[i, k]).wait()

        def body(t, _):
            rows = pl.ds(pl.multiple_of(16 * t, 16), 16)
            total = keep[slot, r, rows, :].astype(F32)
            for k in range(2):
                total = total + ici[i, k, rows, :].astype(F32)
            fin[0, rows, :] = total[:, 0:PAD]
            fin[1, rows, :] = total[:, PAD : 2 * PAD]
            return 0

        lax.fori_loop(0, BLK // 16, body, 0)

        @pl.when(l == d)
        def _():
            copies = [
                pltpu.make_async_copy(fin.at[j], result(i, d, j), fins.at[j]) for j in range(2)
            ]
            for copy in copies:
                copy.start()
            for copy in copies:
                copy.wait()

        @pl.when(l != d)
        def _():
            copies = [
                remote(fin.at[j], result(i, d, j), fins.at[j], finr.at[i, j], (other, r, c))
                for j in range(2)
            ]
            for copy in copies:
                copy.start()
            for copy in copies:
                copy.wait_send()

        for k in range(2):
            half_copy(i, slot, k).wait_send()
            block_copy(i, slot, k).wait_send()

    def attend_back(l):
        for s in range(3):
            acc[s] = jnp.zeros((ROWS, PAD), F32)
        for head in range(4):
            mask, s0, s1 = head_mask(head)
            q = triple[l, 0, :, s0:s1] * mask
            keys = triple[l, 1, :, s0:s1]
            scores = dot_t(q, keys) * scaling
            scores = jnp.where(key_ok, scores, -1e30)
            probs = jnp.exp(scores - lse[l, :, head : head + 1])
            probs_low = probs.astype(BF)
            grad_heads = da[:, s0:s1] * mask
            acc[2, :, s0:s1] += t_dot(probs_low, grad_heads)
            grad_probs = dot_t(grad_heads, triple[l, 2, :, s0:s1])
            inner = jnp.sum(grad_probs * probs, axis=1, keepdims=True)
            grad_scores = (probs * (grad_probs - inner)).astype(BF)
            acc[0, :, s0:s1] += dot(grad_scores, keys * mask)
            acc[1, :, s0:s1] += t_dot(grad_scores, q)
        for s in range(3):
            value = acc[s] * scaling if s < 2 else acc[s]
            g3[s] = value.astype(BF)
        g3[3] = att[l]

    def backward(step, _):
        l = LAYERS - 1 - step

        @pl.when(step == 0)
        def _():
            gather_wait(gtop, second_z)

        @pl.when(step > 0)
        def _():
            gather_start(gtop)
            gather_pass(gtop, 0, 1, 2, 3)
            relay(0, 0)
            finish(l + 1, 1, 1)
            gather_wait(gtop)
            add_pass(0, 1, 2, 3, path=side)

        for h in range(2):

            def hidden(n):
                lanes = pl.ds(pl.multiple_of(n * 256, 256), 256)
                value = dot(gtop[...], wm[l, 2 + h, :, lanes]) * slope[l, h, :, lanes].astype(F32)
                low = value.astype(BF)
                gb[h, :, lanes] = low
                csum[l, pl.ds(2 + h, 1), lanes] = jnp.sum(
                    low.astype(F32), axis=0, keepdims=True
                )

            tiles(3, hidden)

        def back_up(start, size):
            rows = pl.ds(start, size)
            value = dot_t(gb[0], wm[l, 0, rows, :]) + dot_t(gb[1], wm[l, 1, rows, :])
            part[:, pl.ds(start, size)] = value.astype(BF)

        features(back_up, add_start)
        transpose(gtop, 0)
        down_pair = (lax.rem(step, 2), lambda b: 0, lambda b: hid.at[l, b])
        make_send(2, *down_pair, step > 0)
        add_pass(0, 1)

        @pl.when(step > 0)
        def _():
            finish(l + 1, 0, 0)

        make_keep(2, 0, *down_pair, 0)
        add_pass(2)
        make_keep(2, 0, *down_pair, 1)
        add_pass(3)
        merge(2, 0, lax.rem(step, 2))
        add_wait()
        norm_backward(l, 1, gmid, 6 * l + 4)
        gather_start(gmid)
        transpose(x2.at[l], 1)
        gather_pass(gmid, 0, 1)
        up_pair = (lax.rem(step + 1, 2), lambda b: 1, lambda b: gb.at[b])
        make_send(1, *up_pair, step > 0)
        gather_pass(gmid, 2, 3)
        relay(2, 0)
        make_keep(1, 1, *up_pair, 0)
        make_keep(1, 1, *up_pair, 1)

        @pl.when(step == 0)
        def _():
            features(down(l, x2.at[LAYERS - 1]))

        merge(1, 1, lax.rem(step + 1, 2))
        gather_wait(gmid)

        @pl.when(step == 0)
        def _():
            for h in range(2):
                add_start(h, side)

        @pl.when(step > 0)
        def _():
            add_wait(side)
            lax.fori_loop(0, CHUNK // 16, settle(LAYERS - 1, recv2), 0)
            for k in range(N):
                oblk[k] = st[:, BLK * k : BLK * (k + 1)].astype(BF)
            go_start(2)

        da[...] = dot(gmid[...], wa[l, 3]).astype(BF)
        attend_back(l)
        relay(1, 1)
        for s in range(3):
            if s != 1:
                csum[l, s // 2 : s // 2 + 1, 0:PAD] = jnp.sum(
                    g3[s].astype(F32), axis=0, keepdims=True
                )

        def back_qkv(start, size):
            rows = pl.ds(start, size)
            value = dot_t(g3[0], wa[l, 0, rows, :])
            value = value + dot_t(g3[1], wa[l, 1, rows, :])
            value = value + dot_t(g3[2], wa[l, 2, rows, :])
            part[:, pl.ds(start, size)] = value.astype(BF)

        features(back_qkv, add_start)
        transpose(x1.at[l], 0)
        transpose(gmid, 1)
        add_pass(0)
        head_pair = (lax.rem(step, 2), lambda s: s // 3, lambda s: g3[s])
        make_send(0, *head_pair, step >= 0)
        add_pass(1, 2)
        finish(l, 2, 0)
        make_keep(0, 0, *head_pair, 0)
        add_pass(3)
        make_keep(0, 0, *head_pair, 1)

        @pl.when(step > 0)
        def _():
            go_pass(2, out_hbm)

        merge(0, 0, lax.rem(step, 2))
        add_wait()
        norm_backward(l, 0, gtop, jnp.where(l > 0, 6 * l - 1, 12))

        return 0

    lax.fori_loop(0, LAYERS, backward, 0)

    go_wait(2, out_hbm)
    sent(2)
    for k in range(N):
        oblk[k] = gst[:, BLK * k : BLK * (k + 1)].astype(BF)
    go_start(3)

    def c_copy(k):
        return remote(csum, cx.at[k], cxs.at[k], cxr.at[k], (d, near[k], c))

    def v_copy(k):
        return remote(vb.at[near[k]], vx.at[k], vxs.at[k], vxr.at[k], (d, near[k], c))

    def z_copy(k):
        return remote(
            vz.at[c], vz.at[c], vzs.at[k], vzr.at[c], (d, r, lax.rem(c + k + 1, N))
        )

    for k in range(N):
        vb[k] = vsum[:, BLK * k : BLK * (k + 1)]
    for k in range(3):
        v_copy(k).start()
        c_copy(k).start()
    go_pass(3, tg_hbm)
    relay(0, 0)
    total = vb[r]
    for k in range(3):
        v_copy(k).wait_recv()
        total = total + vx[k]
    vz[c] = total
    for k in range(3):
        z_copy(k).start()
    for k in range(3):
        c_copy(k).wait()
    for l in range(LAYERS):
        csum[l] = csum[l] + cx[0, l] + cx[1, l] + cx[2, l]
    c_half = remote(csum.at[other], cd, cds.at[0], cds.at[1], (other, r, c))
    c_half.start()
    for cs in range(N):

        @pl.when(c != cs)
        def _():
            pltpu.make_async_copy(vz.at[cs], vz.at[cs], vzr.at[cs]).wait()

    total = vz[0]
    for cs in range(1, N):
        total = total + vz[cs]
    vd[0] = total
    v_half = remote(vd.at[0], vd.at[1], vds.at[0], vds.at[1], (other, r, c))
    v_half.start()
    finish(0, 1, 1)
    finish(0, 0, 0)
    c_half.wait()
    cout[...] = csum[d] + cd[...]
    v_half.wait()
    vout[...] = vd[0] + vd[1]
    for k in range(3):
        v_copy(k).wait_send()
        z_copy(k).wait_send()

    pl.semaphore_wait(credit, 2)
    go_wait(3, tg_hbm)
    for u in (0, 1, 3):
        sent(u)
    for i in range(3):
        for j in range(2):
            arrived = result(i, other, j)
            pltpu.make_async_copy(arrived, arrived, finr.at[i, j]).wait()
    for k in range(3):
        remote(vec_ref, pin.at[r], vs.at[k], vr.at[k], (d, near[k], c)).wait_send()
    for l in range(LAYERS):
        for i in range(3):
            for k in range(2):
                for h in range(2):
                    send_w(l, i, k, h).wait_send()
                pass_w(l, i, k).wait_send()
            for k in range(3):
                share_w(l, i, k).wait_send()


def fused(*operands):
    dma = pltpu.SemaphoreType.DMA
    vmem = pltpu.VMEM
    whole = pl.BlockSpec(memory_space=pltpu.VMEM)
    anywhere = pl.BlockSpec(memory_space=pl.ANY)
    scratch = [
        vmem((LAYERS, 4, D, PAD), BF),
        vmem((LAYERS, 4, D, HALF), BF),
        vmem((LAYERS, ROWS, D), BF),
        vmem((LAYERS, ROWS, D), BF),
        vmem((LAYERS, 3, ROWS, PAD), BF),
        vmem((LAYERS, ROWS, PAD), BF),
        vmem((LAYERS, ROWS, 128), F32),
        vmem((LAYERS, 2, ROWS, HALF), BF),
        vmem((LAYERS, 2, ROWS, HALF), BF),
        vmem((LAYERS, 2, CHUNK, D), F32),
        vmem((LAYERS, 2, CHUNK, 128), F32),
        vmem((ROWS, D), BF),
        vmem((ROWS, D), BF),
        vmem((2, D, ROWS), BF),
        vmem((ROWS, D), BF),
        vmem((3, CHUNK, D), BF),
        vmem((CHUNK, D), F32),
        vmem((CHUNK, D), F32),
        vmem((N, CHUNK, BLK), BF),
        vmem((N, CHUNK, BLK), BF),
        vmem((N, CHUNK, BLK), BF),
        vmem((4, N, CHUNK, BLK), BF),
        vmem((N, 16, BLK), F32),
        vmem((16, D), F32),
        vmem((2, ROWS, HALF), BF),
        vmem((ROWS, PAD), BF),
        vmem((4, ROWS, PAD), BF),
        vmem((3, ROWS, PAD), F32),
        vmem((2, BLK, HALF), BF),
        vmem((2, N, BLK, HALF), BF),
        vmem((2, N, BLK, HALF), BF),
        vmem((3, 2, BLK, HALF), BF),
        vmem((2, BLK, PAD), F32),
        vmem((3, 2, BLK // 2, HALF), BF),
        vmem((2, LAST, D), BF),
        vmem((2, LAST, D), BF),
        vmem((3, CHUNK, D), BF),
        vmem((16, D), F32),
        vmem((LAYERS, 4, HALF), F32),
        vmem((N, 16, BLK), F32),
        vmem((3, 16, BLK), F32),
        vmem((N, 16, BLK), F32),
        vmem((2, 16, BLK), F32),
        vmem((3, LAYERS, 4, HALF), F32),
        vmem((4, HALF), F32),
        dma((LAYERS, 3, 2)),
        dma((LAYERS, 3, 2, 2)), dma((LAYERS, 3, 2, 2)),
        dma((LAYERS, 3, 2)), dma((LAYERS, 3, 2)),
        dma((LAYERS, 3, 3)), dma((LAYERS, 3, 3)),
        dma((3,)), dma((4,)),
        dma((4, N)), dma((4, N)), dma((4, N)), dma((4, N)),
        dma((8,)), dma((N, 2)), dma((10,)), dma((4,)), dma((2, 2)),
        dma((N,)), dma((2, N)), pltpu.SemaphoreType.REGULAR,
        dma((3, 2)), dma((3, 2)), dma((2,)), dma((3, 2)),
        dma((3, 2)), dma((3, 2)),
        dma((8,)), dma((N, 2)), dma((10,)), dma((4,)), dma((2, 2)),
        dma((3,)), dma((3,)), dma((3,)), dma((N,)), dma((2,)),
        dma((3,)), dma((3,)), dma((2,)),
    ]
    shape = jax.ShapeDtypeStruct
    return pl.pallas_call(
        kernel,
        out_shape=(
            shape((ROWS, BLK), BF),
            shape((ROWS, BLK), BF),
            shape((4, BLK, PAD), F32),
            shape((BLK, 2 * HALF), F32),
            shape((BLK, 2 * HALF), F32),
            shape((16, BLK), F32),
            shape((4, HALF), F32),
        ),
        in_specs=[anywhere] * 5 + [whole] * 3,
        out_specs=(anywhere,) * 5 + (whole, whole),
        scratch_shapes=scratch,
        compiler_params=pltpu.CompilerParams(
            collective_id=0, has_side_effects=True, vmem_limit_bytes=67_043_328
        ),
    )(*operands)


def widen(values, axis=-1, to=PAD):
    axis = axis % values.ndim
    pads = [(0, 0)] * values.ndim
    pads[axis] = (0, to - values.shape[axis])
    return jnp.pad(values, pads)


def per_device_fused(
    tokens, cotangent, qkv_weight, qv_bias, proj_weight, proj_bias,
    up_weight, up_bias, down_weight, down_bias, norm_gain, norm_shift,
):
    dp = lax.axis_index("dp")
    tok = widen(tokens[0], 0, ROWS)
    cot = widen(cotangent[0], 0, ROWS)
    heads = jnp.concatenate(
        [qkv_weight.transpose(0, 2, 1, 3), proj_weight.transpose(0, 2, 1)[:, None]], axis=1
    )
    vec = jnp.concatenate(
        [norm_gain, norm_shift, proj_bias[:, None], down_bias[:, None]], axis=1
    ).reshape(12, BLK)
    vec = widen(vec, 0, 16)
    zero = jnp.zeros_like(qv_bias[:, 0])
    qb = widen(jnp.stack([qv_bias[:, 0], zero, qv_bias[:, 1]], axis=1))
    ub = up_bias.reshape(LAYERS, 2, HALF)
    down = down_weight.transpose(0, 2, 1)
    out, tg, ga, gu, gd, vout, cout = fused(tok, cot, widen(heads), up_weight, down, vec, qb, ub)
    both = vout[:12].reshape(LAYERS, 6, BLK)
    layer = lax.dynamic_slice(both, (dp, 0, 0), (1, 6, BLK))
    return (
        out[None, :SEQ].astype(F32),
        tg[None, :SEQ].astype(F32),
        ga[:3, :, :BLK].transpose(1, 0, 2)[None],
        cout[None, 0:2, :BLK],
        ga[3, :, :BLK].T[None],
        layer[:, 4],
        gu[None],
        cout[2:].reshape(1, 2 * HALF),
        gd.T[None],
        layer[:, 5],
        both[:, 0:2],
        both[:, 2:4],
    )


NORMAL = (((1,), (0,)), ((), ()))
LAST_BOTH = (((1,), (1,)), ((), ()))
FIRST_BOTH = (((0,), (0,)), ((), ()))


def gather_tokens(values):
    return lax.all_gather(values, "col", axis=0, tiled=True)


def gather_blocks(values):
    return lax.all_gather(values, "row", axis=0, tiled=True)


def gather_grad_blocks(values):
    return lax.all_gather(values, "row", axis=0, tiled=True)


def width_totals(first_sum, second_sum):
    return lax.psum((first_sum, second_sum), "row")


def gather_whole(triple_w, up_w, proj_w, down_w):
    row_whole = (triple_w, up_w, proj_w, down_w)
    col_whole = (proj_w, down_w, triple_w, up_w)
    return (row_whole, col_whole)


def row_product(gathered, matrix, contract):
    return lax.psum_scatter(
        lax.dot_general(gathered, matrix, contract, preferred_element_type=jnp.float32).astype(
            jnp.bfloat16
        ),
        "row",
        scatter_dimension=0,
        tiled=True,
    ).astype(jnp.float32)


def col_product(gathered, matrix, contract):
    return lax.psum_scatter(
        lax.dot_general(gathered, matrix, contract, preferred_element_type=jnp.float32).astype(
            jnp.bfloat16
        ),
        "col",
        scatter_dimension=0,
        tiled=True,
    ).astype(jnp.float32)


def norm_forward(stream, factor, shift):
    totals, squares = width_totals(jnp.sum(stream, axis=1), jnp.sum(stream * stream, axis=1))
    centre = totals / D
    spread = squares / D - centre * centre
    centred = stream - centre[:, None]
    scaling = lax.rsqrt(spread + EPSILON)
    standard = centred * scaling[:, None]
    return (standard * factor + shift, standard, scaling)


def norm_backward(grad_norm, standard, scaling, factor):
    factor_grad = jnp.sum(grad_norm * standard, axis=0)
    shift_grad = jnp.sum(grad_norm, axis=0)
    grad_standard = grad_norm * factor
    first_sum, second_sum = width_totals(
        jnp.sum(grad_standard, axis=1), jnp.sum(grad_standard * standard, axis=1)
    )
    grad_stream = scaling[:, None] * (
        grad_standard - first_sum[:, None] / D - standard * (second_sum[:, None] / D)
    )
    return (grad_stream, factor_grad, shift_grad)


def split_triple(triple_out, width):
    images = triple_out.shape[0] // SEQ
    head_count = width // HEAD_DIM
    pieces = triple_out.reshape(images, SEQ, 3, head_count, HEAD_DIM)
    return (pieces[:, :, 0], pieces[:, :, 1], pieces[:, :, 2])


def attend_forward(triple_out, width):
    queries, key_rows, values = split_triple(triple_out, width)
    scaling = HEAD_DIM ** (-0.5)
    scores = (
        jnp.einsum("bqhd,bkhd->bhqk", queries, key_rows, preferred_element_type=jnp.float32)
        * scaling
    )
    row_peak = jnp.max(scores, axis=-1, keepdims=True)
    log_totals = row_peak + jnp.log(jnp.sum(jnp.exp(scores - row_peak), axis=-1, keepdims=True))
    probs_low = jnp.exp(scores - log_totals).astype(jnp.bfloat16)
    attended = jnp.einsum("bhqk,bkhd->bqhd", probs_low, values, preferred_element_type=jnp.float32)
    return (attended.reshape(triple_out.shape[0], width).astype(jnp.bfloat16), log_totals)


def attend_backward(triple_out, log_totals, grad_attended, width):
    queries, key_rows, values = split_triple(triple_out, width)
    scaling = HEAD_DIM ** (-0.5)
    scores = (
        jnp.einsum("bqhd,bkhd->bhqk", queries, key_rows, preferred_element_type=jnp.float32)
        * scaling
    )
    probs = jnp.exp(scores - log_totals)
    probs_low = probs.astype(jnp.bfloat16)
    grad_heads = grad_attended.reshape(values.shape)
    grad_values = jnp.einsum(
        "bhqk,bqhd->bkhd", probs_low, grad_heads, preferred_element_type=jnp.float32
    )
    grad_probs = jnp.einsum(
        "bqhd,bkhd->bhqk", grad_heads, values, preferred_element_type=jnp.float32
    )
    grad_scores = (
        probs * (grad_probs - jnp.sum(grad_probs * probs, axis=-1, keepdims=True))
    ).astype(jnp.bfloat16)
    grad_queries = (
        jnp.einsum("bhqk,bkhd->bqhd", grad_scores, key_rows, preferred_element_type=jnp.float32)
        * scaling
    )
    grad_keys = (
        jnp.einsum("bhqk,bqhd->bkhd", grad_scores, queries, preferred_element_type=jnp.float32)
        * scaling
    )
    stacked = jnp.stack([grad_queries, grad_keys, grad_values], axis=2)
    return stacked.reshape(triple_out.shape[0], 3 * width).astype(jnp.bfloat16)


def layer_forward(stream, weights):
    qkv_w, qv_b, proj_w, proj_b, up_w, up_b, down_w, down_b, factors, shifts = weights
    width = qkv_w.shape[2]
    triple_w = qkv_w.reshape(qkv_w.shape[0], 3 * width)
    row_whole, col_whole = gather_whole(triple_w, up_w, proj_w, down_w)
    first_norm, first_standard, first_scaling = norm_forward(stream, factors[0], shifts[0])
    first_rows = gather_tokens(first_norm.astype(jnp.bfloat16))
    offsets = jnp.concatenate([qv_b[0], jnp.zeros_like(qv_b[0]), qv_b[1]])
    triple_out = (row_product(first_rows, triple_w, NORMAL) + offsets).astype(jnp.bfloat16)
    attended, log_totals = attend_forward(triple_out, width)
    head_rows = gather_blocks(attended)
    stream_mid = stream + col_product(head_rows, proj_w, NORMAL) + proj_b
    second_norm, second_standard, second_scaling = norm_forward(stream_mid, factors[1], shifts[1])
    second_rows = gather_tokens(second_norm.astype(jnp.bfloat16))
    before = row_product(second_rows, up_w, NORMAL) + up_b
    activated = jax.nn.gelu(before, approximate=False).astype(jnp.bfloat16)
    hidden_rows = gather_blocks(activated)
    branch_out = col_product(hidden_rows, down_w, NORMAL)
    stream_out = stream_mid + branch_out + down_b
    saved = (
        first_rows,
        first_standard,
        first_scaling,
        triple_out,
        log_totals,
        head_rows,
        second_rows,
        second_standard,
        second_scaling,
        before,
        hidden_rows,
        row_whole,
        col_whole,
    )
    return (stream_out, saved)


def layer_backward(grad_out, saved, weights):
    qkv_w, qv_b, proj_w, proj_b, up_w, up_b, down_w, down_b, factors, shifts = weights
    (
        first_rows,
        first_standard,
        first_scaling,
        triple_out,
        log_totals,
        head_rows,
        second_rows,
        second_standard,
        second_scaling,
        before,
        hidden_rows,
        row_whole,
        col_whole,
    ) = saved
    width = qkv_w.shape[2]
    triple_w = qkv_w.reshape(qkv_w.shape[0], 3 * width)
    grad_rows = gather_tokens(grad_out.astype(jnp.bfloat16))
    down_grad = lax.dot_general(
        hidden_rows, grad_rows, FIRST_BOTH, preferred_element_type=jnp.float32
    )
    down_off_grad = jnp.sum(grad_rows, axis=0, dtype=jnp.float32)
    grad_active = row_product(grad_rows, down_w, LAST_BOTH)
    _, slope_pull = jax.vjp(partial(jax.nn.gelu, approximate=False), before)
    grad_before = slope_pull(grad_active)[0].astype(jnp.bfloat16)
    before_rows = gather_grad_blocks(grad_before)
    up_grad = lax.dot_general(
        second_rows, before_rows, FIRST_BOTH, preferred_element_type=jnp.float32
    )
    up_off_grad = jnp.sum(before_rows, axis=0, dtype=jnp.float32)
    grad_second = col_product(before_rows, up_w, LAST_BOTH)
    grad_mid, second_factor_grad, second_shift_grad = norm_backward(
        grad_second, second_standard, second_scaling, factors[1]
    )
    grad_mid = grad_mid + grad_out
    mid_rows = gather_tokens(grad_mid.astype(jnp.bfloat16))
    proj_grad = lax.dot_general(head_rows, mid_rows, FIRST_BOTH, preferred_element_type=jnp.float32)
    proj_off_grad = jnp.sum(mid_rows, axis=0, dtype=jnp.float32)
    grad_attended = row_product(mid_rows, proj_w, LAST_BOTH).astype(jnp.bfloat16)
    grad_triple = attend_backward(triple_out, log_totals, grad_attended, width)
    triple_rows = gather_grad_blocks(grad_triple)
    triple_grad = lax.dot_general(
        first_rows, triple_rows, FIRST_BOTH, preferred_element_type=jnp.float32
    )
    column_sums = jnp.sum(triple_rows, axis=0, dtype=jnp.float32).reshape(3, width)
    qv_grad = jnp.stack([column_sums[0], column_sums[2]])
    grad_first = col_product(triple_rows, triple_w, LAST_BOTH)
    grad_in, first_factor_grad, first_shift_grad = norm_backward(
        grad_first, first_standard, first_scaling, factors[0]
    )
    grad_in = grad_in + grad_mid
    factor_grads = jnp.stack([first_factor_grad, second_factor_grad])
    shift_grads = jnp.stack([first_shift_grad, second_shift_grad])
    layer_grads = (
        triple_grad.reshape(qkv_w.shape),
        qv_grad,
        proj_grad,
        proj_off_grad,
        up_grad,
        up_off_grad,
        down_grad,
        down_off_grad,
        factor_grads,
        shift_grads,
    )
    return (grad_in, layer_grads)


def per_device_plain(
    tokens,
    cotangent,
    qkv_weight,
    qv_bias,
    proj_weight,
    proj_bias,
    up_weight,
    up_bias,
    down_weight,
    down_bias,
    norm_gain,
    norm_shift,
):
    image_count, seq_len, width_row = tokens.shape
    stream = tokens.reshape(image_count * seq_len, width_row).astype(jnp.float32)
    layer_params = []
    saved_list = []
    for layer_index in range(LAYERS):
        params = (
            qkv_weight[layer_index],
            qv_bias[layer_index],
            proj_weight[layer_index],
            proj_bias[layer_index],
            up_weight[layer_index],
            up_bias[layer_index],
            down_weight[layer_index],
            down_bias[layer_index],
            norm_gain[layer_index],
            norm_shift[layer_index],
        )
        layer_params.append(params)
        stream, saved = layer_forward(stream, params)
        saved_list.append(saved)
    grad_stream = cotangent.reshape(image_count * seq_len, width_row).astype(jnp.float32)
    per_layer = [None] * LAYERS
    for layer_index in reversed(range(LAYERS)):
        grad_stream, layer_grads = layer_backward(
            grad_stream, saved_list[layer_index], layer_params[layer_index]
        )
        per_layer[layer_index] = layer_grads
    stacked = tuple(
        (jnp.stack([layer_grads[position] for layer_grads in per_layer]) for position in range(10))
    )
    summed = (
        lax.psum_scatter(
            stacked[0].astype(jnp.bfloat16), "dp", scatter_dimension=0, tiled=True
        ).astype(jnp.float32),
        lax.psum_scatter(
            stacked[1].astype(jnp.bfloat16), "dp", scatter_dimension=0, tiled=True
        ).astype(jnp.float32),
        lax.psum_scatter(
            stacked[2].astype(jnp.bfloat16), "dp", scatter_dimension=0, tiled=True
        ).astype(jnp.float32),
        lax.psum_scatter(
            stacked[3].astype(jnp.bfloat16), "dp", scatter_dimension=0, tiled=True
        ).astype(jnp.float32),
        lax.psum_scatter(
            stacked[4].astype(jnp.bfloat16), "dp", scatter_dimension=0, tiled=True
        ).astype(jnp.float32),
        lax.psum_scatter(
            stacked[5].astype(jnp.bfloat16), "dp", scatter_dimension=0, tiled=True
        ).astype(jnp.float32),
        lax.psum_scatter(
            stacked[6].astype(jnp.bfloat16), "dp", scatter_dimension=0, tiled=True
        ).astype(jnp.float32),
        lax.psum_scatter(
            stacked[7].astype(jnp.bfloat16), "dp", scatter_dimension=0, tiled=True
        ).astype(jnp.float32),
    )
    norm_sums = lax.psum((stacked[8], stacked[9]), ("dp", "col"))
    result = stream.reshape(image_count, seq_len, width_row)
    tokens_grad = grad_stream.reshape(image_count, seq_len, width_row)
    return (
        result,
        tokens_grad,
        summed[0],
        summed[1],
        summed[2],
        summed[3],
        summed[4],
        summed[5],
        summed[6],
        summed[7],
        norm_sums[0],
        norm_sums[1],
    )


def solution(mesh):
    placed = (
        P(("dp", "col"), None, "row"),
        P(("dp", "col"), None, "row"),
        P(None, "row", None, "col"),
        P(None, None, "col"),
        P(None, "col", "row"),
        P(None, "row"),
        P(None, "row", "col"),
        P(None, "col"),
        P(None, "col", "row"),
        P(None, "row"),
        P(None, None, "row"),
        P(None, None, "row"),
    )
    sizes = (mesh.shape["dp"], mesh.shape["row"], mesh.shape["col"])
    return jax.shard_map(
        per_device_fused if sizes == (2, N, N) else per_device_plain,
        mesh=mesh,
        in_specs=placed,
        out_specs=(
            P(("dp", "col"), None, "row"),
            P(("dp", "col"), None, "row"),
            P("dp", "row", None, "col"),
            P("dp", None, "col"),
            P("dp", "col", "row"),
            P("dp", "row"),
            P("dp", "row", "col"),
            P("dp", "col"),
            P("dp", "col", "row"),
            P("dp", "row"),
            P(None, None, "row"),
            P(None, None, "row"),
        ),
        check_vma=False,
    )
```

```python
from functools import partial

import jax
import jax.numpy as jnp
from jax import lax
from jax.experimental import pallas as pl
from jax.experimental.pallas import tpu as pltpu
from jax.sharding import PartitionSpec as P

D = 1408
HEAD_DIM = 88
SEQ = 257
LAYERS = 2
EPSILON = 1e-06
MESH = pl.DeviceIdType.MESH
BF = jnp.bfloat16
F32 = jnp.float32

ROWS = 272
STEP = 64
CHUNK = 80
LAST = 72
BLK = 352
PAD = 384
HALF = 768
N = 4


def dot(a, b):
    return jnp.dot(a, b, preferred_element_type=F32)


def dot_t(a, b):
    return lax.dot_general(a, b, (((1,), (1,)), ((), ())), preferred_element_type=F32)


def t_dot(a, b):
    return lax.dot_general(a, b, (((0,), (0,)), ((), ())), preferred_element_type=F32)


def span(index):
    return pl.ds(STEP * index, STEP if index < N - 1 else LAST)


def head_span(head):
    low, high = HEAD_DIM * head, HEAD_DIM * (head + 1)
    return low, high, low // 128 * 128, -(-high // 128) * 128


def kernel(
    io_hbm, wa_hbm, up_hbm, down_hbm, gain_ref, shift_ref, pb_ref, db_ref, qv_ref, ub_ref,
    out_hbm, tg_hbm, ga_hbm, gu_hbm, gd_hbm, vout, cout,
    wa, wm, x1, x2, triple, att, lse, hid, slope, std, inv,
    gtop, gmid, lt, part, recv, st, gst, tin, cin, oblk, mid, pin, pv,
    gb, da, g3, acc, sbuf, prx, keep, ici, fin, hop, rb, rb2, recv2,
    vec_ref, qb_ref, vsum, csum, vb, vx, vz, vd, cx, cd,
    wloc, wsend, wrecv, fsend, frecv, psend, precv, vs, vr, m1s, m1r, m2s, m2r,
    zs, zr, rss, rsr, lr, cs_s, cs_r, credit, gis, gir, fins, finr, hs, hr,
    zs2, zr2, rss2, rsr2, lr2, vxs, vxr, vzs, vzr, vds, cxs, cxr, cds,
):
    d, r, c = lax.axis_index("dp"), lax.axis_index("row"), lax.axis_index("col")
    other = 1 - d
    near = (r + 1 - 2 * lax.rem(r, 2), lax.rem(r + 2, N), N - 1 - r)
    last = c == N - 1

    def remote(src, dst, ssem, rsem, dev):
        return pltpu.make_async_remote_copy(
            src, dst, ssem, rsem, device_id=dev, device_id_type=MESH
        )

    def rblk(index):
        return pl.ds(pl.multiple_of(index * BLK, 16), BLK)

    def rhalf(index, part_):
        return pl.ds(pl.multiple_of(index * BLK + part_ * (BLK // 2), 16), BLK // 2)

    recv[...] = jnp.zeros_like(recv)
    recv2[...] = jnp.zeros_like(recv2)
    for array in (x1.at[0], x1.at[1], x2.at[0], x2.at[1], gtop, gmid):
        array[ROWS - 16 :, :] = jnp.zeros((16, D), BF)
    tin[...] = jnp.zeros_like(tin)
    cin[...] = jnp.zeros_like(cin)
    vsum[...] = jnp.zeros_like(vsum)
    csum[...] = jnp.zeros_like(csum)
    vec_ref[...] = jnp.zeros_like(vec_ref)
    qb_ref[...] = jnp.zeros_like(qb_ref)
    for l in range(LAYERS):
        for j in range(2):
            vec_ref[6 * l + j : 6 * l + j + 1, :] = gain_ref[l, j : j + 1, :]
            vec_ref[6 * l + 2 + j : 6 * l + 3 + j, :] = shift_ref[l, j : j + 1, :]
            qb_ref[l, 2 * j : 2 * j + 1, 0:BLK] = qv_ref[l, j : j + 1, :]
        vec_ref[6 * l + 4 : 6 * l + 5, :] = pb_ref[l : l + 1, :]
        vec_ref[6 * l + 5 : 6 * l + 6, :] = db_ref[l : l + 1, :]
    barrier = pltpu.get_barrier_semaphore()
    for k in range(N * N):
        pl.semaphore_signal(
            barrier, inc=1,
            device_id=(d, lax.rem(r + k // N, N), lax.rem(c + k % N, N)), device_id_type=MESH,
        )
    pl.semaphore_signal(barrier, inc=1, device_id=(other, r, c), device_id_type=MESH)
    pl.semaphore_wait(barrier, N * N + 1)

    for k in range(3):
        remote(vec_ref, pin.at[r], vs.at[k], vr.at[k], (d, near[k], c)).start()
    own_vec = pltpu.make_async_copy(vec_ref, pin.at[r], vr.at[3])
    own_vec.start()

    def by_size(body):
        @pl.when(last)
        def _():
            body(LAST)

        @pl.when(jnp.logical_not(last))
        def _():
            body(STEP)

    def come_start(u, src):
        for ct in range(N):
            size = STEP if ct < N - 1 else LAST
            source, target = src.at[span(ct)], mid.at[u, c, pl.ds(0, size)]

            @pl.when(c == ct)
            def _():
                pltpu.make_async_copy(source, target, m1r.at[u, c]).start()

            @pl.when(c != ct)
            def _():
                remote(source, target, m1s.at[u, ct], m1r.at[u, c], (d, r, ct)).start()

    def come_pass(u, dst):
        def sized(size):
            rows = pl.ds(0, size)
            for p in range(N):
                source, target = mid.at[u, p, rows], dst.at[r, rows]
                pltpu.make_async_copy(source, source, m1r.at[u, p]).wait()

                @pl.when(r == p)
                def _():
                    pltpu.make_async_copy(source, target, m2r.at[u, r]).start()

                @pl.when(r != p)
                def _():
                    remote(source, target, m2s.at[u, p], m2r.at[u, r], (d, p, c)).start()

        by_size(sized)

    def come_wait(u, dst):
        def sized(size):
            for rs in range(N):
                rows = dst.at[rs, pl.ds(0, size)]
                pltpu.make_async_copy(rows, rows, m2r.at[u, rs]).wait()

        by_size(sized)

    def go_start(u):
        def sized(size):
            rows = pl.ds(0, size)
            for k in range(N):
                source, target = oblk.at[k, rows], mid.at[u, r, rows]

                @pl.when(r == k)
                def _():
                    pltpu.make_async_copy(source, target, m1r.at[u, r]).start()

                @pl.when(r != k)
                def _():
                    remote(source, target, m1s.at[u, k], m1r.at[u, r], (d, k, c)).start()

        by_size(sized)

    def go_pass(u, dst):
        def sized(size):
            for p in range(N):
                source = mid.at[u, p, pl.ds(0, size)]
                target = dst.at[pl.ds(pl.multiple_of(STEP * c, 16), size)]
                pltpu.make_async_copy(source, source, m1r.at[u, p]).wait()

                @pl.when(c == p)
                def _():
                    pltpu.make_async_copy(source, target, m2r.at[u, c]).start()

                @pl.when(c != p)
                def _():
                    remote(source, target, m2s.at[u, p], m2r.at[u, c], (d, r, p)).start()

        by_size(sized)

    def go_wait(u, dst):
        for cs in range(N):
            rows = dst.at[span(cs)]
            pltpu.make_async_copy(rows, rows, m2r.at[u, cs]).wait()

    def sent(u):
        for ct in range(N):
            size = STEP if ct < N - 1 else LAST
            rows = mid.at[u, 0, pl.ds(0, size)]

            if u < 2:

                @pl.when(c != ct)
                def _():
                    remote(rows, rows, m1s.at[u, ct], m1r.at[u, 0], (d, r, ct)).wait_send()

            def second(size):
                rows = mid.at[u, 0, pl.ds(0, size)]
                first_row = u < 2

                @pl.when((r != ct) if first_row else (c != ct))
                def _():
                    remote(rows, rows, m2s.at[u, ct], m2r.at[u, 0], (d, r, c)).wait_send()

                if not first_row:

                    @pl.when(r != ct)
                    def _():
                        remote(rows, rows, m1s.at[u, ct], m1r.at[u, 0], (d, ct, c)).wait_send()

            by_size(second)

    come_start(0, io_hbm.at[0])

    def source_w(l, i, which, rows):
        if i == 0:
            return wa_hbm.at[l, pl.ds(2 * which, 2), rows, :]
        lanes = pl.ds(pl.multiple_of(HALF * which, 128), HALF)
        return (up_hbm if i == 1 else down_hbm).at[l, rows, lanes]

    def rows_w(l, i, which, block):
        if i == 0:
            return wa.at[l, pl.ds(2 * which, 2), block, :]
        return wm.at[l, 2 * (i - 1) + which, block, :]

    def local_w(l, i, which):
        return pltpu.make_async_copy(
            source_w(l, i, which, pl.ds(0, BLK)), rows_w(l, i, which, rblk(r)), wloc.at[l, i, which]
        )

    def send_w(l, i, k, h):
        return remote(
            source_w(l, i, d, pl.ds(h * (BLK // 2), BLK // 2)), rows_w(l, i, d, rhalf(r, h)),
            wsend.at[l, i, k, h], wrecv.at[l, i, k, h], (d, near[k], c),
        )

    def pass_w(l, i, k):
        rows = rows_w(l, i, d, rhalf(near[k], k))
        return remote(rows, rows, fsend.at[l, i, k], frecv.at[l, i, k], (d, near[1 - k], c))

    def share_w(l, i, k):
        rows = rows_w(l, i, d, rblk(near[k]))
        return remote(rows, rows, psend.at[l, i, k], precv.at[l, i, k], (other, r, c))

    def direct_w(l, i, parts=(0, 1)):
        for part_ in parts:
            for k in range(2):
                send_w(l, i, k, k if part_ == 0 else 1 - k).start()

    def stage_w(l, i):
        for k in range(2):
            send_w(l, i, k, k).wait_recv()
            pass_w(l, i, k).start()
        for k in range(2):
            send_w(l, i, k, 1 - k).wait_recv()
            share_w(l, i, k).start()

    def close_w(l, i):
        for k in range(2):
            rows = rows_w(l, i, d, rhalf(near[2], k))
            pltpu.make_async_copy(rows, rows, frecv.at[l, i, k]).wait()
        share_w(l, i, 2).start()

    def need_w(l, i):
        for which in range(2):
            local_w(l, i, which).wait()
        for k in range(3):
            rows = rows_w(l, i, other, rblk(near[k]))
            pltpu.make_async_copy(rows, rows, precv.at[l, i, k]).wait()

    direct_w(0, 0, (0,))
    come_pass(0, tin)
    direct_w(0, 0, (1,))
    come_start(1, io_hbm.at[1])
    for l in range(LAYERS):
        for i in range(3):
            for which in range(2):
                local_w(l, i, which).start()

    def half_rows(cs, h):
        return pl.ds(STEP * cs + 32 * h, 32 if h == 0 or cs < N - 1 else LAST - 32)

    halves = ((0, 0), (1, 0), (0, 1), (1, 1))
    targets = ((2, 1), (2, 0), (1, 3), (1, 2))
    relays = ((1, 0, [(2 + far, h) for far, h in halves]), (2, 3, [(1 - far, h) for far, h in halves]))

    first_z, second_z = (zs, zr), (zs2, zr2)

    def gather_start(x, sems=first_z, steps=(0, 1, 2, 3)):
        zs, zr = sems
        for c0 in range(N):

            @pl.when(c == c0)
            def _():
                for n in steps:
                    rows = x.at[half_rows(c0, n % 2)]
                    remote(
                        rows, rows, zs.at[n], zr.at[c0, n % 2], (d, r, targets[c0][n // 2])
                    ).start()

    def gather_pass(x, *steps, sems=first_z):
        zs, zr = sems
        for c0, far, order in relays:

            @pl.when(c == c0)
            def _():
                for n in steps:
                    cs, h = order[n]
                    rows = x.at[half_rows(cs, h)]
                    pltpu.make_async_copy(rows, rows, zr.at[cs, h]).wait()
                    remote(rows, rows, zs.at[4 + n], zr.at[cs, h], (d, r, far)).start()

    def gather_wait(x, sems=first_z):
        zs, zr = sems
        for c0 in range(N):
            passed = [order for at, _, order in relays if at == c0]

            @pl.when(c == c0)
            def _():
                for cs in range(N):
                    for h in range(2):
                        if cs != c0 and not (passed and (cs, h) in passed[0]):
                            rows = x.at[half_rows(cs, h)]
                            pltpu.make_async_copy(rows, rows, zr.at[cs, h]).wait()
                for n in range(4):
                    rows = x.at[half_rows(c0, n % 2)]
                    remote(rows, rows, zs.at[n], zr.at[c0, 0], (d, r, targets[c0][0])).wait_send()
                if passed:
                    for n, (cs, h) in enumerate(passed[0]):
                        rows = x.at[half_rows(cs, h)]
                        remote(rows, rows, zs.at[4 + n], zr.at[cs, h], (d, r, 0)).wait_send()

    sides = ((0, 1, (3, 2)), (3, 2, (0, 1)))
    inner = ((1, 0), (2, 3))

    def size_of(cs):
        return STEP if cs < N - 1 else LAST

    def cols(h):
        return pl.ds(0, HALF) if h == 0 else pl.ds(HALF, D - HALF)

    main = (part, rb, recv, rss, rsr, lr)
    side = (x2.at[LAYERS - 1], rb2, recv2, rss2, rsr2, lr2)

    def end_copy(n, h, middle, dest, path):
        part, rb, recv, rss, rsr, lr = path
        return remote(
            part.at[span(dest), cols(h)], rb.at[n, pl.ds(0, size_of(dest)), cols(h)],
            rss.at[2 * n + h], lr.at[n, h], (d, r, middle),
        )

    def single_copy(dest, h, path):
        part, rb, recv, rss, rsr, lr = path
        return remote(
            part.at[span(dest), cols(h)], recv.at[1, pl.ds(0, size_of(dest)), cols(h)],
            rss.at[4 + h], rsr.at[h], (d, r, dest),
        )

    def sum_copy(n, h, dest, path):
        part, rb, recv, rss, rsr, lr = path
        rows = pl.ds(0, size_of(dest))
        return remote(
            rb.at[n, rows, cols(h)], recv.at[2, rows, cols(h)], rss.at[6 + 2 * n + h],
            rsr.at[2 + h], (d, r, dest),
        )

    def add_start(h, path=main):
        for end, middle, dests in sides:

            @pl.when(c == end)
            def _():
                for n in range(2):
                    end_copy(n, h, middle, dests[n], path).start()
                single_copy(middle, h, path).start()

        for middle, end in inner:

            @pl.when(c == middle)
            def _():
                single_copy(end, h, path).start()

        for cs in range(N):

            @pl.when(c == cs)
            def _():
                path[2][0, 0 : size_of(cs), cols(h)] = path[0][span(cs), cols(h)]

    def add_pass(*steps, path=main):
        part, rb, recv, rss, rsr, lr = path
        for end, middle, dests in sides:

            @pl.when(c == middle)
            def _():
                for step in steps:
                    h, n = step // 2, step % 2
                    dest = dests[n]
                    size = size_of(dest)
                    rows = rb.at[n, pl.ds(0, size), cols(h)]
                    pltpu.make_async_copy(rows, rows, lr.at[n, h]).wait()
                    for start in range(0, size, 16):
                        width = min(16, size - start)
                        mine = part[pl.ds(STEP * dest + start, width), cols(h)]
                        value = rb[n, start : start + width, cols(h)].astype(F32)
                        rb[n, start : start + width, cols(h)] = (
                            value + mine.astype(F32)
                        ).astype(BF)
                    sum_copy(n, h, dest, path).start()

    def add_wait(path=main):
        part, rb, recv, rss, rsr, lr = path
        for cs in range(N):

            @pl.when(c == cs)
            def _():
                for k in (1, 2):
                    for h in range(2):
                        rows = recv.at[k, pl.ds(0, size_of(cs)), cols(h)]
                        pltpu.make_async_copy(rows, rows, rsr.at[2 * (k - 1) + h]).wait()

        for end, middle, dests in sides:

            @pl.when(c == end)
            def _():
                for h in range(2):
                    for n in range(2):
                        end_copy(n, h, middle, dests[n], path).wait_send()
                    single_copy(middle, h, path).wait_send()

            @pl.when(c == middle)
            def _():
                for h in range(2):
                    single_copy(end, h, path).wait_send()
                    for n in range(2):
                        sum_copy(n, h, dests[n], path).wait_send()

    def received(rows, recv=recv):
        total = recv[0, rows, :].astype(F32)
        for k in range(1, recv.shape[0]):
            total = total + recv[k, rows, :].astype(F32)
        return total

    def vector(row):
        return pv[pl.ds(row, 1), :]

    def own_rows(x, t, value):
        @pl.when(jnp.logical_or(t < 4, last))
        def _():
            x[pl.ds(pl.multiple_of(STEP * c + 16 * t, 16), 16), :] = value

    valid = jnp.where(last, SEQ - STEP * (N - 1), STEP)

    def masked(t, value):
        index = lax.broadcasted_iota(jnp.int32, (16, 1), 0) + 16 * t
        return jnp.where(index < valid, value, 0.0)

    def early(x, body):
        lax.fori_loop(0, 2, body, 0)
        gather_start(x, steps=(0,))
        lax.fori_loop(2, CHUNK // 16, body, 0)
        gather_start(x, steps=(1, 2, 3))

    def norm_forward(l, j, x, extra):
        def body(t, _):
            rows = pl.ds(pl.multiple_of(16 * t, 16), 16)
            v = extra(rows)
            st[rows, :] = v
            centre = jnp.sum(v, axis=1, keepdims=True) / D
            spread_ = jnp.sum(v * v, axis=1, keepdims=True) / D - centre * centre
            scale = lax.rsqrt(spread_ + EPSILON)
            standard = (v - centre) * scale
            std[l, j, rows, :] = standard
            inv[l, j, rows, :] = jnp.broadcast_to(scale, (16, 128))
            value = standard * vector(6 * l + j) + vector(6 * l + 2 + j)
            own_rows(x, t, value.astype(BF))
            return 0

        early(x, body)

    def norm_backward(l, j, x, bias_row):
        def body(t, _):
            rows = pl.ds(pl.multiple_of(16 * t, 16), 16)
            e = received(rows)
            standard = std[l, j, rows, :]
            gain_term = masked(t, e * standard)
            vsum[pl.ds(6 * l + j, 1), :] += jnp.sum(gain_term, axis=0, keepdims=True)
            vsum[pl.ds(6 * l + 2 + j, 1), :] += jnp.sum(masked(t, e), axis=0, keepdims=True)
            f = e * vector(6 * l + j)
            first = jnp.sum(f, axis=1, keepdims=True) / D
            second = jnp.sum(f * standard, axis=1, keepdims=True) / D
            scale = inv[l, j, rows, 0:1]
            grad = gst[rows, :] + scale * (f - first - standard * second)
            gst[rows, :] = grad
            if x is not None:
                low = grad.astype(BF)
                own_rows(x, t, low)
                vsum[pl.ds(bias_row, 1), :] += jnp.sum(
                    masked(t, low.astype(F32)), axis=0, keepdims=True
                )
            return 0

        if j == 1:
            early(x, body)
        else:

            @pl.when(l > 0)
            def _():
                early(x, body)

            @pl.when(l == 0)
            def _():
                lax.fori_loop(0, CHUNK // 16, body, 0)

    def tiles(count, body):
        lax.fori_loop(0, count, lambda n, _: (body(n), 0)[1], 0)

    def features(body, start=None):
        body(0, 768)
        if start is not None:
            start(0)
        body(HALF, 640)
        if start is not None:
            start(1)

    def assemble(src, dst):
        for k in range(N):
            dst[:, BLK * k : BLK * (k + 1)] = src[k, :, 0:BLK].astype(F32)

    for k in range(3):
        remote(vec_ref, pin.at[r], vs.at[k], vr.at[k], (d, near[k], c)).wait_recv()
    own_vec.wait()
    assemble(pin, pv)
    come_wait(0, tin)
    come_pass(1, cin)
    assemble(tin, st)

    lane = lax.broadcasted_iota(jnp.int32, (1, PAD), 1)
    key_ok = lax.broadcasted_iota(jnp.int32, (1, ROWS), 1) < SEQ
    scaling = HEAD_DIM**-0.5

    def head_mask(head):
        low, high, s0, s1 = head_span(head)
        lanes = lane[:, s0:s1]
        return jnp.logical_and(lanes >= low, lanes < high).astype(BF), s0, s1

    def attend(l):
        acc[0] = jnp.zeros((ROWS, PAD), F32)
        for head in range(4):
            mask, s0, s1 = head_mask(head)
            q = triple[l, 0, :, s0:s1] * mask
            scores = dot_t(q, triple[l, 1, :, s0:s1]) * scaling
            scores = jnp.where(key_ok, scores, -1e30)
            peak = jnp.max(scores, axis=1, keepdims=True)
            total = peak + jnp.log(jnp.sum(jnp.exp(scores - peak), axis=1, keepdims=True))
            lse[l, :, head : head + 1] = total
            probs = jnp.exp(scores - total).astype(BF)
            acc[0, :, s0:s1] += dot(probs, triple[l, 2, :, s0:s1] * mask)
        att[l] = acc[0].astype(BF)

    def down(l, target):
        def body(start, size):
            rows = pl.ds(start, size)
            value = dot_t(hid[l, 0], wm[l, 2, rows, :]) + dot_t(hid[l, 1], wm[l, 3, rows, :])
            target[:, rows] = value.astype(BF)

        return body

    def settle(l, recv):
        def body(t, _):
            rows = pl.ds(pl.multiple_of(16 * t, 16), 16)
            st[rows, :] = st[rows, :] + received(rows, recv) + vector(6 * l + 5)
            return 0

        return body

    def top_rows(t, _):
        rows = pl.ds(pl.multiple_of(16 * t, 16), 16)
        low = gst[rows, :].astype(BF)
        own_rows(gtop, t, low)
        vsum[pl.ds(6 * (LAYERS - 1) + 5, 1), :] += jnp.sum(
            masked(t, low.astype(F32)), axis=0, keepdims=True
        )
        return 0

    def forward(l, _):
        def take(rows):
            return st[rows, :]

        norm_forward(l, 0, x1.at[l], take)

        @pl.when(l == 0)
        def _():
            stage_w(0, 0)
            direct_w(0, 1)

        gather_pass(x1.at[l], 0, 1, 2, 3)

        @pl.when(l == 0)
        def _():
            close_w(0, 0)

        gather_wait(x1.at[l])

        @pl.when(l == 0)
        def _():
            come_wait(1, cin)
            assemble(cin, gst)
            lax.fori_loop(0, CHUNK // 16, top_rows, 0)
            gather_start(gtop, second_z)

        need_w(l, 0)

        def qkv(s):
            value = dot(x1[l], wa[l, s]) + qb_ref[l, pl.ds(s, 1), :]
            triple[l, s] = value.astype(BF)

        tiles(3, qkv)
        attend(l)
        stage_w(l, 1)
        direct_w(l, 2)

        def proj(start, size):
            value = dot_t(att[l], wa[l, 3, pl.ds(start, size), :])
            part[:, pl.ds(start, size)] = value.astype(BF)

        features(proj, add_start)
        add_pass(0, 1, 2, 3)
        close_w(l, 1)
        add_wait()
        norm_forward(
            l, 1, x2.at[l], lambda rows: st[rows, :] + received(rows) + vector(6 * l + 4)
        )
        gather_pass(x2.at[l], 0, 1)
        stage_w(l, 2)

        @pl.when(l == 0)
        def _():
            direct_w(1, 0)

        gather_pass(x2.at[l], 2, 3)
        gather_wait(x2.at[l])
        close_w(l, 2)
        need_w(l, 1)

        @pl.when(l == 0)
        def _():
            gather_pass(gtop, 0, 1, 2, 3, sems=second_z)


        for h in range(2):

            def up(n):
                lanes = pl.ds(pl.multiple_of(n * 768, 128), 768)
                before = dot(x2[l], wm[l, h, :, lanes]) + ub_ref[pl.ds(l, 1), HALF * h : HALF * (h + 1)]
                half = before * (0.5**0.5)
                cdf = 0.5 + 0.5 * lax.erf(half)
                hid[l, h, :, lanes] = (before * cdf).astype(BF)
                density = jnp.exp(-half * half) * 0.3989422804014327
                slope[l, h, :, lanes] = (cdf + before * density).astype(slope.dtype)

            tiles(1, up)
        need_w(l, 2)

        @pl.when(l == 0)
        def _():
            features(down(l, part), add_start)
            stage_w(1, 0)
            direct_w(1, 1)
            add_pass(0, 1, 2, 3)
            close_w(1, 0)
            add_wait()
            lax.fori_loop(0, CHUNK // 16, settle(l, recv), 0)

        return 0

    lax.fori_loop(0, LAYERS, forward, 0)

    def transpose(src, index):
        def body(n):
            lanes = pl.ds(pl.multiple_of(n * 128, 128), 128)
            lt[index, lanes, :] = src[:, lanes].T

        tiles(D // 128, body)

    def piece(turn, n):
        return remote(
            sbuf.at[n % 2], prx.at[turn, n], cs_s.at[n], cs_r.at[turn, n], (other, r, c)
        )

    def block_tile(ref, i, b, k, left, right):
        rows = rblk(k)
        for j in range(2):
            lanes = pl.ds(PAD * j, PAD)
            if i == 0:
                s = 2 * b + j
                value = dot(lt[left(s), rows, :], right(s))
            else:
                value = dot(lt[left(b), rows, :], right(b)[:, lanes])
            ref[:, lanes] = value.astype(BF)

    order = (near[2], near[0], near[1], r)

    def half_copy(i, slot, k):
        half = pl.ds(k * (BLK // 2), BLK // 2)
        return remote(
            keep.at[slot, near[2], half], hop.at[i, k], hs.at[i, k], hr.at[i, k], (d, near[k], c)
        )

    def block_copy(i, slot, k, h):
        half = pl.ds(h * (BLK // 2), BLK // 2)
        return remote(
            keep.at[slot, near[k], half], ici.at[i, k, half], gis.at[i, k, h], gir.at[i, k, h],
            (d, near[k], c),
        )

    def merge(i, slot, turn, n):
        rows = prx.at[turn, n]
        pltpu.make_async_copy(rows, rows, cs_r.at[turn, n]).wait()

        def strip(t, _):
            rows = pl.ds(pl.multiple_of(16 * t, 16), 16)
            value = keep[slot, order[n], rows, :].astype(F32) + prx[turn, n, rows, :].astype(F32)
            keep[slot, order[n], rows, :] = value.astype(BF)
            return 0

        lax.fori_loop(0, BLK // 16, strip, 0)
        if n == 0:
            for k in range(2):
                half_copy(i, slot, k).start()
        elif n < 3:
            block_copy(i, slot, n - 1, n - 1).start()

    def make(i, slot, turn, left, right, first, n):
        if n == 0:

            @pl.when(first)
            def _():
                pl.semaphore_wait(credit, 1)

        if n >= 2:
            piece(turn, n - 2).wait_send()
        block_tile(sbuf.at[n % 2], i, other, order[n], left, right)
        piece(turn, n).start()
        block_tile(keep.at[slot, order[n]], i, d, order[n], left, right)
        if n > 0:
            merge(i, slot, turn, n - 1)
        if n == 3:
            merge(i, slot, turn, 3)
            for k in (2, 3):
                piece(turn, k).wait_send()
            pl.semaphore_signal(credit, inc=1, device_id=(other, r, c), device_id_type=MESH)

    def relay(i, slot):
        for k in range(2):
            pltpu.make_async_copy(hop.at[i, k], hop.at[i, k], hr.at[i, k]).wait()
            block = near[1 - k]

            def strip(t, _):
                rows = pl.ds(pl.multiple_of(16 * t, 16), 16)
                half = pl.ds(pl.multiple_of(k * (BLK // 2) + 16 * t, 16), 16)
                value = keep[slot, block, half, :].astype(F32) + hop[i, k, rows, :].astype(F32)
                keep[slot, block, half, :] = value.astype(BF)
                return 0

            lax.fori_loop(0, BLK // 32, strip, 0)
            block_copy(i, slot, 1 - k, k).start()

    def result(i, which, j):
        if i == 0:
            return ga_hbm.at[2 * which + j]
        lanes = pl.ds(pl.multiple_of(HALF * which + PAD * j, 128), PAD)
        return (gu_hbm if i == 1 else gd_hbm).at[:, lanes]

    def finish(l, i, slot):
        for k in range(2):
            for h in range(2):
                arrived = ici.at[i, k, pl.ds(h * (BLK // 2), BLK // 2)]
                pltpu.make_async_copy(arrived, arrived, gir.at[i, k, h]).wait()

        def body(t, _):
            rows = pl.ds(pl.multiple_of(16 * t, 16), 16)
            total = keep[slot, r, rows, :].astype(F32)
            for k in range(2):
                total = total + ici[i, k, rows, :].astype(F32)
            fin[0, rows, :] = total[:, 0:PAD]
            fin[1, rows, :] = total[:, PAD : 2 * PAD]
            return 0

        lax.fori_loop(0, BLK // 16, body, 0)

        @pl.when(l == d)
        def _():
            copies = [
                pltpu.make_async_copy(fin.at[j], result(i, d, j), fins.at[j]) for j in range(2)
            ]
            for copy in copies:
                copy.start()
            for copy in copies:
                copy.wait()

        @pl.when(l != d)
        def _():
            copies = [
                remote(fin.at[j], result(i, d, j), fins.at[j], finr.at[i, j], (other, r, c))
                for j in range(2)
            ]
            for copy in copies:
                copy.start()
            for copy in copies:
                copy.wait_send()

        for k in range(2):
            half_copy(i, slot, k).wait_send()
            for h in range(2):
                block_copy(i, slot, k, h).wait_send()

    def attend_back(l):
        for s in range(3):
            acc[s] = jnp.zeros((ROWS, PAD), F32)
        for head in range(4):
            mask, s0, s1 = head_mask(head)
            q = triple[l, 0, :, s0:s1] * mask
            keys = triple[l, 1, :, s0:s1]
            scores = dot_t(q, keys) * scaling
            scores = jnp.where(key_ok, scores, -1e30)
            probs = jnp.exp(scores - lse[l, :, head : head + 1])
            probs_low = probs.astype(BF)
            grad_heads = da[:, s0:s1] * mask
            acc[2, :, s0:s1] += t_dot(probs_low, grad_heads)
            grad_probs = dot_t(grad_heads, triple[l, 2, :, s0:s1])
            inner = jnp.sum(grad_probs * probs, axis=1, keepdims=True)
            grad_scores = (probs * (grad_probs - inner)).astype(BF)
            acc[0, :, s0:s1] += dot(grad_scores, keys * mask)
            acc[1, :, s0:s1] += t_dot(grad_scores, q)
        for s in range(3):
            value = acc[s] * scaling if s < 2 else acc[s]
            g3[s] = value.astype(BF)
        g3[3] = att[l]

    def backward(step, _):
        l = LAYERS - 1 - step

        @pl.when(step == 0)
        def _():
            gather_wait(gtop, second_z)

        @pl.when(step > 0)
        def _():
            gather_pass(gtop, 0, 1, 2, 3)
            relay(0, 0)
            finish(l + 1, 1, 1)
            gather_wait(gtop)
            add_pass(0, 1, 2, 3, path=side)

        for h in range(2):

            def hidden(n):
                lanes = pl.ds(pl.multiple_of(n * 768, 128), 768)
                value = dot(gtop[...], wm[l, 2 + h, :, lanes]) * slope[l, h, :, lanes].astype(F32)
                low = value.astype(BF)
                gb[h, :, lanes] = low
                csum[l, pl.ds(2 + h, 1), lanes] = jnp.sum(
                    low.astype(F32), axis=0, keepdims=True
                )

            tiles(1, hidden)

        def back_up(start, size):
            rows = pl.ds(start, size)
            value = dot_t(gb[0], wm[l, 0, rows, :]) + dot_t(gb[1], wm[l, 1, rows, :])
            part[:, pl.ds(start, size)] = value.astype(BF)

        features(back_up, add_start)
        transpose(gtop, 0)
        down_pair = (2, 0, lax.rem(step, 2), lambda b: 0, lambda b: hid.at[l, b], step > 0)

        @pl.when(step > 0)
        def _():
            finish(l + 1, 0, 0)

        make(*down_pair, 0)
        add_pass(0, 1)
        make(*down_pair, 1)
        add_pass(2)
        make(*down_pair, 2)
        add_pass(3)
        make(*down_pair, 3)
        add_wait()
        norm_backward(l, 1, gmid, 6 * l + 4)
        transpose(x2.at[l], 1)
        up_pair = (1, 1, lax.rem(step + 1, 2), lambda b: 1, lambda b: gb.at[b], step > 0)
        make(*up_pair, 0)
        gather_pass(gmid, 0, 1)
        make(*up_pair, 1)
        gather_pass(gmid, 2, 3)
        relay(2, 0)
        make(*up_pair, 2)
        make(*up_pair, 3)
        transpose(x1.at[l], 0)

        @pl.when(step == 0)
        def _():
            features(down(l, x2.at[LAYERS - 1]))

        gather_wait(gmid)

        @pl.when(step == 0)
        def _():
            for h in range(2):
                add_start(h, side)

        @pl.when(step > 0)
        def _():
            add_wait(side)
            lax.fori_loop(0, CHUNK // 16, settle(LAYERS - 1, recv2), 0)
            for k in range(N):
                oblk[k] = st[:, BLK * k : BLK * (k + 1)].astype(BF)
            go_start(2)

        da[...] = dot(gmid[...], wa[l, 3]).astype(BF)
        attend_back(l)
        relay(1, 1)
        for s in range(3):
            if s != 1:
                csum[l, s // 2 : s // 2 + 1, 0:PAD] = jnp.sum(
                    g3[s].astype(F32), axis=0, keepdims=True
                )

        def back_qkv(start, size):
            rows = pl.ds(start, size)
            value = dot_t(g3[0], wa[l, 0, rows, :])
            value = value + dot_t(g3[1], wa[l, 1, rows, :])
            value = value + dot_t(g3[2], wa[l, 2, rows, :])
            part[:, pl.ds(start, size)] = value.astype(BF)

        features(back_qkv, add_start)
        transpose(gmid, 1)
        finish(l, 2, 0)
        head_pair = (0, 0, lax.rem(step, 2), lambda s: s // 3, lambda s: g3[s], step >= 0)
        make(*head_pair, 0)
        add_pass(0)
        make(*head_pair, 1)
        add_pass(1, 2)
        make(*head_pair, 2)
        add_pass(3)
        make(*head_pair, 3)

        @pl.when(step > 0)
        def _():
            go_pass(2, out_hbm)

        add_wait()
        norm_backward(l, 0, gtop, jnp.where(l > 0, 6 * l - 1, 12))

        return 0

    lax.fori_loop(0, LAYERS, backward, 0)

    go_wait(2, out_hbm)
    sent(2)
    for k in range(N):
        oblk[k] = gst[:, BLK * k : BLK * (k + 1)].astype(BF)
    go_start(3)

    def c_copy(k):
        return remote(csum, cx.at[k], cxs.at[k], cxr.at[k], (d, near[k], c))

    def v_copy(k):
        return remote(vb.at[near[k]], vx.at[k], vxs.at[k], vxr.at[k], (d, near[k], c))

    def z_copy(k):
        return remote(
            vz.at[c], vz.at[c], vzs.at[k], vzr.at[c], (d, r, lax.rem(c + k + 1, N))
        )

    for k in range(N):
        vb[k] = vsum[:, BLK * k : BLK * (k + 1)]
    for k in range(3):
        v_copy(k).start()
        c_copy(k).start()
    go_pass(3, tg_hbm)
    relay(0, 0)
    total = vb[r]
    for k in range(3):
        v_copy(k).wait_recv()
        total = total + vx[k]
    vz[c] = total
    for k in range(3):
        z_copy(k).start()
    for k in range(3):
        c_copy(k).wait()
    for l in range(LAYERS):
        csum[l] = csum[l] + cx[0, l] + cx[1, l] + cx[2, l]
    c_half = remote(csum.at[other], cd, cds.at[0], cds.at[1], (other, r, c))
    c_half.start()
    for cs in range(N):

        @pl.when(c != cs)
        def _():
            pltpu.make_async_copy(vz.at[cs], vz.at[cs], vzr.at[cs]).wait()

    total = vz[0]
    for cs in range(1, N):
        total = total + vz[cs]
    vd[0] = total
    v_half = remote(vd.at[0], vd.at[1], vds.at[0], vds.at[1], (other, r, c))
    v_half.start()
    finish(0, 1, 1)
    finish(0, 0, 0)
    c_half.wait()
    cout[...] = csum[d] + cd[...]
    v_half.wait()
    vout[...] = vd[0] + vd[1]
    for k in range(3):
        v_copy(k).wait_send()
        z_copy(k).wait_send()

    pl.semaphore_wait(credit, 2)
    go_wait(3, tg_hbm)
    for u in (0, 1, 3):
        sent(u)
    for i in range(3):
        for j in range(2):
            arrived = result(i, other, j)
            pltpu.make_async_copy(arrived, arrived, finr.at[i, j]).wait()
    for k in range(3):
        remote(vec_ref, pin.at[r], vs.at[k], vr.at[k], (d, near[k], c)).wait_send()
    for l in range(LAYERS):
        for i in range(3):
            for k in range(2):
                for h in range(2):
                    send_w(l, i, k, h).wait_send()
                pass_w(l, i, k).wait_send()
            for k in range(3):
                share_w(l, i, k).wait_send()


def fused(*operands):
    dma = pltpu.SemaphoreType.DMA
    vmem = pltpu.VMEM
    whole = pl.BlockSpec(memory_space=pltpu.VMEM)
    anywhere = pl.BlockSpec(memory_space=pl.ANY)
    scratch = [
        vmem((LAYERS, 4, D, PAD), BF),
        vmem((LAYERS, 4, D, HALF), BF),
        vmem((LAYERS, ROWS, D), BF),
        vmem((LAYERS, ROWS, D), BF),
        vmem((LAYERS, 3, ROWS, PAD), BF),
        vmem((LAYERS, ROWS, PAD), BF),
        vmem((LAYERS, ROWS, 128), F32),
        vmem((LAYERS, 2, ROWS, HALF), BF),
        vmem((LAYERS, 2, ROWS, HALF), BF),
        vmem((LAYERS, 2, CHUNK, D), F32),
        vmem((LAYERS, 2, CHUNK, 128), F32),
        vmem((ROWS, D), BF),
        vmem((ROWS, D), BF),
        vmem((2, D, ROWS), BF),
        vmem((ROWS, D), BF),
        vmem((3, CHUNK, D), BF),
        vmem((CHUNK, D), F32),
        vmem((CHUNK, D), F32),
        vmem((N, CHUNK, BLK), BF),
        vmem((N, CHUNK, BLK), BF),
        vmem((N, CHUNK, BLK), BF),
        vmem((4, N, CHUNK, BLK), BF),
        vmem((N, 16, BLK), F32),
        vmem((16, D), F32),
        vmem((2, ROWS, HALF), BF),
        vmem((ROWS, PAD), BF),
        vmem((4, ROWS, PAD), BF),
        vmem((3, ROWS, PAD), F32),
        vmem((2, BLK, HALF), BF),
        vmem((2, N, BLK, HALF), BF),
        vmem((2, N, BLK, HALF), BF),
        vmem((3, 2, BLK, HALF), BF),
        vmem((2, BLK, PAD), F32),
        vmem((3, 2, BLK // 2, HALF), BF),
        vmem((2, LAST, D), BF),
        vmem((2, LAST, D), BF),
        vmem((3, CHUNK, D), BF),
        vmem((16, BLK), F32),
        vmem((LAYERS, 3, PAD), F32),
        vmem((16, D), F32),
        vmem((LAYERS, 4, HALF), F32),
        vmem((N, 16, BLK), F32),
        vmem((3, 16, BLK), F32),
        vmem((N, 16, BLK), F32),
        vmem((2, 16, BLK), F32),
        vmem((3, LAYERS, 4, HALF), F32),
        vmem((4, HALF), F32),
        dma((LAYERS, 3, 2)),
        dma((LAYERS, 3, 2, 2)), dma((LAYERS, 3, 2, 2)),
        dma((LAYERS, 3, 2)), dma((LAYERS, 3, 2)),
        dma((LAYERS, 3, 3)), dma((LAYERS, 3, 3)),
        dma((3,)), dma((4,)),
        dma((4, N)), dma((4, N)), dma((4, N)), dma((4, N)),
        dma((8,)), dma((N, 2)), dma((10,)), dma((4,)), dma((2, 2)),
        dma((N,)), dma((2, N)), pltpu.SemaphoreType.REGULAR,
        dma((3, 2, 2)), dma((3, 2, 2)), dma((2,)), dma((3, 2)),
        dma((3, 2)), dma((3, 2)),
        dma((8,)), dma((N, 2)), dma((10,)), dma((4,)), dma((2, 2)),
        dma((3,)), dma((3,)), dma((3,)), dma((N,)), dma((2,)),
        dma((3,)), dma((3,)), dma((2,)),
    ]
    shape = jax.ShapeDtypeStruct
    return pl.pallas_call(
        kernel,
        out_shape=(
            shape((ROWS, BLK), BF),
            shape((ROWS, BLK), BF),
            shape((4, BLK, PAD), F32),
            shape((BLK, 2 * HALF), F32),
            shape((BLK, 2 * HALF), F32),
            shape((16, BLK), F32),
            shape((4, HALF), F32),
        ),
        in_specs=[anywhere] * 4 + [whole] * 6,
        out_specs=(anywhere,) * 5 + (whole, whole),
        scratch_shapes=scratch,
        compiler_params=pltpu.CompilerParams(
            collective_id=0, has_side_effects=True, vmem_limit_bytes=67_043_328
        ),
    )(*operands)


def widen(values, axis=-1, to=PAD):
    axis = axis % values.ndim
    pads = [(0, 0)] * values.ndim
    pads[axis] = (0, to - values.shape[axis])
    return jnp.pad(values, pads)


def per_device_fused(
    tokens, cotangent, qkv_weight, qv_bias, proj_weight, proj_bias,
    up_weight, up_bias, down_weight, down_bias, norm_gain, norm_shift,
):
    dp = lax.axis_index("dp")
    both_in = widen(jnp.concatenate([tokens, cotangent]), 1, ROWS)
    heads = jnp.concatenate(
        [qkv_weight.transpose(0, 2, 1, 3), proj_weight.transpose(0, 2, 1)[:, None]], axis=1
    )
    down = down_weight.transpose(0, 2, 1)
    out, tg, ga, gu, gd, vout, cout = fused(
        both_in, widen(heads), up_weight, down,
        norm_gain, norm_shift, proj_bias, down_bias, qv_bias, up_bias,
    )
    both = vout[:12].reshape(LAYERS, 6, BLK)
    layer = lax.dynamic_slice(both, (dp, 0, 0), (1, 6, BLK))
    return (
        out[None, :SEQ].astype(F32),
        tg[None, :SEQ].astype(F32),
        ga[:3, :, :BLK].transpose(1, 0, 2)[None],
        cout[None, 0:2, :BLK],
        ga[3, :, :BLK].T[None],
        layer[:, 4],
        gu[None],
        cout[2:].reshape(1, 2 * HALF),
        gd.T[None],
        layer[:, 5],
        both[:, 0:2],
        both[:, 2:4],
    )


NORMAL = (((1,), (0,)), ((), ()))
LAST_BOTH = (((1,), (1,)), ((), ()))
FIRST_BOTH = (((0,), (0,)), ((), ()))


def gather_tokens(values):
    return lax.all_gather(values, "col", axis=0, tiled=True)


def gather_blocks(values):
    return lax.all_gather(values, "row", axis=0, tiled=True)


def gather_grad_blocks(values):
    return lax.all_gather(values, "row", axis=0, tiled=True)


def width_totals(first_sum, second_sum):
    return lax.psum((first_sum, second_sum), "row")


def gather_whole(triple_w, up_w, proj_w, down_w):
    row_whole = (triple_w, up_w, proj_w, down_w)
    col_whole = (proj_w, down_w, triple_w, up_w)
    return (row_whole, col_whole)


def row_product(gathered, matrix, contract):
    return lax.psum_scatter(
        lax.dot_general(gathered, matrix, contract, preferred_element_type=jnp.float32).astype(
            jnp.bfloat16
        ),
        "row",
        scatter_dimension=0,
        tiled=True,
    ).astype(jnp.float32)


def col_product(gathered, matrix, contract):
    return lax.psum_scatter(
        lax.dot_general(gathered, matrix, contract, preferred_element_type=jnp.float32).astype(
            jnp.bfloat16
        ),
        "col",
        scatter_dimension=0,
        tiled=True,
    ).astype(jnp.float32)


def norm_forward(stream, factor, shift):
    totals, squares = width_totals(jnp.sum(stream, axis=1), jnp.sum(stream * stream, axis=1))
    centre = totals / D
    spread = squares / D - centre * centre
    centred = stream - centre[:, None]
    scaling = lax.rsqrt(spread + EPSILON)
    standard = centred * scaling[:, None]
    return (standard * factor + shift, standard, scaling)


def norm_backward(grad_norm, standard, scaling, factor):
    factor_grad = jnp.sum(grad_norm * standard, axis=0)
    shift_grad = jnp.sum(grad_norm, axis=0)
    grad_standard = grad_norm * factor
    first_sum, second_sum = width_totals(
        jnp.sum(grad_standard, axis=1), jnp.sum(grad_standard * standard, axis=1)
    )
    grad_stream = scaling[:, None] * (
        grad_standard - first_sum[:, None] / D - standard * (second_sum[:, None] / D)
    )
    return (grad_stream, factor_grad, shift_grad)


def split_triple(triple_out, width):
    images = triple_out.shape[0] // SEQ
    head_count = width // HEAD_DIM
    pieces = triple_out.reshape(images, SEQ, 3, head_count, HEAD_DIM)
    return (pieces[:, :, 0], pieces[:, :, 1], pieces[:, :, 2])


def attend_forward(triple_out, width):
    queries, key_rows, values = split_triple(triple_out, width)
    scaling = HEAD_DIM ** (-0.5)
    scores = (
        jnp.einsum("bqhd,bkhd->bhqk", queries, key_rows, preferred_element_type=jnp.float32)
        * scaling
    )
    row_peak = jnp.max(scores, axis=-1, keepdims=True)
    log_totals = row_peak + jnp.log(jnp.sum(jnp.exp(scores - row_peak), axis=-1, keepdims=True))
    probs_low = jnp.exp(scores - log_totals).astype(jnp.bfloat16)
    attended = jnp.einsum("bhqk,bkhd->bqhd", probs_low, values, preferred_element_type=jnp.float32)
    return (attended.reshape(triple_out.shape[0], width).astype(jnp.bfloat16), log_totals)


def attend_backward(triple_out, log_totals, grad_attended, width):
    queries, key_rows, values = split_triple(triple_out, width)
    scaling = HEAD_DIM ** (-0.5)
    scores = (
        jnp.einsum("bqhd,bkhd->bhqk", queries, key_rows, preferred_element_type=jnp.float32)
        * scaling
    )
    probs = jnp.exp(scores - log_totals)
    probs_low = probs.astype(jnp.bfloat16)
    grad_heads = grad_attended.reshape(values.shape)
    grad_values = jnp.einsum(
        "bhqk,bqhd->bkhd", probs_low, grad_heads, preferred_element_type=jnp.float32
    )
    grad_probs = jnp.einsum(
        "bqhd,bkhd->bhqk", grad_heads, values, preferred_element_type=jnp.float32
    )
    grad_scores = (
        probs * (grad_probs - jnp.sum(grad_probs * probs, axis=-1, keepdims=True))
    ).astype(jnp.bfloat16)
    grad_queries = (
        jnp.einsum("bhqk,bkhd->bqhd", grad_scores, key_rows, preferred_element_type=jnp.float32)
        * scaling
    )
    grad_keys = (
        jnp.einsum("bhqk,bqhd->bkhd", grad_scores, queries, preferred_element_type=jnp.float32)
        * scaling
    )
    stacked = jnp.stack([grad_queries, grad_keys, grad_values], axis=2)
    return stacked.reshape(triple_out.shape[0], 3 * width).astype(jnp.bfloat16)


def layer_forward(stream, weights):
    qkv_w, qv_b, proj_w, proj_b, up_w, up_b, down_w, down_b, factors, shifts = weights
    width = qkv_w.shape[2]
    triple_w = qkv_w.reshape(qkv_w.shape[0], 3 * width)
    row_whole, col_whole = gather_whole(triple_w, up_w, proj_w, down_w)
    first_norm, first_standard, first_scaling = norm_forward(stream, factors[0], shifts[0])
    first_rows = gather_tokens(first_norm.astype(jnp.bfloat16))
    offsets = jnp.concatenate([qv_b[0], jnp.zeros_like(qv_b[0]), qv_b[1]])
    triple_out = (row_product(first_rows, triple_w, NORMAL) + offsets).astype(jnp.bfloat16)
    attended, log_totals = attend_forward(triple_out, width)
    head_rows = gather_blocks(attended)
    stream_mid = stream + col_product(head_rows, proj_w, NORMAL) + proj_b
    second_norm, second_standard, second_scaling = norm_forward(stream_mid, factors[1], shifts[1])
    second_rows = gather_tokens(second_norm.astype(jnp.bfloat16))
    before = row_product(second_rows, up_w, NORMAL) + up_b
    activated = jax.nn.gelu(before, approximate=False).astype(jnp.bfloat16)
    hidden_rows = gather_blocks(activated)
    branch_out = col_product(hidden_rows, down_w, NORMAL)
    stream_out = stream_mid + branch_out + down_b
    saved = (
        first_rows,
        first_standard,
        first_scaling,
        triple_out,
        log_totals,
        head_rows,
        second_rows,
        second_standard,
        second_scaling,
        before,
        hidden_rows,
        row_whole,
        col_whole,
    )
    return (stream_out, saved)


def layer_backward(grad_out, saved, weights):
    qkv_w, qv_b, proj_w, proj_b, up_w, up_b, down_w, down_b, factors, shifts = weights
    (
        first_rows,
        first_standard,
        first_scaling,
        triple_out,
        log_totals,
        head_rows,
        second_rows,
        second_standard,
        second_scaling,
        before,
        hidden_rows,
        row_whole,
        col_whole,
    ) = saved
    width = qkv_w.shape[2]
    triple_w = qkv_w.reshape(qkv_w.shape[0], 3 * width)
    grad_rows = gather_tokens(grad_out.astype(jnp.bfloat16))
    down_grad = lax.dot_general(
        hidden_rows, grad_rows, FIRST_BOTH, preferred_element_type=jnp.float32
    )
    down_off_grad = jnp.sum(grad_rows, axis=0, dtype=jnp.float32)
    grad_active = row_product(grad_rows, down_w, LAST_BOTH)
    _, slope_pull = jax.vjp(partial(jax.nn.gelu, approximate=False), before)
    grad_before = slope_pull(grad_active)[0].astype(jnp.bfloat16)
    before_rows = gather_grad_blocks(grad_before)
    up_grad = lax.dot_general(
        second_rows, before_rows, FIRST_BOTH, preferred_element_type=jnp.float32
    )
    up_off_grad = jnp.sum(before_rows, axis=0, dtype=jnp.float32)
    grad_second = col_product(before_rows, up_w, LAST_BOTH)
    grad_mid, second_factor_grad, second_shift_grad = norm_backward(
        grad_second, second_standard, second_scaling, factors[1]
    )
    grad_mid = grad_mid + grad_out
    mid_rows = gather_tokens(grad_mid.astype(jnp.bfloat16))
    proj_grad = lax.dot_general(head_rows, mid_rows, FIRST_BOTH, preferred_element_type=jnp.float32)
    proj_off_grad = jnp.sum(mid_rows, axis=0, dtype=jnp.float32)
    grad_attended = row_product(mid_rows, proj_w, LAST_BOTH).astype(jnp.bfloat16)
    grad_triple = attend_backward(triple_out, log_totals, grad_attended, width)
    triple_rows = gather_grad_blocks(grad_triple)
    triple_grad = lax.dot_general(
        first_rows, triple_rows, FIRST_BOTH, preferred_element_type=jnp.float32
    )
    column_sums = jnp.sum(triple_rows, axis=0, dtype=jnp.float32).reshape(3, width)
    qv_grad = jnp.stack([column_sums[0], column_sums[2]])
    grad_first = col_product(triple_rows, triple_w, LAST_BOTH)
    grad_in, first_factor_grad, first_shift_grad = norm_backward(
        grad_first, first_standard, first_scaling, factors[0]
    )
    grad_in = grad_in + grad_mid
    factor_grads = jnp.stack([first_factor_grad, second_factor_grad])
    shift_grads = jnp.stack([first_shift_grad, second_shift_grad])
    layer_grads = (
        triple_grad.reshape(qkv_w.shape),
        qv_grad,
        proj_grad,
        proj_off_grad,
        up_grad,
        up_off_grad,
        down_grad,
        down_off_grad,
        factor_grads,
        shift_grads,
    )
    return (grad_in, layer_grads)


def per_device_plain(
    tokens,
    cotangent,
    qkv_weight,
    qv_bias,
    proj_weight,
    proj_bias,
    up_weight,
    up_bias,
    down_weight,
    down_bias,
    norm_gain,
    norm_shift,
):
    image_count, seq_len, width_row = tokens.shape
    stream = tokens.reshape(image_count * seq_len, width_row).astype(jnp.float32)
    layer_params = []
    saved_list = []
    for layer_index in range(LAYERS):
        params = (
            qkv_weight[layer_index],
            qv_bias[layer_index],
            proj_weight[layer_index],
            proj_bias[layer_index],
            up_weight[layer_index],
            up_bias[layer_index],
            down_weight[layer_index],
            down_bias[layer_index],
            norm_gain[layer_index],
            norm_shift[layer_index],
        )
        layer_params.append(params)
        stream, saved = layer_forward(stream, params)
        saved_list.append(saved)
    grad_stream = cotangent.reshape(image_count * seq_len, width_row).astype(jnp.float32)
    per_layer = [None] * LAYERS
    for layer_index in reversed(range(LAYERS)):
        grad_stream, layer_grads = layer_backward(
            grad_stream, saved_list[layer_index], layer_params[layer_index]
        )
        per_layer[layer_index] = layer_grads
    stacked = tuple(
        (jnp.stack([layer_grads[position] for layer_grads in per_layer]) for position in range(10))
    )
    summed = (
        lax.psum_scatter(
            stacked[0].astype(jnp.bfloat16), "dp", scatter_dimension=0, tiled=True
        ).astype(jnp.float32),
        lax.psum_scatter(
            stacked[1].astype(jnp.bfloat16), "dp", scatter_dimension=0, tiled=True
        ).astype(jnp.float32),
        lax.psum_scatter(
            stacked[2].astype(jnp.bfloat16), "dp", scatter_dimension=0, tiled=True
        ).astype(jnp.float32),
        lax.psum_scatter(
            stacked[3].astype(jnp.bfloat16), "dp", scatter_dimension=0, tiled=True
        ).astype(jnp.float32),
        lax.psum_scatter(
            stacked[4].astype(jnp.bfloat16), "dp", scatter_dimension=0, tiled=True
        ).astype(jnp.float32),
        lax.psum_scatter(
            stacked[5].astype(jnp.bfloat16), "dp", scatter_dimension=0, tiled=True
        ).astype(jnp.float32),
        lax.psum_scatter(
            stacked[6].astype(jnp.bfloat16), "dp", scatter_dimension=0, tiled=True
        ).astype(jnp.float32),
        lax.psum_scatter(
            stacked[7].astype(jnp.bfloat16), "dp", scatter_dimension=0, tiled=True
        ).astype(jnp.float32),
    )
    norm_sums = lax.psum((stacked[8], stacked[9]), ("dp", "col"))
    result = stream.reshape(image_count, seq_len, width_row)
    tokens_grad = grad_stream.reshape(image_count, seq_len, width_row)
    return (
        result,
        tokens_grad,
        summed[0],
        summed[1],
        summed[2],
        summed[3],
        summed[4],
        summed[5],
        summed[6],
        summed[7],
        norm_sums[0],
        norm_sums[1],
    )


def solution(mesh):
    placed = (
        P(("dp", "col"), None, "row"),
        P(("dp", "col"), None, "row"),
        P(None, "row", None, "col"),
        P(None, None, "col"),
        P(None, "col", "row"),
        P(None, "row"),
        P(None, "row", "col"),
        P(None, "col"),
        P(None, "col", "row"),
        P(None, "row"),
        P(None, None, "row"),
        P(None, None, "row"),
    )
    sizes = (mesh.shape["dp"], mesh.shape["row"], mesh.shape["col"])
    return jax.shard_map(
        per_device_fused if sizes == (2, N, N) else per_device_plain,
        mesh=mesh,
        in_specs=placed,
        out_specs=(
            P(("dp", "col"), None, "row"),
            P(("dp", "col"), None, "row"),
            P("dp", "row", None, "col"),
            P("dp", None, "col"),
            P("dp", "col", "row"),
            P("dp", "row"),
            P("dp", "row", "col"),
            P("dp", "col"),
            P("dp", "col", "row"),
            P("dp", "row"),
            P(None, None, "row"),
            P(None, None, "row"),
        ),
        check_vma=False,
    )
```

```python
from functools import partial

import jax
import jax.numpy as jnp
from jax import lax
from jax.experimental import pallas as pl
from jax.experimental.pallas import tpu as pltpu
from jax.sharding import PartitionSpec as P

D = 1408
HEAD_DIM = 88
SEQ = 257
LAYERS = 2
EPSILON = 1e-06
MESH = pl.DeviceIdType.MESH
BF = jnp.bfloat16
F32 = jnp.float32

ROWS = 272
START = (0, 80, 128, 176)
SIZE = (80, 48, 48, 88)
FIRST = (40, 24, 24, 40)
CHUNK = 96
LAST = 88
BLK = 352
PAD = 384
HALF = 768
N = 4


def dot(a, b):
    return jnp.dot(a, b, preferred_element_type=F32)


def dot_t(a, b):
    return lax.dot_general(a, b, (((1,), (1,)), ((), ())), preferred_element_type=F32)


def t_dot(a, b):
    return lax.dot_general(a, b, (((0,), (0,)), ((), ())), preferred_element_type=F32)


def span(index):
    return pl.ds(START[index], SIZE[index])


def head_span(head):
    low, high = HEAD_DIM * head, HEAD_DIM * (head + 1)
    return low, high, low // 128 * 128, -(-high // 128) * 128


def kernel(
    io_hbm, wa_hbm, up_hbm, down_hbm, gain_ref, shift_ref, pb_ref, db_ref, qv_ref, ub_ref,
    out_hbm, tg_hbm, ga_hbm, gu_hbm, gd_hbm, vout, cout,
    wa, wm, x1, x2, triple, att, lse, hid, slope, std, inv,
    gtop, gmid, lt, part, recv, st, gst, tin, cin, oblk, mid, pin, pv,
    gb, da, g3, acc, sbuf, prx, keep, ici, fin, hop, rb, rb2, recv2,
    vec_ref, qb_ref, vsum, csum, vb, vx, vz, vd, cx, cd,
    wloc, wsend, wrecv, fsend, frecv, psend, precv, vs, vr, m1s, m1r, m2s, m2r,
    zs, zr, rss, rsr, lr, cs_s, cs_r, credit, gis, gir, fins, finr, hs, hr,
    zs2, zr2, rss2, rsr2, lr2, vxs, vxr, vzs, vzr, vds, cxs, cxr, cds,
):
    d, r, c = lax.axis_index("dp"), lax.axis_index("row"), lax.axis_index("col")
    other = 1 - d
    near = (r + 1 - 2 * lax.rem(r, 2), lax.rem(r + 2, N), N - 1 - r)
    last = c == N - 1

    def remote(src, dst, ssem, rsem, dev):
        return pltpu.make_async_remote_copy(
            src, dst, ssem, rsem, device_id=dev, device_id_type=MESH
        )

    def rblk(index):
        return pl.ds(pl.multiple_of(index * BLK, 16), BLK)

    def rhalf(index, part_):
        return pl.ds(pl.multiple_of(index * BLK + part_ * (BLK // 2), 16), BLK // 2)

    recv[...] = jnp.zeros_like(recv)
    recv2[...] = jnp.zeros_like(recv2)
    for array in (x1.at[0], x1.at[1], x2.at[0], x2.at[1], gtop, gmid):
        array[ROWS - 16 :, :] = jnp.zeros((16, D), BF)
    tin[...] = jnp.zeros_like(tin)
    cin[...] = jnp.zeros_like(cin)
    vsum[...] = jnp.zeros_like(vsum)
    csum[...] = jnp.zeros_like(csum)
    vec_ref[...] = jnp.zeros_like(vec_ref)
    qb_ref[...] = jnp.zeros_like(qb_ref)
    for l in range(LAYERS):
        for j in range(2):
            vec_ref[6 * l + j : 6 * l + j + 1, :] = gain_ref[l, j : j + 1, :]
            vec_ref[6 * l + 2 + j : 6 * l + 3 + j, :] = shift_ref[l, j : j + 1, :]
            qb_ref[l, 2 * j : 2 * j + 1, 0:BLK] = qv_ref[l, j : j + 1, :]
        vec_ref[6 * l + 4 : 6 * l + 5, :] = pb_ref[l : l + 1, :]
        vec_ref[6 * l + 5 : 6 * l + 6, :] = db_ref[l : l + 1, :]
    barrier = pltpu.get_barrier_semaphore()
    for k in range(N * N):
        pl.semaphore_signal(
            barrier, inc=1,
            device_id=(d, lax.rem(r + k // N, N), lax.rem(c + k % N, N)), device_id_type=MESH,
        )
    pl.semaphore_signal(barrier, inc=1, device_id=(other, r, c), device_id_type=MESH)
    pl.semaphore_wait(barrier, N * N + 1)

    for k in range(3):
        remote(vec_ref, pin.at[r], vs.at[k], vr.at[k], (d, near[k], c)).start()
    own_vec = pltpu.make_async_copy(vec_ref, pin.at[r], vr.at[3])
    own_vec.start()

    def by_size(body):
        @pl.when(c == 0)
        def _():
            body(SIZE[0])

        @pl.when(jnp.logical_and(c > 0, c < N - 1))
        def _():
            body(SIZE[1])

        @pl.when(last)
        def _():
            body(SIZE[N - 1])

    begin = jnp.where(c < 2, 80 * c, 48 * c + 32)
    count = jnp.where(c == 0, 5, jnp.where(last, 6, 3))
    ahead = jnp.where(jnp.logical_or(c == 0, last), 3, 2)

    def come_start(u, src):
        for ct in range(N):
            size = SIZE[ct]
            source, target = src.at[span(ct)], mid.at[u, c, pl.ds(0, size)]

            @pl.when(c == ct)
            def _():
                pltpu.make_async_copy(source, target, m1r.at[u, c]).start()

            @pl.when(c != ct)
            def _():
                remote(source, target, m1s.at[u, ct], m1r.at[u, c], (d, r, ct)).start()

    def come_pass(u, dst):
        def sized(size):
            rows = pl.ds(0, size)
            for p in range(N):
                source, target = mid.at[u, p, rows], dst.at[r, rows]
                pltpu.make_async_copy(source, source, m1r.at[u, p]).wait()

                @pl.when(r == p)
                def _():
                    pltpu.make_async_copy(source, target, m2r.at[u, r]).start()

                @pl.when(r != p)
                def _():
                    remote(source, target, m2s.at[u, p], m2r.at[u, r], (d, p, c)).start()

        by_size(sized)

    def come_wait(u, dst):
        def sized(size):
            for rs in range(N):
                rows = dst.at[rs, pl.ds(0, size)]
                pltpu.make_async_copy(rows, rows, m2r.at[u, rs]).wait()

        by_size(sized)

    def go_start(u):
        def sized(size):
            rows = pl.ds(0, size)
            for k in range(N):
                source, target = oblk.at[k, rows], mid.at[u, r, rows]

                @pl.when(r == k)
                def _():
                    pltpu.make_async_copy(source, target, m1r.at[u, r]).start()

                @pl.when(r != k)
                def _():
                    remote(source, target, m1s.at[u, k], m1r.at[u, r], (d, k, c)).start()

        by_size(sized)

    def go_pass(u, dst):
        def sized(size):
            for p in range(N):
                source = mid.at[u, p, pl.ds(0, size)]
                target = dst.at[pl.ds(pl.multiple_of(begin, 16), size)]
                pltpu.make_async_copy(source, source, m1r.at[u, p]).wait()

                @pl.when(c == p)
                def _():
                    pltpu.make_async_copy(source, target, m2r.at[u, c]).start()

                @pl.when(c != p)
                def _():
                    remote(source, target, m2s.at[u, p], m2r.at[u, c], (d, r, p)).start()

        by_size(sized)

    def go_wait(u, dst):
        for cs in range(N):
            rows = dst.at[span(cs)]
            pltpu.make_async_copy(rows, rows, m2r.at[u, cs]).wait()

    def sent(u):
        for ct in range(N):
            size = SIZE[ct]
            rows = mid.at[u, 0, pl.ds(0, size)]

            if u < 2:

                @pl.when(c != ct)
                def _():
                    remote(rows, rows, m1s.at[u, ct], m1r.at[u, 0], (d, r, ct)).wait_send()

            def second(size):
                rows = mid.at[u, 0, pl.ds(0, size)]
                first_row = u < 2

                @pl.when((r != ct) if first_row else (c != ct))
                def _():
                    remote(rows, rows, m2s.at[u, ct], m2r.at[u, 0], (d, r, c)).wait_send()

                if not first_row:

                    @pl.when(r != ct)
                    def _():
                        remote(rows, rows, m1s.at[u, ct], m1r.at[u, 0], (d, ct, c)).wait_send()

            by_size(second)

    come_start(0, io_hbm.at[0])

    def source_w(l, i, which, rows):
        if i == 0:
            return wa_hbm.at[l, pl.ds(2 * which, 2), rows, :]
        lanes = pl.ds(pl.multiple_of(HALF * which, 128), HALF)
        return (up_hbm if i == 1 else down_hbm).at[l, rows, lanes]

    def rows_w(l, i, which, block):
        if i == 0:
            return wa.at[l, pl.ds(2 * which, 2), block, :]
        return wm.at[l, 2 * (i - 1) + which, block, :]

    def local_w(l, i, which):
        return pltpu.make_async_copy(
            source_w(l, i, which, pl.ds(0, BLK)), rows_w(l, i, which, rblk(r)), wloc.at[l, i, which]
        )

    def send_w(l, i, k, h):
        return remote(
            source_w(l, i, d, pl.ds(h * (BLK // 2), BLK // 2)), rows_w(l, i, d, rhalf(r, h)),
            wsend.at[l, i, k, h], wrecv.at[l, i, k, h], (d, near[k], c),
        )

    def pass_w(l, i, k):
        rows = rows_w(l, i, d, rhalf(near[k], k))
        return remote(rows, rows, fsend.at[l, i, k], frecv.at[l, i, k], (d, near[1 - k], c))

    def share_w(l, i, k):
        rows = rows_w(l, i, d, rblk(near[k]))
        return remote(rows, rows, psend.at[l, i, k], precv.at[l, i, k], (other, r, c))

    def direct_w(l, i, parts=(0, 1)):
        for part_ in parts:
            for k in range(2):
                send_w(l, i, k, k if part_ == 0 else 1 - k).start()

    def stage_w(l, i):
        for k in range(2):
            send_w(l, i, k, k).wait_recv()
            pass_w(l, i, k).start()
        for k in range(2):
            send_w(l, i, k, 1 - k).wait_recv()
            share_w(l, i, k).start()

    def close_w(l, i):
        for k in range(2):
            rows = rows_w(l, i, d, rhalf(near[2], k))
            pltpu.make_async_copy(rows, rows, frecv.at[l, i, k]).wait()
        share_w(l, i, 2).start()

    def need_w(l, i):
        for which in range(2):
            local_w(l, i, which).wait()
        for k in range(3):
            rows = rows_w(l, i, other, rblk(near[k]))
            pltpu.make_async_copy(rows, rows, precv.at[l, i, k]).wait()

    direct_w(0, 0, (0,))
    come_pass(0, tin)
    direct_w(0, 0, (1,))
    come_start(1, io_hbm.at[1])
    for l in range(LAYERS):
        for i in range(3):
            for which in range(2):
                local_w(l, i, which).start()

    def half_rows(cs, h):
        return pl.ds(START[cs] + FIRST[cs] * h, FIRST[cs] if h == 0 else SIZE[cs] - FIRST[cs])

    halves = ((0, 0), (1, 0), (0, 1), (1, 1))
    targets = ((2, 1), (2, 0), (1, 3), (1, 2))
    relays = ((1, 0, [(2 + far, h) for far, h in halves]), (2, 3, [(1 - far, h) for far, h in halves]))

    first_z, second_z = (zs, zr), (zs2, zr2)

    def gather_start(x, sems=first_z, steps=(0, 1, 2, 3)):
        zs, zr = sems
        for c0 in range(N):

            @pl.when(c == c0)
            def _():
                for n in steps:
                    rows = x.at[half_rows(c0, n % 2)]
                    remote(
                        rows, rows, zs.at[n], zr.at[c0, n % 2], (d, r, targets[c0][n // 2])
                    ).start()

    def gather_pass(x, *steps, sems=first_z):
        zs, zr = sems
        for c0, far, order in relays:

            @pl.when(c == c0)
            def _():
                for n in steps:
                    cs, h = order[n]
                    rows = x.at[half_rows(cs, h)]
                    pltpu.make_async_copy(rows, rows, zr.at[cs, h]).wait()
                    remote(rows, rows, zs.at[4 + n], zr.at[cs, h], (d, r, far)).start()

    def gather_wait(x, sems=first_z):
        zs, zr = sems
        for c0 in range(N):
            passed = [order for at, _, order in relays if at == c0]

            @pl.when(c == c0)
            def _():
                for cs in range(N):
                    for h in range(2):
                        if cs != c0 and not (passed and (cs, h) in passed[0]):
                            rows = x.at[half_rows(cs, h)]
                            pltpu.make_async_copy(rows, rows, zr.at[cs, h]).wait()
                for n in range(4):
                    rows = x.at[half_rows(c0, n % 2)]
                    remote(rows, rows, zs.at[n], zr.at[c0, 0], (d, r, targets[c0][0])).wait_send()
                if passed:
                    for n, (cs, h) in enumerate(passed[0]):
                        rows = x.at[half_rows(cs, h)]
                        remote(rows, rows, zs.at[4 + n], zr.at[cs, h], (d, r, 0)).wait_send()

    sides = ((0, 1, (3, 2)), (3, 2, (0, 1)))
    inner = ((1, 0), (2, 3))

    def size_of(cs):
        return SIZE[cs]

    def cols(h):
        return pl.ds(0, HALF) if h == 0 else pl.ds(HALF, D - HALF)

    main = (part, rb, recv, rss, rsr, lr)
    side = (x2.at[LAYERS - 1], rb2, recv2, rss2, rsr2, lr2)

    def end_copy(n, h, middle, dest, path):
        part, rb, recv, rss, rsr, lr = path
        return remote(
            part.at[span(dest), cols(h)], rb.at[n, pl.ds(0, size_of(dest)), cols(h)],
            rss.at[2 * n + h], lr.at[n, h], (d, r, middle),
        )

    def single_copy(dest, h, path):
        part, rb, recv, rss, rsr, lr = path
        return remote(
            part.at[span(dest), cols(h)], recv.at[1, pl.ds(0, size_of(dest)), cols(h)],
            rss.at[4 + h], rsr.at[h], (d, r, dest),
        )

    def sum_copy(n, h, dest, path):
        part, rb, recv, rss, rsr, lr = path
        rows = pl.ds(0, size_of(dest))
        return remote(
            rb.at[n, rows, cols(h)], recv.at[2, rows, cols(h)], rss.at[6 + 2 * n + h],
            rsr.at[2 + h], (d, r, dest),
        )

    def add_start(h, path=main):
        for end, middle, dests in sides:

            @pl.when(c == end)
            def _():
                for n in range(2):
                    end_copy(n, h, middle, dests[n], path).start()
                single_copy(middle, h, path).start()

        for middle, end in inner:

            @pl.when(c == middle)
            def _():
                single_copy(end, h, path).start()

        for cs in range(N):

            @pl.when(c == cs)
            def _():
                path[2][0, 0 : size_of(cs), cols(h)] = path[0][span(cs), cols(h)]

    def add_pass(*steps, path=main):
        part, rb, recv, rss, rsr, lr = path
        for end, middle, dests in sides:

            @pl.when(c == middle)
            def _():
                for step in steps:
                    h, n = step // 2, step % 2
                    dest = dests[n]
                    size = size_of(dest)
                    rows = rb.at[n, pl.ds(0, size), cols(h)]
                    pltpu.make_async_copy(rows, rows, lr.at[n, h]).wait()
                    for start in range(0, size, 16):
                        width = min(16, size - start)
                        mine = part[pl.ds(START[dest] + start, width), cols(h)]
                        value = rb[n, start : start + width, cols(h)].astype(F32)
                        rb[n, start : start + width, cols(h)] = (
                            value + mine.astype(F32)
                        ).astype(BF)
                    sum_copy(n, h, dest, path).start()

    def add_wait(path=main):
        part, rb, recv, rss, rsr, lr = path
        for cs in range(N):

            @pl.when(c == cs)
            def _():
                for k in (1, 2):
                    for h in range(2):
                        rows = recv.at[k, pl.ds(0, size_of(cs)), cols(h)]
                        pltpu.make_async_copy(rows, rows, rsr.at[2 * (k - 1) + h]).wait()

        for end, middle, dests in sides:

            @pl.when(c == end)
            def _():
                for h in range(2):
                    for n in range(2):
                        end_copy(n, h, middle, dests[n], path).wait_send()
                    single_copy(middle, h, path).wait_send()

            @pl.when(c == middle)
            def _():
                for h in range(2):
                    single_copy(end, h, path).wait_send()
                    for n in range(2):
                        sum_copy(n, h, dests[n], path).wait_send()

    def received(rows, recv=recv):
        total = recv[0, rows, :].astype(F32)
        for k in range(1, recv.shape[0]):
            total = total + recv[k, rows, :].astype(F32)
        return total

    def vector(row):
        return pv[pl.ds(row, 1), :]

    def own_rows(x, t, value):
        x[pl.ds(pl.multiple_of(begin + 16 * t, 16), 16), :] = value

    valid = jnp.where(last, SEQ - START[N - 1], 16 * count)

    def masked(t, value):
        index = lax.broadcasted_iota(jnp.int32, (16, 1), 0) + 16 * t
        return jnp.where(index < valid, value, 0.0)

    def early(x, body):
        lax.fori_loop(0, ahead, body, 0)
        gather_start(x, steps=(0,))
        lax.fori_loop(ahead, count, body, 0)
        gather_start(x, steps=(1, 2, 3))

    def norm_forward(l, j, x, extra):
        def body(t, _):
            rows = pl.ds(pl.multiple_of(16 * t, 16), 16)
            v = extra(rows)
            st[rows, :] = v
            centre = jnp.sum(v, axis=1, keepdims=True) / D
            spread_ = jnp.sum(v * v, axis=1, keepdims=True) / D - centre * centre
            scale = lax.rsqrt(spread_ + EPSILON)
            standard = (v - centre) * scale
            std[l, j, rows, :] = standard.astype(BF)
            inv[l, j, rows, :] = jnp.broadcast_to(scale, (16, 128))
            value = standard * vector(6 * l + j) + vector(6 * l + 2 + j)
            own_rows(x, t, value.astype(BF))
            return 0

        early(x, body)

    def norm_backward(l, j, x, bias_row):
        def body(t, _):
            rows = pl.ds(pl.multiple_of(16 * t, 16), 16)
            e = received(rows)
            standard = std[l, j, rows, :].astype(F32)
            gain_term = masked(t, e * standard)
            vsum[pl.ds(6 * l + j, 1), :] += jnp.sum(gain_term, axis=0, keepdims=True)
            vsum[pl.ds(6 * l + 2 + j, 1), :] += jnp.sum(masked(t, e), axis=0, keepdims=True)
            f = e * vector(6 * l + j)
            first = jnp.sum(f, axis=1, keepdims=True) / D
            second = jnp.sum(f * standard, axis=1, keepdims=True) / D
            scale = inv[l, j, rows, 0:1]
            grad = gst[rows, :] + scale * (f - first - standard * second)
            gst[rows, :] = grad
            if x is not None:
                low = grad.astype(BF)
                own_rows(x, t, low)
                vsum[pl.ds(bias_row, 1), :] += jnp.sum(
                    masked(t, low.astype(F32)), axis=0, keepdims=True
                )
            return 0

        if j == 1:
            early(x, body)
        else:

            @pl.when(l > 0)
            def _():
                early(x, body)

            @pl.when(l == 0)
            def _():
                lax.fori_loop(0, count, body, 0)

    def tiles(count, body):
        lax.fori_loop(0, count, lambda n, _: (body(n), 0)[1], 0)

    def features(body, start=None):
        body(0, 768)
        if start is not None:
            start(0)
        body(HALF, 640)
        if start is not None:
            start(1)

    def assemble(src, dst):
        for k in range(N):
            dst[:, BLK * k : BLK * (k + 1)] = src[k, :, 0:BLK].astype(F32)

    for k in range(3):
        remote(vec_ref, pin.at[r], vs.at[k], vr.at[k], (d, near[k], c)).wait_recv()
    own_vec.wait()
    assemble(pin, pv)
    come_wait(0, tin)
    come_pass(1, cin)
    assemble(tin, st)

    lane = lax.broadcasted_iota(jnp.int32, (1, PAD), 1)
    key_ok = lax.broadcasted_iota(jnp.int32, (1, ROWS), 1) < SEQ
    scaling = HEAD_DIM**-0.5

    def head_mask(head):
        low, high, s0, s1 = head_span(head)
        lanes = lane[:, s0:s1]
        return jnp.logical_and(lanes >= low, lanes < high).astype(BF), s0, s1

    def attend(l):
        acc[0] = jnp.zeros((ROWS, PAD), F32)
        for head in range(4):
            mask, s0, s1 = head_mask(head)
            q = triple[l, 0, :, s0:s1] * mask
            scores = dot_t(q, triple[l, 1, :, s0:s1]) * scaling
            scores = jnp.where(key_ok, scores, -1e30)
            peak = jnp.max(scores, axis=1, keepdims=True)
            total = peak + jnp.log(jnp.sum(jnp.exp(scores - peak), axis=1, keepdims=True))
            lse[l, :, head : head + 1] = total
            probs = jnp.exp(scores - total).astype(BF)
            acc[0, :, s0:s1] += dot(probs, triple[l, 2, :, s0:s1] * mask)
        att[l] = acc[0].astype(BF)

    def down(l, target):
        def body(start, size):
            rows = pl.ds(start, size)
            value = dot_t(hid[l, 0], wm[l, 2, rows, :]) + dot_t(hid[l, 1], wm[l, 3, rows, :])
            target[:, rows] = value.astype(BF)

        return body

    def settle(l, recv):
        def body(t, _):
            rows = pl.ds(pl.multiple_of(16 * t, 16), 16)
            st[rows, :] = st[rows, :] + received(rows, recv) + vector(6 * l + 5)
            return 0

        return body

    def top_rows(t, _):
        rows = pl.ds(pl.multiple_of(16 * t, 16), 16)
        low = gst[rows, :].astype(BF)
        own_rows(gtop, t, low)
        vsum[pl.ds(6 * (LAYERS - 1) + 5, 1), :] += jnp.sum(
            masked(t, low.astype(F32)), axis=0, keepdims=True
        )
        return 0

    def forward(l, _):
        def take(rows):
            return st[rows, :]

        norm_forward(l, 0, x1.at[l], take)

        @pl.when(l == 0)
        def _():
            stage_w(0, 0)
            direct_w(0, 1)

        gather_pass(x1.at[l], 0, 1, 2, 3)

        @pl.when(l == 0)
        def _():
            close_w(0, 0)

        gather_wait(x1.at[l])

        @pl.when(l == 0)
        def _():
            come_wait(1, cin)
            assemble(cin, gst)
            lax.fori_loop(0, count, top_rows, 0)
            gather_start(gtop, second_z)

        need_w(l, 0)

        def qkv(s):
            value = dot(x1[l], wa[l, s]) + qb_ref[l, pl.ds(s, 1), :]
            triple[l, s] = value.astype(BF)

        tiles(3, qkv)
        attend(l)
        stage_w(l, 1)
        direct_w(l, 2)

        def proj(start, size):
            value = dot_t(att[l], wa[l, 3, pl.ds(start, size), :])
            part[:, pl.ds(start, size)] = value.astype(BF)

        features(proj, add_start)
        add_pass(0, 1, 2, 3)
        close_w(l, 1)
        add_wait()
        norm_forward(
            l, 1, x2.at[l], lambda rows: st[rows, :] + received(rows) + vector(6 * l + 4)
        )
        gather_pass(x2.at[l], 0, 1)
        stage_w(l, 2)

        @pl.when(l == 0)
        def _():
            direct_w(1, 0)

        gather_pass(x2.at[l], 2, 3)
        gather_wait(x2.at[l])
        close_w(l, 2)
        need_w(l, 1)

        @pl.when(l == 0)
        def _():
            gather_pass(gtop, 0, 1, 2, 3, sems=second_z)


        for h in range(2):

            def up(n):
                lanes = pl.ds(pl.multiple_of(n * 768, 128), 768)
                before = dot(x2[l], wm[l, h, :, lanes]) + ub_ref[pl.ds(l, 1), HALF * h : HALF * (h + 1)]
                half = before * (0.5**0.5)
                cdf = 0.5 + 0.5 * lax.erf(half)
                hid[l, h, :, lanes] = (before * cdf).astype(BF)
                density = jnp.exp(-half * half) * 0.3989422804014327
                slope[l, h, :, lanes] = (cdf + before * density).astype(slope.dtype)

            tiles(1, up)
        need_w(l, 2)

        @pl.when(l == 0)
        def _():
            features(down(l, part), add_start)
            stage_w(1, 0)
            direct_w(1, 1)
            add_pass(0, 1, 2, 3)
            close_w(1, 0)
            add_wait()
            lax.fori_loop(0, count, settle(l, recv), 0)

        return 0

    lax.fori_loop(0, LAYERS, forward, 0)

    def transpose(src, index):
        def body(n):
            lanes = pl.ds(pl.multiple_of(n * 128, 128), 128)
            lt[index, lanes, :] = src[:, lanes].T

        tiles(D // 128, body)

    def piece(turn, n):
        return remote(
            sbuf.at[n % 2], prx.at[turn, n], cs_s.at[n], cs_r.at[turn, n], (other, r, c)
        )

    def block_tile(ref, i, b, k, left, right):
        rows = rblk(k)
        for j in range(2):
            lanes = pl.ds(PAD * j, PAD)
            if i == 0:
                s = 2 * b + j
                value = dot(lt[left(s), rows, :], right(s))
            else:
                value = dot(lt[left(b), rows, :], right(b)[:, lanes])
            ref[:, lanes] = value.astype(BF)

    order = (near[2], near[0], near[1], r)

    def half_copy(i, slot, k):
        half = pl.ds(k * (BLK // 2), BLK // 2)
        return remote(
            keep.at[slot, near[2], half], hop.at[i, k], hs.at[i, k], hr.at[i, k], (d, near[k], c)
        )

    def block_copy(i, slot, k, h):
        half = pl.ds(h * (BLK // 2), BLK // 2)
        return remote(
            keep.at[slot, near[k], half], ici.at[i, k, half], gis.at[i, k, h], gir.at[i, k, h],
            (d, near[k], c),
        )

    def merge(i, slot, turn, n):
        rows = prx.at[turn, n]
        pltpu.make_async_copy(rows, rows, cs_r.at[turn, n]).wait()

        def strip(t, _):
            rows = pl.ds(pl.multiple_of(16 * t, 16), 16)
            value = keep[slot, order[n], rows, :].astype(F32) + prx[turn, n, rows, :].astype(F32)
            keep[slot, order[n], rows, :] = value.astype(BF)
            return 0

        lax.fori_loop(0, BLK // 16, strip, 0)
        if n == 0:
            for k in range(2):
                half_copy(i, slot, k).start()
        elif n < 3:
            block_copy(i, slot, n - 1, n - 1).start()

    def make(i, slot, turn, left, right, first, n):
        if n == 0:

            @pl.when(first)
            def _():
                pl.semaphore_wait(credit, 1)

        if n >= 2:
            piece(turn, n - 2).wait_send()
        block_tile(sbuf.at[n % 2], i, other, order[n], left, right)
        piece(turn, n).start()
        block_tile(keep.at[slot, order[n]], i, d, order[n], left, right)
        if n > 0:
            merge(i, slot, turn, n - 1)
        if n == 3:
            merge(i, slot, turn, 3)
            for k in (2, 3):
                piece(turn, k).wait_send()
            pl.semaphore_signal(credit, inc=1, device_id=(other, r, c), device_id_type=MESH)

    def relay(i, slot):
        for k in range(2):
            pltpu.make_async_copy(hop.at[i, k], hop.at[i, k], hr.at[i, k]).wait()
            block = near[1 - k]

            def strip(t, _):
                rows = pl.ds(pl.multiple_of(16 * t, 16), 16)
                half = pl.ds(pl.multiple_of(k * (BLK // 2) + 16 * t, 16), 16)
                value = keep[slot, block, half, :].astype(F32) + hop[i, k, rows, :].astype(F32)
                keep[slot, block, half, :] = value.astype(BF)
                return 0

            lax.fori_loop(0, BLK // 32, strip, 0)
            block_copy(i, slot, 1 - k, k).start()

    def result(i, which, j):
        if i == 0:
            return ga_hbm.at[2 * which + j]
        lanes = pl.ds(pl.multiple_of(HALF * which + PAD * j, 128), PAD)
        return (gu_hbm if i == 1 else gd_hbm).at[:, lanes]

    def finish(l, i, slot):
        for k in range(2):
            for h in range(2):
                arrived = ici.at[i, k, pl.ds(h * (BLK // 2), BLK // 2)]
                pltpu.make_async_copy(arrived, arrived, gir.at[i, k, h]).wait()

        def body(t, _):
            rows = pl.ds(pl.multiple_of(16 * t, 16), 16)
            total = keep[slot, r, rows, :].astype(F32)
            for k in range(2):
                total = total + ici[i, k, rows, :].astype(F32)
            fin[0, rows, :] = total[:, 0:PAD]
            fin[1, rows, :] = total[:, PAD : 2 * PAD]
            return 0

        lax.fori_loop(0, BLK // 16, body, 0)

        @pl.when(l == d)
        def _():
            copies = [
                pltpu.make_async_copy(fin.at[j], result(i, d, j), fins.at[j]) for j in range(2)
            ]
            for copy in copies:
                copy.start()
            for copy in copies:
                copy.wait()

        @pl.when(l != d)
        def _():
            copies = [
                remote(fin.at[j], result(i, d, j), fins.at[j], finr.at[i, j], (other, r, c))
                for j in range(2)
            ]
            for copy in copies:
                copy.start()
            for copy in copies:
                copy.wait_send()

        for k in range(2):
            half_copy(i, slot, k).wait_send()
            for h in range(2):
                block_copy(i, slot, k, h).wait_send()

    def attend_back(l):
        for s in range(3):
            acc[s] = jnp.zeros((ROWS, PAD), F32)
        for head in range(4):
            mask, s0, s1 = head_mask(head)
            q = triple[l, 0, :, s0:s1] * mask
            keys = triple[l, 1, :, s0:s1]
            scores = dot_t(q, keys) * scaling
            scores = jnp.where(key_ok, scores, -1e30)
            probs = jnp.exp(scores - lse[l, :, head : head + 1])
            probs_low = probs.astype(BF)
            grad_heads = da[:, s0:s1] * mask
            acc[2, :, s0:s1] += t_dot(probs_low, grad_heads)
            grad_probs = dot_t(grad_heads, triple[l, 2, :, s0:s1])
            inner = jnp.sum(grad_probs * probs, axis=1, keepdims=True)
            grad_scores = (probs * (grad_probs - inner)).astype(BF)
            acc[0, :, s0:s1] += dot(grad_scores, keys * mask)
            acc[1, :, s0:s1] += t_dot(grad_scores, q)
        for s in range(3):
            value = acc[s] * scaling if s < 2 else acc[s]
            g3[s] = value.astype(BF)
        g3[3] = att[l]

    def backward(step, _):
        l = LAYERS - 1 - step

        @pl.when(step == 0)
        def _():
            gather_wait(gtop, second_z)

        @pl.when(step > 0)
        def _():
            gather_pass(gtop, 0, 1, 2, 3)
            relay(0, 0)
            finish(l + 1, 1, 1)
            gather_wait(gtop)
            add_pass(0, 1, 2, 3, path=side)

        for h in range(2):

            def hidden(n):
                lanes = pl.ds(pl.multiple_of(n * 768, 128), 768)
                value = dot(gtop[...], wm[l, 2 + h, :, lanes]) * slope[l, h, :, lanes].astype(F32)
                low = value.astype(BF)
                gb[h, :, lanes] = low
                csum[l, pl.ds(2 + h, 1), lanes] = jnp.sum(
                    low.astype(F32), axis=0, keepdims=True
                )

            tiles(1, hidden)

        def back_up(start, size):
            rows = pl.ds(start, size)
            value = dot_t(gb[0], wm[l, 0, rows, :]) + dot_t(gb[1], wm[l, 1, rows, :])
            part[:, pl.ds(start, size)] = value.astype(BF)

        features(back_up, add_start)
        transpose(gtop, 0)
        down_pair = (2, 0, lax.rem(step, 2), lambda b: 0, lambda b: hid.at[l, b], step > 0)

        @pl.when(step > 0)
        def _():
            finish(l + 1, 0, 0)

        make(*down_pair, 0)
        add_pass(0, 1)
        make(*down_pair, 1)
        add_pass(2)
        make(*down_pair, 2)
        add_pass(3)
        make(*down_pair, 3)
        add_wait()
        norm_backward(l, 1, gmid, 6 * l + 4)
        transpose(x2.at[l], 1)
        up_pair = (1, 1, lax.rem(step + 1, 2), lambda b: 1, lambda b: gb.at[b], step > 0)
        make(*up_pair, 0)
        gather_pass(gmid, 0, 1)
        make(*up_pair, 1)
        gather_pass(gmid, 2, 3)
        relay(2, 0)
        make(*up_pair, 2)
        make(*up_pair, 3)
        transpose(x1.at[l], 0)

        @pl.when(step == 0)
        def _():
            features(down(l, x2.at[LAYERS - 1]))

        gather_wait(gmid)

        @pl.when(step == 0)
        def _():
            for h in range(2):
                add_start(h, side)

        @pl.when(step > 0)
        def _():
            add_wait(side)
            lax.fori_loop(0, count, settle(LAYERS - 1, recv2), 0)
            for k in range(N):
                oblk[k] = st[0:LAST, BLK * k : BLK * (k + 1)].astype(BF)
            go_start(2)

        da[...] = dot(gmid[...], wa[l, 3]).astype(BF)
        attend_back(l)
        relay(1, 1)
        for s in range(3):
            if s != 1:
                csum[l, s // 2 : s // 2 + 1, 0:PAD] = jnp.sum(
                    g3[s].astype(F32), axis=0, keepdims=True
                )

        def back_qkv(start, size):
            rows = pl.ds(start, size)
            value = dot_t(g3[0], wa[l, 0, rows, :])
            value = value + dot_t(g3[1], wa[l, 1, rows, :])
            value = value + dot_t(g3[2], wa[l, 2, rows, :])
            part[:, pl.ds(start, size)] = value.astype(BF)

        features(back_qkv, add_start)
        transpose(gmid, 1)
        finish(l, 2, 0)
        head_pair = (0, 0, lax.rem(step, 2), lambda s: s // 3, lambda s: g3[s], step >= 0)
        make(*head_pair, 0)
        add_pass(0)
        make(*head_pair, 1)
        add_pass(1, 2)
        make(*head_pair, 2)
        add_pass(3)
        make(*head_pair, 3)

        @pl.when(step > 0)
        def _():
            go_pass(2, out_hbm)

        add_wait()
        norm_backward(l, 0, gtop, jnp.where(l > 0, 6 * l - 1, 12))

        return 0

    lax.fori_loop(0, LAYERS, backward, 0)

    go_wait(2, out_hbm)
    sent(2)
    for k in range(N):
        oblk[k] = gst[0:LAST, BLK * k : BLK * (k + 1)].astype(BF)
    go_start(3)

    def c_copy(k):
        return remote(csum, cx.at[k], cxs.at[k], cxr.at[k], (d, near[k], c))

    def v_copy(k):
        return remote(vb.at[near[k]], vx.at[k], vxs.at[k], vxr.at[k], (d, near[k], c))

    def z_copy(k):
        return remote(
            vz.at[c], vz.at[c], vzs.at[k], vzr.at[c], (d, r, lax.rem(c + k + 1, N))
        )

    for k in range(N):
        vb[k] = vsum[:, BLK * k : BLK * (k + 1)]
    for k in range(3):
        v_copy(k).start()
        c_copy(k).start()
    go_pass(3, tg_hbm)
    relay(0, 0)
    total = vb[r]
    for k in range(3):
        v_copy(k).wait_recv()
        total = total + vx[k]
    vz[c] = total
    for k in range(3):
        z_copy(k).start()
    for k in range(3):
        c_copy(k).wait()
    for l in range(LAYERS):
        csum[l] = csum[l] + cx[0, l] + cx[1, l] + cx[2, l]
    c_half = remote(csum.at[other], cd, cds.at[0], cds.at[1], (other, r, c))
    c_half.start()
    for cs in range(N):

        @pl.when(c != cs)
        def _():
            pltpu.make_async_copy(vz.at[cs], vz.at[cs], vzr.at[cs]).wait()

    total = vz[0]
    for cs in range(1, N):
        total = total + vz[cs]
    vd[0] = total
    v_half = remote(vd.at[0], vd.at[1], vds.at[0], vds.at[1], (other, r, c))
    v_half.start()
    finish(0, 1, 1)
    finish(0, 0, 0)
    c_half.wait()
    cout[...] = csum[d] + cd[...]
    v_half.wait()
    vout[...] = vd[0] + vd[1]
    for k in range(3):
        v_copy(k).wait_send()
        z_copy(k).wait_send()

    pl.semaphore_wait(credit, 2)
    go_wait(3, tg_hbm)
    for u in (0, 1, 3):
        sent(u)
    for i in range(3):
        for j in range(2):
            arrived = result(i, other, j)
            pltpu.make_async_copy(arrived, arrived, finr.at[i, j]).wait()
    for k in range(3):
        remote(vec_ref, pin.at[r], vs.at[k], vr.at[k], (d, near[k], c)).wait_send()
    for l in range(LAYERS):
        for i in range(3):
            for k in range(2):
                for h in range(2):
                    send_w(l, i, k, h).wait_send()
                pass_w(l, i, k).wait_send()
            for k in range(3):
                share_w(l, i, k).wait_send()


def fused(*operands):
    dma = pltpu.SemaphoreType.DMA
    vmem = pltpu.VMEM
    whole = pl.BlockSpec(memory_space=pltpu.VMEM)
    anywhere = pl.BlockSpec(memory_space=pl.ANY)
    scratch = [
        vmem((LAYERS, 4, D, PAD), BF),
        vmem((LAYERS, 4, D, HALF), BF),
        vmem((LAYERS, ROWS, D), BF),
        vmem((LAYERS, ROWS, D), BF),
        vmem((LAYERS, 3, ROWS, PAD), BF),
        vmem((LAYERS, ROWS, PAD), BF),
        vmem((LAYERS, ROWS, 128), F32),
        vmem((LAYERS, 2, ROWS, HALF), BF),
        vmem((LAYERS, 2, ROWS, HALF), BF),
        vmem((LAYERS, 2, CHUNK, D), BF),
        vmem((LAYERS, 2, CHUNK, 128), F32),
        vmem((ROWS, D), BF),
        vmem((ROWS, D), BF),
        vmem((2, D, ROWS), BF),
        vmem((ROWS, D), BF),
        vmem((3, CHUNK, D), BF),
        vmem((CHUNK, D), F32),
        vmem((CHUNK, D), F32),
        vmem((N, CHUNK, BLK), BF),
        vmem((N, CHUNK, BLK), BF),
        vmem((N, LAST, BLK), BF),
        vmem((4, N, LAST, BLK), BF),
        vmem((N, 16, BLK), F32),
        vmem((16, D), F32),
        vmem((2, ROWS, HALF), BF),
        vmem((ROWS, PAD), BF),
        vmem((4, ROWS, PAD), BF),
        vmem((3, ROWS, PAD), F32),
        vmem((2, BLK, HALF), BF),
        vmem((2, N, BLK, HALF), BF),
        vmem((2, N, BLK, HALF), BF),
        vmem((3, 2, BLK, HALF), BF),
        vmem((2, BLK, PAD), F32),
        vmem((3, 2, BLK // 2, HALF), BF),
        vmem((2, LAST, D), BF),
        vmem((2, LAST, D), BF),
        vmem((3, CHUNK, D), BF),
        vmem((16, BLK), F32),
        vmem((LAYERS, 3, PAD), F32),
        vmem((16, D), F32),
        vmem((LAYERS, 4, HALF), F32),
        vmem((N, 16, BLK), F32),
        vmem((3, 16, BLK), F32),
        vmem((N, 16, BLK), F32),
        vmem((2, 16, BLK), F32),
        vmem((3, LAYERS, 4, HALF), F32),
        vmem((4, HALF), F32),
        dma((LAYERS, 3, 2)),
        dma((LAYERS, 3, 2, 2)), dma((LAYERS, 3, 2, 2)),
        dma((LAYERS, 3, 2)), dma((LAYERS, 3, 2)),
        dma((LAYERS, 3, 3)), dma((LAYERS, 3, 3)),
        dma((3,)), dma((4,)),
        dma((4, N)), dma((4, N)), dma((4, N)), dma((4, N)),
        dma((8,)), dma((N, 2)), dma((10,)), dma((4,)), dma((2, 2)),
        dma((N,)), dma((2, N)), pltpu.SemaphoreType.REGULAR,
        dma((3, 2, 2)), dma((3, 2, 2)), dma((2,)), dma((3, 2)),
        dma((3, 2)), dma((3, 2)),
        dma((8,)), dma((N, 2)), dma((10,)), dma((4,)), dma((2, 2)),
        dma((3,)), dma((3,)), dma((3,)), dma((N,)), dma((2,)),
        dma((3,)), dma((3,)), dma((2,)),
    ]
    shape = jax.ShapeDtypeStruct
    return pl.pallas_call(
        kernel,
        out_shape=(
            shape((ROWS, BLK), BF),
            shape((ROWS, BLK), BF),
            shape((4, BLK, PAD), F32),
            shape((BLK, 2 * HALF), F32),
            shape((BLK, 2 * HALF), F32),
            shape((16, BLK), F32),
            shape((4, HALF), F32),
        ),
        in_specs=[anywhere] * 4 + [whole] * 6,
        out_specs=(anywhere,) * 5 + (whole, whole),
        scratch_shapes=scratch,
        compiler_params=pltpu.CompilerParams(
            collective_id=0, has_side_effects=True, vmem_limit_bytes=67_043_328
        ),
    )(*operands)


def widen(values, axis=-1, to=PAD):
    axis = axis % values.ndim
    pads = [(0, 0)] * values.ndim
    pads[axis] = (0, to - values.shape[axis])
    return jnp.pad(values, pads)


def per_device_fused(
    tokens, cotangent, qkv_weight, qv_bias, proj_weight, proj_bias,
    up_weight, up_bias, down_weight, down_bias, norm_gain, norm_shift,
):
    dp = lax.axis_index("dp")
    both_in = widen(jnp.concatenate([tokens, cotangent]), 1, ROWS)
    heads = jnp.concatenate(
        [qkv_weight.transpose(0, 2, 1, 3), proj_weight.transpose(0, 2, 1)[:, None]], axis=1
    )
    down = down_weight.transpose(0, 2, 1)
    out, tg, ga, gu, gd, vout, cout = fused(
        both_in, widen(heads), up_weight, down,
        norm_gain, norm_shift, proj_bias, down_bias, qv_bias, up_bias,
    )
    both = vout[:12].reshape(LAYERS, 6, BLK)
    layer = lax.dynamic_slice(both, (dp, 0, 0), (1, 6, BLK))
    return (
        out[None, :SEQ].astype(F32),
        tg[None, :SEQ].astype(F32),
        ga[:3, :, :BLK].transpose(1, 0, 2)[None],
        cout[None, 0:2, :BLK],
        ga[3, :, :BLK].T[None],
        layer[:, 4],
        gu[None],
        cout[2:].reshape(1, 2 * HALF),
        gd.T[None],
        layer[:, 5],
        both[:, 0:2],
        both[:, 2:4],
    )


NORMAL = (((1,), (0,)), ((), ()))
LAST_BOTH = (((1,), (1,)), ((), ()))
FIRST_BOTH = (((0,), (0,)), ((), ()))


def gather_tokens(values):
    return lax.all_gather(values, "col", axis=0, tiled=True)


def gather_blocks(values):
    return lax.all_gather(values, "row", axis=0, tiled=True)


def gather_grad_blocks(values):
    return lax.all_gather(values, "row", axis=0, tiled=True)


def width_totals(first_sum, second_sum):
    return lax.psum((first_sum, second_sum), "row")


def gather_whole(triple_w, up_w, proj_w, down_w):
    row_whole = (triple_w, up_w, proj_w, down_w)
    col_whole = (proj_w, down_w, triple_w, up_w)
    return (row_whole, col_whole)


def row_product(gathered, matrix, contract):
    return lax.psum_scatter(
        lax.dot_general(gathered, matrix, contract, preferred_element_type=jnp.float32).astype(
            jnp.bfloat16
        ),
        "row",
        scatter_dimension=0,
        tiled=True,
    ).astype(jnp.float32)


def col_product(gathered, matrix, contract):
    return lax.psum_scatter(
        lax.dot_general(gathered, matrix, contract, preferred_element_type=jnp.float32).astype(
            jnp.bfloat16
        ),
        "col",
        scatter_dimension=0,
        tiled=True,
    ).astype(jnp.float32)


def norm_forward(stream, factor, shift):
    totals, squares = width_totals(jnp.sum(stream, axis=1), jnp.sum(stream * stream, axis=1))
    centre = totals / D
    spread = squares / D - centre * centre
    centred = stream - centre[:, None]
    scaling = lax.rsqrt(spread + EPSILON)
    standard = centred * scaling[:, None]
    return (standard * factor + shift, standard, scaling)


def norm_backward(grad_norm, standard, scaling, factor):
    factor_grad = jnp.sum(grad_norm * standard, axis=0)
    shift_grad = jnp.sum(grad_norm, axis=0)
    grad_standard = grad_norm * factor
    first_sum, second_sum = width_totals(
        jnp.sum(grad_standard, axis=1), jnp.sum(grad_standard * standard, axis=1)
    )
    grad_stream = scaling[:, None] * (
        grad_standard - first_sum[:, None] / D - standard * (second_sum[:, None] / D)
    )
    return (grad_stream, factor_grad, shift_grad)


def split_triple(triple_out, width):
    images = triple_out.shape[0] // SEQ
    head_count = width // HEAD_DIM
    pieces = triple_out.reshape(images, SEQ, 3, head_count, HEAD_DIM)
    return (pieces[:, :, 0], pieces[:, :, 1], pieces[:, :, 2])


def attend_forward(triple_out, width):
    queries, key_rows, values = split_triple(triple_out, width)
    scaling = HEAD_DIM ** (-0.5)
    scores = (
        jnp.einsum("bqhd,bkhd->bhqk", queries, key_rows, preferred_element_type=jnp.float32)
        * scaling
    )
    row_peak = jnp.max(scores, axis=-1, keepdims=True)
    log_totals = row_peak + jnp.log(jnp.sum(jnp.exp(scores - row_peak), axis=-1, keepdims=True))
    probs_low = jnp.exp(scores - log_totals).astype(jnp.bfloat16)
    attended = jnp.einsum("bhqk,bkhd->bqhd", probs_low, values, preferred_element_type=jnp.float32)
    return (attended.reshape(triple_out.shape[0], width).astype(jnp.bfloat16), log_totals)


def attend_backward(triple_out, log_totals, grad_attended, width):
    queries, key_rows, values = split_triple(triple_out, width)
    scaling = HEAD_DIM ** (-0.5)
    scores = (
        jnp.einsum("bqhd,bkhd->bhqk", queries, key_rows, preferred_element_type=jnp.float32)
        * scaling
    )
    probs = jnp.exp(scores - log_totals)
    probs_low = probs.astype(jnp.bfloat16)
    grad_heads = grad_attended.reshape(values.shape)
    grad_values = jnp.einsum(
        "bhqk,bqhd->bkhd", probs_low, grad_heads, preferred_element_type=jnp.float32
    )
    grad_probs = jnp.einsum(
        "bqhd,bkhd->bhqk", grad_heads, values, preferred_element_type=jnp.float32
    )
    grad_scores = (
        probs * (grad_probs - jnp.sum(grad_probs * probs, axis=-1, keepdims=True))
    ).astype(jnp.bfloat16)
    grad_queries = (
        jnp.einsum("bhqk,bkhd->bqhd", grad_scores, key_rows, preferred_element_type=jnp.float32)
        * scaling
    )
    grad_keys = (
        jnp.einsum("bhqk,bqhd->bkhd", grad_scores, queries, preferred_element_type=jnp.float32)
        * scaling
    )
    stacked = jnp.stack([grad_queries, grad_keys, grad_values], axis=2)
    return stacked.reshape(triple_out.shape[0], 3 * width).astype(jnp.bfloat16)


def layer_forward(stream, weights):
    qkv_w, qv_b, proj_w, proj_b, up_w, up_b, down_w, down_b, factors, shifts = weights
    width = qkv_w.shape[2]
    triple_w = qkv_w.reshape(qkv_w.shape[0], 3 * width)
    row_whole, col_whole = gather_whole(triple_w, up_w, proj_w, down_w)
    first_norm, first_standard, first_scaling = norm_forward(stream, factors[0], shifts[0])
    first_rows = gather_tokens(first_norm.astype(jnp.bfloat16))
    offsets = jnp.concatenate([qv_b[0], jnp.zeros_like(qv_b[0]), qv_b[1]])
    triple_out = (row_product(first_rows, triple_w, NORMAL) + offsets).astype(jnp.bfloat16)
    attended, log_totals = attend_forward(triple_out, width)
    head_rows = gather_blocks(attended)
    stream_mid = stream + col_product(head_rows, proj_w, NORMAL) + proj_b
    second_norm, second_standard, second_scaling = norm_forward(stream_mid, factors[1], shifts[1])
    second_rows = gather_tokens(second_norm.astype(jnp.bfloat16))
    before = row_product(second_rows, up_w, NORMAL) + up_b
    activated = jax.nn.gelu(before, approximate=False).astype(jnp.bfloat16)
    hidden_rows = gather_blocks(activated)
    branch_out = col_product(hidden_rows, down_w, NORMAL)
    stream_out = stream_mid + branch_out + down_b
    saved = (
        first_rows,
        first_standard,
        first_scaling,
        triple_out,
        log_totals,
        head_rows,
        second_rows,
        second_standard,
        second_scaling,
        before,
        hidden_rows,
        row_whole,
        col_whole,
    )
    return (stream_out, saved)


def layer_backward(grad_out, saved, weights):
    qkv_w, qv_b, proj_w, proj_b, up_w, up_b, down_w, down_b, factors, shifts = weights
    (
        first_rows,
        first_standard,
        first_scaling,
        triple_out,
        log_totals,
        head_rows,
        second_rows,
        second_standard,
        second_scaling,
        before,
        hidden_rows,
        row_whole,
        col_whole,
    ) = saved
    width = qkv_w.shape[2]
    triple_w = qkv_w.reshape(qkv_w.shape[0], 3 * width)
    grad_rows = gather_tokens(grad_out.astype(jnp.bfloat16))
    down_grad = lax.dot_general(
        hidden_rows, grad_rows, FIRST_BOTH, preferred_element_type=jnp.float32
    )
    down_off_grad = jnp.sum(grad_rows, axis=0, dtype=jnp.float32)
    grad_active = row_product(grad_rows, down_w, LAST_BOTH)
    _, slope_pull = jax.vjp(partial(jax.nn.gelu, approximate=False), before)
    grad_before = slope_pull(grad_active)[0].astype(jnp.bfloat16)
    before_rows = gather_grad_blocks(grad_before)
    up_grad = lax.dot_general(
        second_rows, before_rows, FIRST_BOTH, preferred_element_type=jnp.float32
    )
    up_off_grad = jnp.sum(before_rows, axis=0, dtype=jnp.float32)
    grad_second = col_product(before_rows, up_w, LAST_BOTH)
    grad_mid, second_factor_grad, second_shift_grad = norm_backward(
        grad_second, second_standard, second_scaling, factors[1]
    )
    grad_mid = grad_mid + grad_out
    mid_rows = gather_tokens(grad_mid.astype(jnp.bfloat16))
    proj_grad = lax.dot_general(head_rows, mid_rows, FIRST_BOTH, preferred_element_type=jnp.float32)
    proj_off_grad = jnp.sum(mid_rows, axis=0, dtype=jnp.float32)
    grad_attended = row_product(mid_rows, proj_w, LAST_BOTH).astype(jnp.bfloat16)
    grad_triple = attend_backward(triple_out, log_totals, grad_attended, width)
    triple_rows = gather_grad_blocks(grad_triple)
    triple_grad = lax.dot_general(
        first_rows, triple_rows, FIRST_BOTH, preferred_element_type=jnp.float32
    )
    column_sums = jnp.sum(triple_rows, axis=0, dtype=jnp.float32).reshape(3, width)
    qv_grad = jnp.stack([column_sums[0], column_sums[2]])
    grad_first = col_product(triple_rows, triple_w, LAST_BOTH)
    grad_in, first_factor_grad, first_shift_grad = norm_backward(
        grad_first, first_standard, first_scaling, factors[0]
    )
    grad_in = grad_in + grad_mid
    factor_grads = jnp.stack([first_factor_grad, second_factor_grad])
    shift_grads = jnp.stack([first_shift_grad, second_shift_grad])
    layer_grads = (
        triple_grad.reshape(qkv_w.shape),
        qv_grad,
        proj_grad,
        proj_off_grad,
        up_grad,
        up_off_grad,
        down_grad,
        down_off_grad,
        factor_grads,
        shift_grads,
    )
    return (grad_in, layer_grads)


def per_device_plain(
    tokens,
    cotangent,
    qkv_weight,
    qv_bias,
    proj_weight,
    proj_bias,
    up_weight,
    up_bias,
    down_weight,
    down_bias,
    norm_gain,
    norm_shift,
):
    image_count, seq_len, width_row = tokens.shape
    stream = tokens.reshape(image_count * seq_len, width_row).astype(jnp.float32)
    layer_params = []
    saved_list = []
    for layer_index in range(LAYERS):
        params = (
            qkv_weight[layer_index],
            qv_bias[layer_index],
            proj_weight[layer_index],
            proj_bias[layer_index],
            up_weight[layer_index],
            up_bias[layer_index],
            down_weight[layer_index],
            down_bias[layer_index],
            norm_gain[layer_index],
            norm_shift[layer_index],
        )
        layer_params.append(params)
        stream, saved = layer_forward(stream, params)
        saved_list.append(saved)
    grad_stream = cotangent.reshape(image_count * seq_len, width_row).astype(jnp.float32)
    per_layer = [None] * LAYERS
    for layer_index in reversed(range(LAYERS)):
        grad_stream, layer_grads = layer_backward(
            grad_stream, saved_list[layer_index], layer_params[layer_index]
        )
        per_layer[layer_index] = layer_grads
    stacked = tuple(
        (jnp.stack([layer_grads[position] for layer_grads in per_layer]) for position in range(10))
    )
    summed = (
        lax.psum_scatter(
            stacked[0].astype(jnp.bfloat16), "dp", scatter_dimension=0, tiled=True
        ).astype(jnp.float32),
        lax.psum_scatter(
            stacked[1].astype(jnp.bfloat16), "dp", scatter_dimension=0, tiled=True
        ).astype(jnp.float32),
        lax.psum_scatter(
            stacked[2].astype(jnp.bfloat16), "dp", scatter_dimension=0, tiled=True
        ).astype(jnp.float32),
        lax.psum_scatter(
            stacked[3].astype(jnp.bfloat16), "dp", scatter_dimension=0, tiled=True
        ).astype(jnp.float32),
        lax.psum_scatter(
            stacked[4].astype(jnp.bfloat16), "dp", scatter_dimension=0, tiled=True
        ).astype(jnp.float32),
        lax.psum_scatter(
            stacked[5].astype(jnp.bfloat16), "dp", scatter_dimension=0, tiled=True
        ).astype(jnp.float32),
        lax.psum_scatter(
            stacked[6].astype(jnp.bfloat16), "dp", scatter_dimension=0, tiled=True
        ).astype(jnp.float32),
        lax.psum_scatter(
            stacked[7].astype(jnp.bfloat16), "dp", scatter_dimension=0, tiled=True
        ).astype(jnp.float32),
    )
    norm_sums = lax.psum((stacked[8], stacked[9]), ("dp", "col"))
    result = stream.reshape(image_count, seq_len, width_row)
    tokens_grad = grad_stream.reshape(image_count, seq_len, width_row)
    return (
        result,
        tokens_grad,
        summed[0],
        summed[1],
        summed[2],
        summed[3],
        summed[4],
        summed[5],
        summed[6],
        summed[7],
        norm_sums[0],
        norm_sums[1],
    )


def solution(mesh):
    placed = (
        P(("dp", "col"), None, "row"),
        P(("dp", "col"), None, "row"),
        P(None, "row", None, "col"),
        P(None, None, "col"),
        P(None, "col", "row"),
        P(None, "row"),
        P(None, "row", "col"),
        P(None, "col"),
        P(None, "col", "row"),
        P(None, "row"),
        P(None, None, "row"),
        P(None, None, "row"),
    )
    sizes = (mesh.shape["dp"], mesh.shape["row"], mesh.shape["col"])
    return jax.shard_map(
        per_device_fused if sizes == (2, N, N) else per_device_plain,
        mesh=mesh,
        in_specs=placed,
        out_specs=(
            P(("dp", "col"), None, "row"),
            P(("dp", "col"), None, "row"),
            P("dp", "row", None, "col"),
            P("dp", None, "col"),
            P("dp", "col", "row"),
            P("dp", "row"),
            P("dp", "row", "col"),
            P("dp", "col"),
            P("dp", "col", "row"),
            P("dp", "row"),
            P(None, None, "row"),
            P(None, None, "row"),
        ),
        check_vma=False,
    )
```
